128 devices in a mesh: member: 4 (over z_hi, core), py: 4 (over x), pz: 8 (over y, z_lo).
Axes of the slice: x: 4, y: 4, z: 4 (z_hi: 2, z_lo: 2; z = z_hi * 2 + z_lo), core: 2. Of those that a mesh axis runs over, the one named last changes fastest.
Arguments:
- velocity_hat: float32 [8, 3, 96, 36864], P('member', None, None, ('py', 'pz')), parts along dimension 0, may hold values from -448 to 448
- time_step: float32 [4], P('member'), parts along dimension 0, may hold values from 0.003 to 0.006
- power: float32 [4], P('member'), parts along dimension 0, may hold values from 20 to 80
- cutoffs: int32 [12], P('member'), parts along dimension 0, may hold values from 48 to 64, as said below
Outputs:
- velocity_next: float32 [8, 3, 96, 36864], P('member', None, None, ('py', 'pz')), parts along dimension 0
- cfl_number: float32 [4], P('member'), parts along dimension 0
- energy: float32 [4], P('member'), parts along dimension 0
The draws below stay inside these ranges and needn't reach their ends.
There are 4 independent parts, one for each index of `member`. The reference program is written for one: setup_inputs(seed, part) draws one part's arguments, and reference() takes and returns one part's arrays. A program takes and returns all parts, laid end to end along the dimension named above; each array names one. Nothing has to cross between parts.
Inputs may be any that keep to these rules, and one draw needn't show every extreme that they name: `cutoffs`: in every draw one of the three equals 64.
All inputs are finite; a program needn't handle non-finite values.
Results may differ from the reference program's by a relative error of at most 0.0002.
Values sent between devices are 32-bit elements; how exact they have to be, the bound alone decides.
A program may use at most 128 MiB of HBM per device.

```python
import math
import jax
import jax.numpy as jnp
from jax import lax

GRID = 192
SECTIONS = 1


def signed_wave(points):
    index = jnp.arange(points, dtype=jnp.int32)
    return jnp.where(index < points // 2, index, index - points)


def draw_velocity_hat(key, part):
    folded = jax.random.fold_in(key, 17)
    noise_key, scale_key = jax.random.split(folded)
    array_shape = (2, 3, GRID // 2, GRID, GRID)
    depth_wave = jnp.arange(GRID // 2, dtype=jnp.int32)[:, None, None]
    across_y = signed_wave(GRID)[None, :, None]
    along_x = signed_wave(GRID)[None, None, :]
    lowest = (depth_wave <= 2) & (jnp.abs(across_y) <= 2) & (jnp.abs(along_x) <= 2)
    values = jnp.clip(jax.random.normal(noise_key, array_shape, jnp.float32), -4.0, 4.0)
    amplify = 64.0
    result = jnp.where(lowest, amplify * values, values).astype(jnp.float32)
    return result.reshape(2, 3, GRID // 2, GRID * GRID)


def draw_cutoffs(key, part):
    folded = jax.random.fold_in(key, 23)
    value_key, pick_key = jax.random.split(folded)
    values = jax.random.randint(value_key, (3,), GRID // 4, GRID // 3 + 1, dtype=jnp.int32)
    chosen = jax.random.randint(pick_key, (), 0, 3, dtype=jnp.int32)
    return jnp.where(jnp.arange(3, dtype=jnp.int32) == chosen, GRID // 3, values).astype(jnp.int32)


def setup_inputs(seed: int = 0, part: int = 0) -> dict:
    key_list = jax.random.split(jax.random.key(seed), 5)
    part_splits = jax.random.split(jax.random.fold_in(key_list[4], part), 5)
    return {
        "velocity_hat": draw_velocity_hat(jax.random.fold_in(jax.random.fold_in(key_list[4], part), 71), part),
        "time_step": jnp.clip(jax.random.uniform(part_splits[1], (1,), jnp.float32, 0.003, 0.006), 0.003, 0.006),
        "power": jnp.clip(jnp.exp(jax.random.uniform(part_splits[2], (1,), jnp.float32, math.log(20.0), math.log(80.0))), 20.0, 80.0),
        "cutoffs": draw_cutoffs(jax.random.fold_in(jax.random.fold_in(key_list[4], part), 71), part),
    }


viscosity = 0.004
keep_share = (0.0, 0.75, 1.0 / 3.0)


def signed_index(points):
    index = jnp.arange(points, dtype=jnp.int32)
    return jnp.where(index < points // 2, index, index - points)


def to_grid(spectra):
    points = spectra.shape[-1]
    result = []
    for component in range(spectra.shape[0]):
        strips = jnp.fft.ifft(jnp.fft.ifft(spectra[component], axis=2), axis=1)
        padded = jnp.concatenate([strips, jnp.zeros_like(strips[:1])], axis=0)
        result.append(jnp.fft.irfft(padded, n=points, axis=0) * (float(points) ** 1.5))
    return jnp.stack(result)


def to_spectrum(fields):
    points = fields.shape[-1]
    result = []
    for component in range(fields.shape[0]):
        planes = jnp.fft.rfft(fields[component], axis=0)[: points // 2]
        result.append(jnp.fft.fft(jnp.fft.fft(planes, axis=1), axis=2) * (float(points) ** -1.5))
    return result


def reference(velocity_hat, time_step, power, cutoffs):
    points = 2 * velocity_hat.shape[2]
    velocity_hat = velocity_hat.reshape(2, 3, points // 2, points, points)
    wave_z = jnp.arange(points // 2, dtype=jnp.int32)[:, None, None]
    wave_y = signed_index(points)[None, :, None]
    wave_x = signed_index(points)[None, None, :]
    keep_mask = ((jnp.abs(wave_x) <= cutoffs[0]) & (jnp.abs(wave_y) <= cutoffs[1]) & (wave_z <= cutoffs[2])).astype(jnp.float32)
    waves = (wave_x.astype(jnp.float32), wave_y.astype(jnp.float32), wave_z.astype(jnp.float32))
    wave_square = waves[0] * waves[0] + waves[1] * waves[1] + waves[2] * waves[2]
    inverse_square = 1.0 / jnp.maximum(wave_square, 1.0)

    def project(field):
        normal_part = waves[0] * field[0] + waves[1] * field[1] + waves[2] * field[2]
        return [keep_mask * (field[axis_index] - waves[axis_index] * normal_part * inverse_square) for axis_index in range(3)]

    step_size = time_step[0]
    current = [lax.complex(velocity_hat[0, axis_index], velocity_hat[1, axis_index]) for axis_index in range(3)]
    initial = current
    cfl_values = []
    energy_values = []
    for section_index in range(SECTIONS):
        solenoidal = project(current)
        if section_index == 0:
            initial = solenoidal
        curled = [waves[1] * solenoidal[2] - waves[2] * solenoidal[1],
                  waves[2] * solenoidal[0] - waves[0] * solenoidal[2],
                  waves[0] * solenoidal[1] - waves[1] * solenoidal[0]]
        vorticity_hat = [1j * term for term in curled]
        physical = to_grid(jnp.stack(solenoidal + vorticity_hat))
        velocity = physical[:3]
        vorticity = physical[3:]
        nonlinear = jnp.stack([velocity[1] * vorticity[2] - velocity[2] * vorticity[1],
                               velocity[2] * vorticity[0] - velocity[0] * vorticity[2],
                               velocity[0] * vorticity[1] - velocity[1] * vorticity[0]])
        fastest = jnp.max(jnp.abs(velocity[0]) + jnp.abs(velocity[1]) + jnp.abs(velocity[2]))
        energy = 0.5 * jnp.sum(velocity * velocity) / float(points ** 3)
        forced = project(to_spectrum(nonlinear))
        forcing = power[0] / jnp.maximum(2.0 * energy, 0.5)
        update = [solenoidal[axis_index] + step_size * (forced[axis_index] + forcing * solenoidal[axis_index] - viscosity * wave_square * solenoidal[axis_index]) for axis_index in range(3)]
        keep_weight = keep_share[section_index]
        current = [keep_weight * initial[axis_index] + (1.0 - keep_weight) * update[axis_index] for axis_index in range(3)]
        cfl_values.append(step_size * fastest * points / (2.0 * math.pi))
        energy_values.append(energy)
    velocity_next = jnp.stack([jnp.stack([jnp.real(term) for term in current]), jnp.stack([jnp.imag(term) for term in current])]).astype(jnp.float32)
    velocity_next = velocity_next.reshape(2, 3, points // 2, points * points)
    return velocity_next, jnp.stack(cfl_values), jnp.stack(energy_values)
```

```python
import functools
import math

import jax
import jax.numpy as jnp
import ml_dtypes
import numpy as np
from jax import lax
from jax.experimental import pallas as pl
from jax.experimental.pallas import tpu as pltpu
from jax.sharding import PartitionSpec as P

GRID = 192
PARTS = 32
BAND = 6
DEPTH = 72
LIVE = tuple(range(11)) + tuple(range(21, 32))
viscosity = 0.004
f32 = jnp.float32
bf16 = jnp.bfloat16


def halves(table):
    high = table.astype(ml_dtypes.bfloat16)
    low = (table - high.astype(np.float64)).astype(ml_dtypes.bfloat16)
    return np.stack([high, low])


def angle(rows, cols):
    turns = np.outer(rows, cols) % GRID
    return turns * (2.0 * math.pi / GRID)


@functools.lru_cache
def tables():
    n = GRID
    every = np.arange(n)
    phase = angle(every, every)
    tx = np.zeros((2, PARTS, 8, 512))
    cosine, sine = (f(phase).reshape(PARTS, BAND, n) for f in (np.cos, np.sin))
    tx[0, :, :BAND, :n], tx[0, :, :BAND, 256 : 256 + n] = cosine, -sine
    tx[1, :, :BAND, :n], tx[1, :, :BAND, 256 : 256 + n] = sine, cosine
    tx = tx.reshape(512, 512)
    ey = np.zeros((2 * n, 2 * n))
    for at, band in enumerate(LIVE):
        phase = angle(every, band * BAND + np.arange(BAND))
        cols = slice(8 * at, 8 * at + BAND)
        ey[:n, cols] = np.cos(phase)
        ey[n:, cols] = np.sin(phase)
        cols = slice(n + 8 * at, n + 8 * at + BAND)
        ey[:n, cols] = -np.sin(phase)
        ey[n:, cols] = np.cos(phase)
    factor = float(n) ** -1.5
    depth = np.arange(n // 3 + 1)
    phase = angle(depth, every)
    weight = np.where(depth == 0, 1.0, 2.0)[:, None] * factor
    zt = np.zeros((256, n))
    zt[: len(depth)] = weight * np.cos(phase)
    zt[128 : 128 + len(depth)] = -weight * np.sin(phase)
    zb = np.zeros((n, 256))
    zb[:, : len(depth)] = factor * np.cos(phase.T)
    zb[:, 128 : 128 + len(depth)] = -factor * np.sin(phase.T)
    eyt = np.zeros((272, 2 * n))
    for at, band in enumerate(LIVE):
        phase = angle(band * BAND + np.arange(BAND), every)
        rows = slice(12 * at, 12 * at + BAND)
        eyt[rows, :n], eyt[rows, n:] = np.cos(phase), np.sin(phase)
        rows = slice(12 * at + BAND, 12 * at + 2 * BAND)
        eyt[rows, :n], eyt[rows, n:] = -np.sin(phase), np.cos(phase)
    return tuple(halves(t) for t in (tx, ey, zt, zb, eyt))


def split(value):
    high = value.astype(bf16)
    return high, (value - high.astype(f32)).astype(bf16)


def table_by_data(table, data, dims):
    high, low = split(data)
    dot = functools.partial(
        lax.dot_general, dimension_numbers=(dims, ((), ())), preferred_element_type=f32
    )
    return dot(table[0], high) + dot(table[0], low) + dot(table[1], high)


def data_by_table(data, table):
    high, low = split(data)
    dot = functools.partial(jnp.dot, preferred_element_type=f32)
    return dot(high, table[0]) + dot(low, table[0]) + dot(high, table[1])


def signed(index):
    return jnp.where(index < GRID // 2, index, index - GRID)


def pair_waves(pair, cut_ref):
    band = lax.axis_index("py") * lax.axis_size("pz") + lax.axis_index("pz")
    lane = lax.broadcasted_iota(jnp.int32, (DEPTH, 384), 1)
    upper = lane >= GRID
    kx = signed(jnp.where(upper, lane - GRID, lane))
    ky = signed(band * BAND + 2 * pair + upper.astype(jnp.int32))
    kz = lax.broadcasted_iota(jnp.int32, (DEPTH, 384), 0)
    keep = (
        (jnp.abs(kx) <= cut_ref[0]) & (jnp.abs(ky) <= cut_ref[1]) & (kz <= cut_ref[2])
    )
    waves = tuple(k.astype(f32) for k in (kx, ky, kz))
    square = waves[0] * waves[0] + waves[1] * waves[1] + waves[2] * waves[2]
    return waves, square, 1.0 / jnp.maximum(square, 1.0), keep


def project(field, waves, inverse, keep):
    normal = (waves[0] * field[0] + waves[1] * field[1] + waves[2] * field[2]) * inverse
    return [jnp.where(keep, field[a] - waves[a] * normal, 0.0) for a in range(3)]


def spread_kernel(cut_ref, in_ref, tx_ref, out_ref, data, made):
    data[5 * DEPTH :, :] = jnp.zeros((384 - 5 * DEPTH, 512), f32)

    def step(pair, carry):
        window = pl.ds(pl.multiple_of(pair * 384, 128), 384)
        waves, _, inverse, keep = pair_waves(pair, cut_ref)
        parts = []
        for c in range(2):
            field = [in_ref[c, a, :, window] for a in range(3)]
            sol = project(field, waves, inverse, keep)
            curl_y = waves[2] * sol[0] - waves[0] * sol[2]
            curl_z = waves[0] * sol[1] - waves[1] * sol[0]
            parts.append((sol, (curl_y, curl_z)))
        fields = (
            parts[0][0] + [-parts[1][1][0], -parts[1][1][1]],
            parts[1][0] + [parts[0][1][0], parts[0][1][1]],
        )
        for odd in range(2):
            for c in range(2):
                for f in range(5):
                    value = fields[c][f]
                    if odd:
                        value = pltpu.roll(value[:, 128:], 192, 1)
                    else:
                        value = value[:, :256]
                    data[f * DEPTH : (f + 1) * DEPTH, c * 256 : (c + 1) * 256] = value
            made[odd] = table_by_data(tx_ref, data[...], ((1,), (1,)))
        rows = pl.ds(pl.multiple_of(pair * 24, 8), 24)
        for d in range(PARTS):
            pieces = [
                made[odd, c * 256 + d * 8 : c * 256 + d * 8 + BAND, :]
                for odd in range(2)
                for c in range(2)
            ]
            piece = jnp.concatenate(pieces, axis=0)
            for third in range(3):
                out_ref[d, third, rows, :] = piece[:, third * 128 : (third + 1) * 128]
        return carry

    lax.fori_loop(0, 3, step, 0)


def grid_kernel(in_ref, ey_ref, zt_ref, zb_ref, eyt_ref, out_ref, rows_ref, strips, physical, back, made, top, total):
    rows_ref[...] = jnp.zeros_like(rows_ref)
    top[...] = jnp.zeros_like(top)
    total[...] = jnp.zeros_like(total)
    at = lax.broadcasted_iota(jnp.int32, (192, DEPTH), 0)
    band = at // 8
    band = jnp.where(band < 11, band, band + 10)
    ky = signed(band * BAND + at % 8).astype(f32)
    kz = lax.broadcasted_iota(jnp.int32, (192, DEPTH), 1).astype(f32)
    lane = lax.broadcasted_iota(jnp.int32, (192, 128), 1)

    def step(pair, carry):
        for odd in range(2):
            x = 2 * pair + odd
            for c in range(2):
                for i, s in enumerate(LIVE):
                    for third in range(3):
                        rows_ref[
                            c * 192 + 8 * i : c * 192 + 8 * i + BAND,
                            third * 128 : (third + 1) * 128,
                        ] = in_ref[s, third, pl.ds(c * BAND + x, BAND, stride=12), :]
            turned = [
                ky * rows_ref[c * 192 : (c + 1) * 192, 144:216]
                - kz * rows_ref[c * 192 : (c + 1) * 192, 72:144]
                for c in range(2)
            ]
            rows_ref[:192, 384 : 384 + DEPTH] = -turned[1]
            rows_ref[192:, 384 : 384 + DEPTH] = turned[0]
            strips[...] = table_by_data(ey_ref, rows_ref[...], ((1,), (0,)))
            for f in range(6):
                low = 72 * f if f < 5 else 384
                both = jnp.concatenate(
                    [strips[:192, low : low + 128], strips[192:, low : low + 128]], axis=1
                )
                physical[f] = data_by_table(both, zt_ref)
            u = [physical[f] for f in range(3)]
            w = [physical[5], physical[3], physical[4]]
            speed = jnp.abs(u[0]) + jnp.abs(u[1]) + jnp.abs(u[2])
            squares = u[0] * u[0] + u[1] * u[1] + u[2] * u[2]
            top[...] = jnp.maximum(top[...], jnp.max(speed.reshape(24, 8, GRID), axis=0))
            total[...] += jnp.sum(squares.reshape(24, 8, GRID), axis=0)
            q = [
                data_by_table(u[1] * w[2] - u[2] * w[1], zb_ref),
                data_by_table(u[2] * w[0] - u[0] * w[2], zb_ref),
                data_by_table(u[0] * w[1] - u[1] * w[0], zb_ref),
            ]
            for c in range(2):
                q0, q1, q2 = (part[:, c * 128 : (c + 1) * 128] for part in q)
                q1 = pltpu.roll(q1, 72, 1)
                back[c * 192 : (c + 1) * 192, :128] = jnp.where(lane < 72, q0, q1)
                back[c * 192 : (c + 1) * 192, 128:] = jnp.where(
                    lane < 16, q1, pltpu.roll(q2, 16, 1)
                )
            made[odd] = table_by_data(eyt_ref, back[...], ((1,), (0,)))
        rows = pl.ds(pl.multiple_of(pair * 24, 8), 24)
        for i, s in enumerate(LIVE):
            piece = jnp.concatenate(
                [made[0, 12 * i : 12 * i + 12, :], made[1, 12 * i : 12 * i + 12, :]], axis=0
            )
            for half in range(2):
                out_ref[s, half, rows, :] = piece[:, half * 128 : (half + 1) * 128]
        return carry

    for d in range(11, 21):
        out_ref[d] = jnp.zeros((2, 72, 128), f32)
    lax.fori_loop(0, 3, step, 0)
    fastest = jnp.max(top[...])
    summed = jnp.sum(total[...])
    spare = lax.broadcasted_iota(jnp.int32, (8, 128), 1)
    for d in range(PARTS):
        tile = out_ref[d, 1, :8, :]
        out_ref[d, 1, :8, :] = jnp.where(
            spare == 112, fastest, jnp.where(spare == 113, summed, tile)
        )


def close_kernel(cut_ref, dt_ref, power_ref, old_ref, in_ref, tx_ref, out_ref, cfl_ref, energy_ref, gathered, terms, spectra):
    gathered[...] = jnp.zeros_like(gathered)
    stats = [in_ref[s, 1, :8, :] for s in range(PARTS)]
    fastest, summed = stats[0], stats[0]
    for s in range(1, PARTS):
        fastest = jnp.maximum(fastest, stats[s])
        summed = summed + stats[s]
    spot = lax.broadcasted_iota(jnp.int32, (8, 128), 1)
    first = lax.broadcasted_iota(jnp.int32, (8, 128), 0) == 0
    fastest = jnp.max(jnp.where((spot == 112) & first, fastest, 0.0))
    summed = jnp.sum(jnp.where((spot == 113) & first, summed, 0.0))
    energy = 0.5 * summed * (1.0 / float(GRID**3))
    dt = dt_ref[0]
    cfl_ref[0] = dt * fastest * GRID * (1.0 / (2.0 * math.pi))
    energy_ref[0] = energy
    twice = jnp.maximum(jnp.full((DEPTH, 384), 2.0 * energy, f32), 0.5)
    forcing = power_ref[0] / twice

    out_ref[:, :, DEPTH:, :] = jnp.zeros((2, 3, 96 - DEPTH, 1152), f32)

    def step(pair, carry):
        window = pl.ds(pl.multiple_of(pair * 384, 128), 384)
        for odd in range(2):
            ky = 2 * pair + odd
            for c in range(2):
                for half in range(2):
                    for s in range(PARTS):
                        gathered[8 * s : 8 * s + BAND, :] = in_ref[
                            s, half, pl.ds(c * BAND + ky, BAND, stride=12), :
                        ]
                    terms[half * 128 : (half + 1) * 128, c * 256 : (c + 1) * 256] = gathered[...].T
            spectra[odd] = data_by_table(terms[: 3 * DEPTH, :], tx_ref)
        waves, square, inverse, keep = pair_waves(pair, cut_ref)
        for c in range(2):
            old = project([old_ref[c, a, :, window] for a in range(3)], waves, inverse, keep)
            new = []
            for a in range(3):
                rows = slice(a * DEPTH, (a + 1) * DEPTH)
                even = spectra[0, rows, c * 256 : (c + 1) * 256]
                odd = pltpu.roll(spectra[1, rows, c * 256 : (c + 1) * 256], 64, 1)
                new.append(
                    jnp.concatenate([even[:, :128], even[:, 128:] + odd[:, :128], odd[:, 128:]], axis=1)
                )
            forced = project(new, waves, inverse, keep)
            for a in range(3):
                out_ref[c, a, :DEPTH, window] = old[a] + dt * (
                    forced[a] + forcing * old[a] - viscosity * square * old[a]
                )
        return carry

    lax.fori_loop(0, 3, step, 0)


VM = pl.BlockSpec(memory_space=pltpu.VMEM)
SM = pl.BlockSpec(memory_space=pltpu.SMEM)
GRANT = pltpu.CompilerParams(vmem_limit_bytes=60 * 1024 * 1024)


def on_device(velocity_hat, time_step, power, cutoffs):
    tx, ey, zt, zb, eyt = (jnp.asarray(t) for t in tables())
    shape = jax.ShapeDtypeStruct
    block = pl.BlockSpec((2, 3, DEPTH, 1152), lambda i: (0, 0, 0, 0))
    whole = lambda a: pl.BlockSpec(a.shape, lambda i: (0,) * a.ndim)
    chunks = pl.pallas_call(
        spread_kernel,
        grid=(1,),
        out_shape=shape((PARTS, 3, 72, 128), f32),
        in_specs=[SM, block, whole(tx)],
        out_specs=pl.BlockSpec((PARTS, 3, 72, 128), lambda i: (0, 0, 0, 0)),
        scratch_shapes=[pltpu.VMEM((384, 512), f32), pltpu.VMEM((2, 512, 384), f32)],
        compiler_params=GRANT,
    )(cutoffs, velocity_hat, tx)
    chunks = lax.all_to_all(chunks, ("py", "pz"), 0, 0, tiled=True)
    chunks = pl.pallas_call(
        grid_kernel,
        out_shape=shape((PARTS, 2, 72, 128), f32),
        in_specs=[VM] * 5,
        out_specs=VM,
        scratch_shapes=[
            pltpu.VMEM((384, 512), f32),
            pltpu.VMEM((384, 512), f32),
            pltpu.VMEM((6, GRID, GRID), f32),
            pltpu.VMEM((384, 256), f32),
            pltpu.VMEM((2, 272, 256), f32),
            pltpu.VMEM((8, GRID), f32),
            pltpu.VMEM((8, GRID), f32),
        ],
        compiler_params=GRANT,
    )(chunks, ey, zt, zb, eyt)
    chunks = lax.all_to_all(chunks, ("py", "pz"), 0, 0, tiled=True)
    return pl.pallas_call(
        close_kernel,
        grid=(1,),
        out_shape=(shape((2, 3, 96, 1152), f32), shape((1,), f32), shape((1,), f32)),
        in_specs=[SM, SM, SM, block, whole(chunks), whole(tx)],
        out_specs=(pl.BlockSpec((2, 3, 96, 1152), lambda i: (0, 0, 0, 0)), SM, SM),
        scratch_shapes=[pltpu.VMEM((256, 128), f32), pltpu.VMEM((256, 512), f32), pltpu.VMEM((2, 3 * DEPTH, 512), f32)],
        compiler_params=GRANT,
    )(cutoffs, time_step, power, velocity_hat, chunks, tx)


def solution(mesh):
    return jax.shard_map(
        on_device,
        mesh=mesh,
        in_specs=(P("member", None, None, ("py", "pz")), P("member"), P("member"), P("member")),
        out_specs=(P("member", None, None, ("py", "pz")), P("member"), P("member")),
        check_vma=False,
    )
```

```python
import functools
import math

import jax
import jax.numpy as jnp
import ml_dtypes
import numpy as np
from jax import lax
from jax.experimental import pallas as pl
from jax.experimental.pallas import tpu as pltpu
from jax.sharding import PartitionSpec as P

GRID = 192
PARTS = 32
BAND = 6
DEPTH = 72
LIVE = tuple(range(11)) + tuple(range(21, 32))
viscosity = 0.004
f32 = jnp.float32
bf16 = jnp.bfloat16


def halves(table):
    high = table.astype(ml_dtypes.bfloat16)
    low = (table - high.astype(np.float64)).astype(ml_dtypes.bfloat16)
    return np.stack([high, low])


def angle(rows, cols):
    turns = np.outer(rows, cols) % GRID
    return turns * (2.0 * math.pi / GRID)


@functools.lru_cache
def tables():
    n = GRID
    every = np.arange(n)
    phase = angle(every, every)
    tx = np.zeros((2, PARTS, 8, 512))
    cosine, sine = (f(phase).reshape(PARTS, BAND, n) for f in (np.cos, np.sin))
    tx[0, :, :BAND, :n], tx[0, :, :BAND, 256 : 256 + n] = cosine, -sine
    tx[1, :, :BAND, :n], tx[1, :, :BAND, 256 : 256 + n] = sine, cosine
    tx = tx.reshape(512, 512)
    ey = np.zeros((2 * n, 2 * n))
    for at, band in enumerate(LIVE):
        phase = angle(every, band * BAND + np.arange(BAND))
        cols = slice(8 * at, 8 * at + BAND)
        ey[:n, cols] = np.cos(phase)
        ey[n:, cols] = np.sin(phase)
        cols = slice(n + 8 * at, n + 8 * at + BAND)
        ey[:n, cols] = -np.sin(phase)
        ey[n:, cols] = np.cos(phase)
    factor = float(n) ** -1.5
    depth = np.arange(n // 3 + 1)
    phase = angle(depth, every)
    weight = np.where(depth == 0, 1.0, 2.0)[:, None] * factor
    zt = np.zeros((256, n))
    zt[: len(depth)] = weight * np.cos(phase)
    zt[128 : 128 + len(depth)] = -weight * np.sin(phase)
    zb = np.zeros((n, 256))
    zb[:, : len(depth)] = factor * np.cos(phase.T)
    zb[:, 128 : 128 + len(depth)] = -factor * np.sin(phase.T)
    eyt = np.zeros((272, 2 * n))
    for at, band in enumerate(LIVE):
        phase = angle(band * BAND + np.arange(BAND), every)
        rows = slice(12 * at, 12 * at + BAND)
        eyt[rows, :n], eyt[rows, n:] = np.cos(phase), np.sin(phase)
        rows = slice(12 * at + BAND, 12 * at + 2 * BAND)
        eyt[rows, :n], eyt[rows, n:] = -np.sin(phase), np.cos(phase)
    return tuple(halves(t) for t in (tx, ey, zt, zb, eyt))


def split(value):
    high = value.astype(bf16)
    return high, (value - high.astype(f32)).astype(bf16)


def table_by_data(table, data, dims):
    high, low = split(data)
    dot = functools.partial(
        lax.dot_general, dimension_numbers=(dims, ((), ())), preferred_element_type=f32
    )
    return dot(table[0], high) + dot(table[0], low) + dot(table[1], high)


def data_by_table(data, table):
    high, low = split(data)
    dot = functools.partial(jnp.dot, preferred_element_type=f32)
    return dot(high, table[0]) + dot(low, table[0]) + dot(high, table[1])


def signed(index):
    return jnp.where(index < GRID // 2, index, index - GRID)


def pair_waves(pair, cut_ref):
    band = lax.axis_index("py") * lax.axis_size("pz") + lax.axis_index("pz")
    lane = lax.broadcasted_iota(jnp.int32, (DEPTH, 384), 1)
    upper = lane >= GRID
    kx = signed(jnp.where(upper, lane - GRID, lane))
    ky = signed(band * BAND + 2 * pair + upper.astype(jnp.int32))
    kz = lax.broadcasted_iota(jnp.int32, (DEPTH, 384), 0)
    keep = (
        (jnp.abs(kx) <= cut_ref[0]) & (jnp.abs(ky) <= cut_ref[1]) & (kz <= cut_ref[2])
    )
    waves = tuple(k.astype(f32) for k in (kx, ky, kz))
    square = waves[0] * waves[0] + waves[1] * waves[1] + waves[2] * waves[2]
    return waves, square, 1.0 / jnp.maximum(square, 1.0), keep


def project(field, waves, inverse, keep):
    normal = (waves[0] * field[0] + waves[1] * field[1] + waves[2] * field[2]) * inverse
    return [jnp.where(keep, field[a] - waves[a] * normal, 0.0) for a in range(3)]


MESH = pl.DeviceIdType.MESH
TURNS = ((1, 1), (3, 0), (2, 1), (0, 0), (1, 0), (3, 1), (2, 0), (0, 1))
OFFSETS = tuple(
    (dx, *TURNS[(k + 2 * j) % 8]) for k in range(8) for j, dx in enumerate((2, 1, 3, 0))
)


def is_live(band):
    return (band < 11) | (band >= 21)


def exchange_kernel(
    cut_ref, in_hbm, tx_hbm, ey_hbm, zt_hbm, zb_hbm, eyt_hbm, out_hbm, stats_hbm,
    held, tx_ref, ey_ref, zt_ref, zb_ref, eyt_ref, data, made, ready, arrived,
    rows_ref, strips, physical, back, closed, answer, top, total, stat,
    load_sems, send_sems, recv_sems, back_send, back_recv, stat_send, stat_recv, own_sems,
):
    px, pz = lax.axis_index("py"), lax.axis_index("pz")
    me = px * 8 + pz

    def peer(offset):
        x = lax.rem(px + offset[0], 4)
        y = lax.rem(pz // 2 + offset[1], 4)
        z = lax.rem(pz % 2 + offset[2], 2)
        return x, y * 2 + z

    def flat(device):
        return device[0] * 8 + device[1]

    def to(device):
        return {"py": device[0], "pz": device[1]}

    others = [(j, offset) for j, offset in enumerate(OFFSETS) if offset != (0, 0, 0)]
    self_slot = OFFSETS.index((0, 0, 0))

    loads = [
        pltpu.make_async_copy(
            in_hbm.at[:, :, pl.ds(0, DEPTH), pl.ds(384 * p, 384)], held.at[p], load_sems.at[p]
        )
        for p in range(3)
    ]
    tabled = [
        pltpu.make_async_copy(source, target, load_sems.at[3 + k])
        for k, (source, target) in enumerate(
            ((tx_hbm, tx_ref), (ey_hbm, ey_ref), (zt_hbm, zt_ref), (zb_hbm, zb_ref), (eyt_hbm, eyt_ref))
        )
    ]
    for copy in (loads[0], tabled[0], *loads[1:], *tabled[1:]):
        copy.start()

    barrier = pltpu.get_barrier_semaphore()
    for _, offset in others:
        pl.semaphore_signal(barrier, inc=1, device_id=to(peer(offset)), device_id_type=MESH)

    def first_copy(j, device, pair):
        rows = pl.ds(24 * pair, 24)
        return pltpu.make_async_remote_copy(
            src_ref=ready.at[j, :, rows, :],
            dst_ref=arrived.at[me, :, rows, :],
            send_sem=send_sems.at[j],
            recv_sem=recv_sems.at[me],
            device_id=to(device),
            device_id_type=MESH,
        )

    data[5 * DEPTH :, :] = jnp.zeros((384 - 5 * DEPTH, 512), f32)
    tabled[0].wait()

    for pair in range(3):
        loads[pair].wait()

        @pl.when(is_live(me))
        def _():
            waves, _, inverse, keep = pair_waves(pair, cut_ref)
            parts = []
            for c in range(2):
                sol = project([held[pair, c, a] for a in range(3)], waves, inverse, keep)
                curl_y = waves[2] * sol[0] - waves[0] * sol[2]
                curl_z = waves[0] * sol[1] - waves[1] * sol[0]
                parts.append((sol, (curl_y, curl_z)))
            fields = (
                parts[0][0] + [-parts[1][1][0], -parts[1][1][1]],
                parts[1][0] + [parts[0][1][0], parts[0][1][1]],
            )
            for odd in range(2):
                for c in range(2):
                    for f in range(5):
                        value = fields[c][f]
                        if odd:
                            value = pltpu.roll(value[:, 128:], 192, 1)
                        else:
                            value = value[:, :256]
                        data[f * DEPTH : (f + 1) * DEPTH, c * 256 : (c + 1) * 256] = value
                made[odd] = table_by_data(tx_ref, data[...], ((1,), (1,)))

        if pair == 0:
            pl.semaphore_wait(barrier, PARTS - 1)

        @pl.when(is_live(me))
        def _():
            for j, offset in enumerate(OFFSETS):
                d = flat(peer(offset))
                pieces = [
                    made[odd, pl.ds(pl.multiple_of(c * 256 + d * 8, 8), 8), :][:BAND]
                    for odd in range(2)
                    for c in range(2)
                ]
                piece = jnp.concatenate(pieces, axis=0)
                for third in range(3):
                    part = piece[:, third * 128 : (third + 1) * 128]
                    if j == self_slot:
                        arrived[me, third, 24 * pair : 24 * pair + 24, :] = part
                    else:
                        ready[j, third, 24 * pair : 24 * pair + 24, :] = part
                if j != self_slot:
                    first_copy(j, peer(offset), pair).start()

    rows_ref[...] = jnp.zeros_like(rows_ref)
    top[...] = jnp.zeros_like(top)
    total[...] = jnp.zeros_like(total)
    at = lax.broadcasted_iota(jnp.int32, (192, DEPTH), 0)
    band = at // 8
    band = jnp.where(band < 11, band, band + 10)
    ky = signed(band * BAND + at % 8).astype(f32)
    kz = lax.broadcasted_iota(jnp.int32, (192, DEPTH), 1).astype(f32)
    lane = lax.broadcasted_iota(jnp.int32, (192, 128), 1)
    for copy in tabled[1:]:
        copy.wait()

    def whole_first(slot, source):
        return pltpu.make_async_remote_copy(
            src_ref=ready.at[slot],
            dst_ref=arrived.at[source],
            send_sem=send_sems.at[slot],
            recv_sem=recv_sems.at[source],
            device_id=to((px, pz)),
            device_id_type=MESH,
        )

    for s in LIVE:

        @pl.when(s != me)
        def _():
            whole_first(0, s).wait_recv()

    def second_copy(j, device, pair):
        rows = pl.ds(24 * pair, 24)
        return pltpu.make_async_remote_copy(
            src_ref=answer.at[flat(device), :, rows, :],
            dst_ref=out_hbm.at[me, :, rows, :],
            send_sem=back_send.at[j],
            recv_sem=back_recv.at[me],
            device_id=to(device),
            device_id_type=MESH,
        )

    for pair in range(3):

        def one(odd, carry):
            x = 2 * pair + odd
            for c in range(2):
                for i, s in enumerate(LIVE):
                    for third in range(3):
                        rows_ref[
                            c * 192 + 8 * i : c * 192 + 8 * i + BAND,
                            third * 128 : (third + 1) * 128,
                        ] = arrived[s, third, pl.ds(c * BAND + x, BAND, stride=12), :]
            turned = [
                ky * rows_ref[c * 192 : (c + 1) * 192, 144:216]
                - kz * rows_ref[c * 192 : (c + 1) * 192, 72:144]
                for c in range(2)
            ]
            rows_ref[:192, 384 : 384 + DEPTH] = -turned[1]
            rows_ref[192:, 384 : 384 + DEPTH] = turned[0]
            strips[...] = table_by_data(ey_ref, rows_ref[...], ((1,), (0,)))
            for f in range(6):
                low = 72 * f if f < 5 else 384
                both = jnp.concatenate(
                    [strips[:192, low : low + 128], strips[192:, low : low + 128]], axis=1
                )
                physical[f] = data_by_table(both, zt_ref)
            u = [physical[f] for f in range(3)]
            w = [physical[5], physical[3], physical[4]]
            speed = jnp.abs(u[0]) + jnp.abs(u[1]) + jnp.abs(u[2])
            squares = u[0] * u[0] + u[1] * u[1] + u[2] * u[2]
            top[...] = jnp.maximum(top[...], jnp.max(speed.reshape(24, 8, GRID), axis=0))
            total[...] += jnp.sum(squares.reshape(24, 8, GRID), axis=0)
            q = [
                data_by_table(u[1] * w[2] - u[2] * w[1], zb_ref),
                data_by_table(u[2] * w[0] - u[0] * w[2], zb_ref),
                data_by_table(u[0] * w[1] - u[1] * w[0], zb_ref),
            ]
            for c in range(2):
                q0, q1, q2 = (part[:, c * 128 : (c + 1) * 128] for part in q)
                q1 = pltpu.roll(q1, 72, 1)
                back[c * 192 : (c + 1) * 192, :128] = jnp.where(lane < 72, q0, q1)
                back[c * 192 : (c + 1) * 192, 128:] = jnp.where(
                    lane < 16, q1, pltpu.roll(q2, 16, 1)
                )
            closed[odd] = table_by_data(eyt_ref, back[...], ((1,), (0,)))
            return carry

        lax.fori_loop(0, 2, one, 0)
        for i, s in enumerate(LIVE):
            piece = jnp.concatenate(
                [closed[0, 12 * i : 12 * i + 12, :], closed[1, 12 * i : 12 * i + 12, :]], axis=0
            )
            for half in range(2):
                answer[s, half, 24 * pair : 24 * pair + 24, :] = piece[
                    :, half * 128 : (half + 1) * 128
                ]
        for j, offset in others:
            device = peer(offset)

            @pl.when(is_live(flat(device)))
            def _():
                second_copy(j, device, pair).start()

    spot = lax.broadcasted_iota(jnp.int32, (8, 128), 1)
    stat[...] = jnp.where(spot == 0, jnp.max(top[...]), jnp.sum(total[...]))

    def stat_copy(j, device):
        return pltpu.make_async_remote_copy(
            src_ref=stat,
            dst_ref=stats_hbm.at[me],
            send_sem=stat_send.at[j],
            recv_sem=stat_recv.at[me],
            device_id=to(device),
            device_id_type=MESH,
        )

    own = (
        pltpu.make_async_copy(answer.at[me], out_hbm.at[me], own_sems.at[0]),
        pltpu.make_async_copy(stat, stats_hbm.at[me], own_sems.at[1]),
    )
    pl.when(is_live(me))(own[0].start)
    own[1].start()
    for j, offset in others:
        stat_copy(j, peer(offset)).start()
    pl.when(is_live(me))(own[0].wait)
    own[1].wait()

    def whole_second(j, source):
        return pltpu.make_async_remote_copy(
            src_ref=answer.at[0],
            dst_ref=out_hbm.at[source],
            send_sem=back_send.at[j],
            recv_sem=back_recv.at[source],
            device_id=to((px, pz)),
            device_id_type=MESH,
        )

    for j, offset in others:
        device = peer(offset)
        stat_copy(j, device).wait_send()
        pl.when(is_live(me))(whole_first(j, 0).wait_send)
        pl.when(is_live(flat(device)))(whole_second(j, 0).wait_send)
    for s in range(PARTS):

        @pl.when(s != me)
        def _():
            pltpu.make_async_remote_copy(
                src_ref=stat,
                dst_ref=stats_hbm.at[s],
                send_sem=stat_send.at[0],
                recv_sem=stat_recv.at[s],
                device_id=to((px, pz)),
                device_id_type=MESH,
            ).wait_recv()

        @pl.when((s != me) & is_live(me))
        def _():
            whole_second(0, s).wait_recv()


def close_kernel(cut_ref, dt_ref, power_ref, old_ref, in_ref, stats_ref, tx_ref, out_ref, cfl_ref, energy_ref, gathered, terms, spectra):
    gathered[...] = jnp.zeros_like(gathered)
    fastest = stats_ref[0]
    summed = stats_ref[0]
    for s in range(1, PARTS):
        fastest = jnp.maximum(fastest, stats_ref[s])
        summed = summed + stats_ref[s]
    fastest, summed = jnp.max(fastest[:, :1]), jnp.max(summed[:, 1:2])
    energy = 0.5 * summed * (1.0 / float(GRID**3))
    dt = dt_ref[0]
    cfl_ref[0] = dt * fastest * GRID * (1.0 / (2.0 * math.pi))
    energy_ref[0] = energy
    twice = jnp.maximum(jnp.full((DEPTH, 384), 2.0 * energy, f32), 0.5)
    forcing = power_ref[0] / twice

    out_ref[:, :, DEPTH:, :] = jnp.zeros((2, 3, 96 - DEPTH, 1152), f32)

    def step(pair, carry):
        window = pl.ds(pl.multiple_of(pair * 384, 128), 384)
        for odd in range(2):
            ky = 2 * pair + odd
            for c in range(2):
                for half in range(2):
                    for s in range(PARTS):
                        gathered[8 * s : 8 * s + BAND, :] = in_ref[
                            s, half, pl.ds(c * BAND + ky, BAND, stride=12), :
                        ]
                    terms[half * 128 : (half + 1) * 128, c * 256 : (c + 1) * 256] = gathered[...].T
            spectra[odd] = data_by_table(terms[: 3 * DEPTH, :], tx_ref)
        waves, square, inverse, keep = pair_waves(pair, cut_ref)
        for c in range(2):
            old = project([old_ref[c, a, :, window] for a in range(3)], waves, inverse, keep)
            new = []
            for a in range(3):
                rows = slice(a * DEPTH, (a + 1) * DEPTH)
                even = spectra[0, rows, c * 256 : (c + 1) * 256]
                odd = pltpu.roll(spectra[1, rows, c * 256 : (c + 1) * 256], 64, 1)
                new.append(
                    jnp.concatenate([even[:, :128], even[:, 128:] + odd[:, :128], odd[:, 128:]], axis=1)
                )
            forced = project(new, waves, inverse, keep)
            for a in range(3):
                out_ref[c, a, :DEPTH, window] = old[a] + dt * (
                    forced[a] + forcing * old[a] - viscosity * square * old[a]
                )
        return carry

    live = is_live(lax.axis_index("py") * lax.axis_size("pz") + lax.axis_index("pz"))

    @pl.when(live)
    def _():
        lax.fori_loop(0, 3, step, 0)

    @pl.when(jnp.logical_not(live))
    def _():
        out_ref[:, :, :DEPTH, :] = jnp.zeros((2, 3, DEPTH, 1152), f32)


SM = pl.BlockSpec(memory_space=pltpu.SMEM)
ANY = pl.BlockSpec(memory_space=pl.ANY)
VMEM_BYTES = 60 * 1024 * 1024


def on_device(velocity_hat, time_step, power, cutoffs):
    tx, ey, zt, zb, eyt = (jnp.asarray(t) for t in tables())
    shape = jax.ShapeDtypeStruct
    block = pl.BlockSpec((2, 3, DEPTH, 1152), lambda i: (0, 0, 0, 0))
    whole = lambda a: pl.BlockSpec(a.shape, lambda i: (0,) * a.ndim)
    dma = pltpu.SemaphoreType.DMA
    chunks, stats = pl.pallas_call(
        exchange_kernel,
        out_shape=(shape((PARTS, 2, 72, 128), f32), shape((PARTS, 8, 128), f32)),
        in_specs=[SM] + [ANY] * 6,
        out_specs=(ANY, ANY),
        scratch_shapes=[
            pltpu.VMEM((3, 2, 3, DEPTH, 384), f32),
            *(pltpu.VMEM(t.shape, bf16) for t in (tx, ey, zt, zb, eyt)),
            pltpu.VMEM((384, 512), f32),
            pltpu.VMEM((2, 512, 384), f32),
            pltpu.VMEM((PARTS, 3, 72, 128), f32),
            pltpu.VMEM((PARTS, 3, 72, 128), f32),
            pltpu.VMEM((384, 512), f32),
            pltpu.VMEM((384, 512), f32),
            pltpu.VMEM((6, GRID, GRID), f32),
            pltpu.VMEM((384, 256), f32),
            pltpu.VMEM((2, 272, 256), f32),
            pltpu.VMEM((PARTS, 2, 72, 128), f32),
            pltpu.VMEM((8, GRID), f32),
            pltpu.VMEM((8, GRID), f32),
            pltpu.VMEM((8, 128), f32),
            dma((8,)),
            *[dma((PARTS,))] * 6,
            dma((2,)),
        ],
        compiler_params=pltpu.CompilerParams(
            collective_id=0, has_side_effects=True, vmem_limit_bytes=VMEM_BYTES
        ),
    )(cutoffs, velocity_hat, tx, ey, zt, zb, eyt)
    return pl.pallas_call(
        close_kernel,
        grid=(1,),
        out_shape=(shape((2, 3, 96, 1152), f32), shape((1,), f32), shape((1,), f32)),
        in_specs=[SM, SM, SM, block, whole(chunks), whole(stats), whole(tx)],
        out_specs=(pl.BlockSpec((2, 3, 96, 1152), lambda i: (0, 0, 0, 0)), SM, SM),
        scratch_shapes=[
            pltpu.VMEM((256, 128), f32),
            pltpu.VMEM((256, 512), f32),
            pltpu.VMEM((2, 3 * DEPTH, 512), f32),
        ],
        compiler_params=pltpu.CompilerParams(vmem_limit_bytes=VMEM_BYTES),
    )(cutoffs, time_step, power, velocity_hat, chunks, stats, tx)


def solution(mesh):
    return jax.shard_map(
        on_device,
        mesh=mesh,
        in_specs=(P("member", None, None, ("py", "pz")), P("member"), P("member"), P("member")),
        out_specs=(P("member", None, None, ("py", "pz")), P("member"), P("member")),
        check_vma=False,
    )
```

```python
import functools
import math

import jax
import jax.numpy as jnp
import ml_dtypes
import numpy as np
from jax import lax
from jax.experimental import pallas as pl
from jax.experimental.pallas import tpu as pltpu
from jax.sharding import PartitionSpec as P

GRID = 192
PARTS = 32
BAND = 6
DEPTH = 72
LIVE = tuple(range(11)) + tuple(range(21, 32))
viscosity = 0.004
f32 = jnp.float32
bf16 = jnp.bfloat16


def halves(table):
    high = table.astype(ml_dtypes.bfloat16)
    low = (table - high.astype(np.float64)).astype(ml_dtypes.bfloat16)
    return np.stack([high, low])


def angle(rows, cols):
    turns = np.outer(rows, cols) % GRID
    return turns * (2.0 * math.pi / GRID)


@functools.lru_cache
def tables():
    n = GRID
    every = np.arange(n)
    phase = angle(every, every)
    tx = np.zeros((PARTS, 8, 768))
    cosine, sine = (f(phase).reshape(PARTS, BAND, n) for f in (np.cos, np.sin))
    for at, part in ((0, cosine), (256, sine), (512, -sine)):
        tx[:, :BAND, at : at + n] = part
    tx = tx.reshape(256, 768)
    cs = np.zeros((n, 512))
    cs[:, :n] = cosine.transpose(1, 0, 2).reshape(n, n)
    cs[:, 256 : 256 + n] = sine.transpose(1, 0, 2).reshape(n, n)
    ey = np.zeros((2 * n, 256))
    eyt = np.zeros((8 * len(LIVE), 2 * n))
    for at, band in enumerate(LIVE):
        phase = angle(every, band * BAND + np.arange(BAND))
        cols = slice(8 * band, 8 * band + BAND)
        ey[:n, cols], ey[n:, cols] = np.cos(phase), np.sin(phase)
        rows = slice(8 * at, 8 * at + BAND)
        eyt[rows, :n], eyt[rows, n:] = np.cos(phase).T, np.sin(phase).T
    factor = float(n) ** -1.5
    phase = angle(np.arange(65), every)
    cosine, sine = factor * np.cos(phase), factor * np.sin(phase)
    zt = np.zeros((256, n))
    weight = np.where(np.arange(64) == 0, 1.0, 2.0)[:, None]
    zt[:64], zt[64:128] = weight * cosine[:64], -weight * sine[:64]
    for f in range(6):
        zt[128 + 16 * f : 136 + 16 * f] = 2.0 * cosine[64]
        zt[136 + 16 * f : 144 + 16 * f] = -2.0 * sine[64]
    zb = np.zeros((n, 256))
    zb[:, :64], zb[:, 64:128] = cosine[:64].T, -sine[:64].T
    for x in range(BAND):
        for a in range(3):
            zb[:, 128 + 8 * x + 2 * a] = cosine[64]
            zb[:, 128 + 8 * x + 2 * a + 1] = -sine[64]
    return tuple(halves(t) for t in (tx, cs, ey, zt, zb, eyt))


def split(value):
    high = value.astype(bf16)
    return high, (value - high.astype(f32)).astype(bf16)


def table_by_data(table, data, dims):
    high, low = split(data)
    dot = functools.partial(
        lax.dot_general, dimension_numbers=(dims, ((), ())), preferred_element_type=f32
    )
    return dot(table[0], high) + dot(table[0], low) + dot(table[1], high)


def data_by_table(data, table):
    high, low = split(data)
    dot = functools.partial(jnp.dot, preferred_element_type=f32)
    return dot(high, table[0]) + dot(low, table[0]) + dot(high, table[1])


def signed(index):
    return jnp.where(index < GRID // 2, index, index - GRID)


def pair_waves(pair, cut_ref):
    band = lax.axis_index("py") * lax.axis_size("pz") + lax.axis_index("pz")
    lane = lax.broadcasted_iota(jnp.int32, (DEPTH, 384), 1)
    upper = lane >= GRID
    kx = signed(jnp.where(upper, lane - GRID, lane))
    ky = signed(band * BAND + 2 * pair + upper.astype(jnp.int32))
    kz = lax.broadcasted_iota(jnp.int32, (DEPTH, 384), 0)
    keep = (
        (jnp.abs(kx) <= cut_ref[0]) & (jnp.abs(ky) <= cut_ref[1]) & (kz <= cut_ref[2])
    )
    waves = tuple(k.astype(f32) for k in (kx, ky, kz))
    square = waves[0] * waves[0] + waves[1] * waves[1] + waves[2] * waves[2]
    return waves, square, 1.0 / jnp.maximum(square, 1.0), keep


def project(field, waves, inverse, keep):
    normal = (waves[0] * field[0] + waves[1] * field[1] + waves[2] * field[2]) * inverse
    return [jnp.where(keep, field[a] - waves[a] * normal, 0.0) for a in range(3)]


MESH = pl.DeviceIdType.MESH
TURNS = ((1, 1), (3, 0), (2, 1), (0, 0), (1, 0), (3, 1), (2, 0), (0, 1))
OFFSETS = tuple(
    (dx, *TURNS[(k + 2 * j) % 8]) for k in range(8) for j, dx in enumerate((2, 1, 3, 0))
)


SLOTS = 31
LAST = 12
GROUPS = ((0, 13), (13, 12), (25, 6))
STRIDE = 520


def slot_of(f, x):
    return f * BAND + x + (f >= 2) * 1


def is_live(band):
    return (band < 11) | (band >= 21)


def exchange_kernel(
    cut_ref, in_hbm, tx_hbm, ey_hbm, zt_hbm, zb_hbm, eyt_hbm, out_hbm, last_hbm, stats_hbm,
    held, tx_ref, ey_ref, zt_ref, zb_ref, eyt_ref, data, data64, wide64, made, ready, arrived,
    turns, strips64, physical, back, back64, closed, closed64, top, total, stat,
    load_sems, send_sems, recv_sems, back_send, back_recv, last_send, last_recv,
    stat_send, stat_recv, own_sems,
):
    px, pz = lax.axis_index("py"), lax.axis_index("pz")
    me = px * 8 + pz
    live = is_live(me)

    def peer(offset):
        x = lax.rem(px + offset[0], 4)
        y = lax.rem(pz // 2 + offset[1], 4)
        z = lax.rem(pz % 2 + offset[2], 2)
        return x, y * 2 + z

    def flat(device):
        return device[0] * 8 + device[1]

    def place(band):
        return jnp.where(band < 11, band, band - 10)

    def remote(source, target, send, recv, device):
        return pltpu.make_async_remote_copy(
            src_ref=source,
            dst_ref=target,
            send_sem=send,
            recv_sem=recv,
            device_id={"py": device[0], "pz": device[1]},
            device_id_type=MESH,
        )

    others = [(j, offset) for j, offset in enumerate(OFFSETS) if offset != (0, 0, 0)]

    loads = [
        pltpu.make_async_copy(
            in_hbm.at[:, :, pl.ds(0, DEPTH), pl.ds(384 * p, 384)], held.at[p], load_sems.at[p]
        )
        for p in range(3)
    ]
    tabled = [
        pltpu.make_async_copy(source, target, load_sems.at[3 + k])
        for k, (source, target) in enumerate(
            ((ey_hbm, ey_ref), (zt_hbm, zt_ref), (zb_hbm, zb_ref), (eyt_hbm, eyt_ref))
        )
    ]
    quarters = [
        pltpu.make_async_copy(
            tx_hbm.at[:, :, pl.ds(low, 256)],
            tx_ref.at[:, pl.ds(256 * (k // 2), 256), pl.ds(256 * (k % 2), 256)],
            load_sems.at[7 + k],
        )
        for k, low in enumerate((0, 512, 256, 0))
    ]
    for copy in (*loads, *quarters, *tabled):
        copy.start()

    def clear(slot, carry):
        arrived[slot] = jnp.zeros((PARTS, 8, 128), f32)
        return carry

    lax.fori_loop(0, SLOTS, clear, 0)
    barrier = pltpu.get_barrier_semaphore()
    for _, offset in others:
        device = peer(offset)
        pl.semaphore_signal(
            barrier, inc=1, device_id={"py": device[0], "pz": device[1]}, device_id_type=MESH
        )

    def first_copy(group, device):
        low, count = GROUPS[group]
        return remote(
            ready.at[flat(device), pl.ds(low, count), pl.ds(0, BAND), :],
            arrived.at[pl.ds(low, count), me, pl.ds(0, BAND), :],
            send_sems.at[flat(device)],
            recv_sems.at[group, me],
            device,
        )

    lane8 = lax.broadcasted_iota(jnp.int32, (8, 128), 1)
    low6 = lax.broadcasted_iota(jnp.int32, (BAND, 128), 1) < 64

    data64[...] = jnp.zeros_like(data64)
    for pair in range(3):
        loads[pair].wait()

        @pl.when(live)
        def _():
            waves, _, inverse, keep = pair_waves(pair, cut_ref)
            parts = []
            for c in range(2):
                sol = project([held[pair, c, a] for a in range(3)], waves, inverse, keep)
                curl_y = waves[2] * sol[0] - waves[0] * sol[2]
                curl_z = waves[0] * sol[1] - waves[1] * sol[0]
                parts.append((sol, (curl_y, curl_z)))
            fields = []
            for c in range(2):
                turn = parts[1 - c][1]
                if c == 0:
                    turn = (-turn[0], -turn[1])
                sol = parts[c][0]
                fields.append((sol[1], sol[2], sol[0], turn[0], turn[1]))
            for odd in range(2):
                ky = 2 * pair + odd
                for c in range(2):
                    cols = slice(c * 256, (c + 1) * 256)
                    for f in range(5):
                        value = fields[c][f]
                        if odd:
                            value = pltpu.roll(value[:, 128:], 192, 1)
                        else:
                            value = value[:, :256]
                        low = 768 * (f // 2) + 128 * ky + 64 * (f % 2)
                        data[low : low + 64, cols] = value[:64]
                        if f == 4:
                            data[low + 64 : low + 128, cols] = value[:64]
                        data64[8 * f + ky : 8 * f + ky + 1, cols] = value[64:65]

    for copy in quarters:
        copy.wait()

    @pl.when(live)
    def _():
        high, low = split(data64[...])
        dot = functools.partial(
            lax.dot_general,
            dimension_numbers=(((1,), (1,)), ((), ())),
            preferred_element_type=f32,
        )
        wide = dot(high, tx_ref[0]) + dot(low, tx_ref[0]) + dot(high, tx_ref[1])
        for k in range(4):
            wide64[k] = wide[:, 128 * k : 128 * (k + 1)]
        for d in range(PARTS):
            tile = jnp.zeros((8, 128), f32)
            for f in range(5):
                for c in range(2):
                    spot = 16 * f + 8 * c
                    part = wide64[2 * c + d // 16, 8 * f : 8 * f + 8, :]
                    shift = (spot - 8 * (d % 16)) % 128
                    if shift:
                        part = pltpu.roll(part, shift, 1)
                    tile = jnp.where((lane8 >= spot) & (lane8 < spot + 8), part, tile)
            ready[d, LAST] = tile

    for group in range(3):

        @pl.when(live)
        def _():
            for pair in range(3):
                low = 768 * group + 256 * pair
                wide = table_by_data(tx_ref, data[low : low + 256, :], ((1,), (1,)))
                for odd in range(2):
                    at = (2 * pair + odd) * STRIDE
                    made[at : at + 512, :] = wide[:, 128 * odd : 128 * (odd + 1)]

        if group == 0:
            pl.semaphore_wait(barrier, PARTS - 1)

        @pl.when(live)
        def _():
            def fill(d, write):
                for x in range(BAND):
                    re, im = (
                        made[pl.ds(256 * c + 8 * d + x, BAND, stride=STRIDE), :] for c in range(2)
                    )
                    if group == 2:
                        write(4, x, jnp.where(low6, re, im))
                    else:
                        write(2 * group, x, jnp.where(low6, re, pltpu.roll(im, 64, 1)))
                        write(2 * group + 1, x, jnp.where(low6, pltpu.roll(re, 64, 1), im))

            for j, offset in others:
                device = peer(offset)
                d = flat(device)

                def write(f, x, value):
                    ready[d, slot_of(f, x), :BAND, :] = value

                fill(d, write)
                first_copy(group, device).start()

            def keep_own(f, x, value):
                arrived[slot_of(f, x), me, :BAND, :] = value

            fill(me, keep_own)
            if group == 0:
                arrived[LAST, me] = ready[me, LAST]

    top[...] = jnp.zeros_like(top)
    total[...] = jnp.zeros_like(total)
    for copy in tabled:
        copy.wait()

    row = lax.broadcasted_iota(jnp.int32, (256, 128), 0)
    col = lax.broadcasted_iota(jnp.int32, (256, 128), 1)
    ky = signed(row // 8 * BAND + row % 8).astype(f32)
    kz = (col % 64).astype(f32)
    sign = jnp.where(col < 64, -1.0, 1.0)
    lane = lax.broadcasted_iota(jnp.int32, (GRID, 128), 1)
    lower = lane < 64

    def await_group(group):
        low, count = GROUPS[group]
        for s in LIVE:

            @pl.when(s != me)
            def _():
                remote(
                    ready.at[0, pl.ds(low, count), pl.ds(0, BAND), :],
                    arrived.at[pl.ds(low, count), s, pl.ds(0, BAND), :],
                    send_sems.at[0],
                    recv_sems.at[group, s],
                    (px, pz),
                ).wait_recv()

    def to_grid(f, pair):
        wide = table_by_data(ey_ref, turns[...], ((1,), (0,)))
        for odd in range(2):
            x = 2 * pair + odd
            cosine = wide[:GRID, 128 * odd : 128 * (odd + 1)]
            sine = pltpu.roll(wide[GRID:, 128 * odd : 128 * (odd + 1)], 64, 1)
            near = cosine + jnp.where(lower, -sine, sine)
            mine = (lane == 16 * f + x) | (lane == 16 * f + 8 + x)
            far = jnp.where(mine, strips64[...], 0.0)
            physical[f, x] = data_by_table(jnp.concatenate([near, far], axis=1), zt_ref)

    def plain(first, last):
        def step(k, carry):
            f, pair = k // 3, k % 3
            slot = slot_of(f, 2 * pair)
            for odd in range(2):
                turns[:, 128 * odd : 128 * (odd + 1)] = arrived[slot + odd].reshape(256, 128)
            to_grid(f, pair)
            return carry

        lax.fori_loop(3 * first, 3 * last, step, 0)

    def turned(pair, carry):
        for odd in range(2):
            x = 2 * pair + odd
            d = ky * arrived[BAND + x].reshape(256, 128) - kz * arrived[x].reshape(256, 128)
            turns[:, 128 * odd : 128 * (odd + 1)] = sign * pltpu.roll(d, 64, 1)
        to_grid(5, pair)
        return carry

    await_group(0)
    tile = arrived[LAST].reshape(256, 128)
    d = ky * pltpu.roll(tile, 64, 1) - 64.0 * pltpu.roll(tile, 80, 1)
    d = jnp.where(col < 88, -pltpu.roll(d, 120, 1), pltpu.roll(d, 8, 1))
    tile = jnp.where((col >= 80) & (col < 96), d, tile)
    wide = table_by_data(ey_ref, tile, ((1,), (0,)))
    strips64[...] = wide[:GRID] + jnp.where(
        lane // 8 % 2 == 0, -pltpu.roll(wide[GRID:], 120, 1), pltpu.roll(wide[GRID:], 8, 1)
    )
    plain(0, 2)
    lax.fori_loop(0, 3, turned, 0)
    await_group(1)
    plain(2, 4)
    await_group(2)
    plain(4, 5)

    back64[...] = jnp.zeros_like(back64)

    def plane(x, carry):
        u = [physical[f, x] for f in (2, 0, 1)]
        w = [physical[f, x] for f in (5, 3, 4)]
        speed = jnp.abs(u[0]) + jnp.abs(u[1]) + jnp.abs(u[2])
        squares = u[0] * u[0] + u[1] * u[1] + u[2] * u[2]
        top[...] = jnp.maximum(top[...], jnp.max(speed.reshape(24, 8, GRID), axis=0))
        total[...] += jnp.sum(squares.reshape(24, 8, GRID), axis=0)
        q = []
        for a in range(3):
            b, c = (a + 1) % 3, (a + 2) % 3
            q.append(data_by_table(u[b] * w[c] - u[c] * w[b], zb_ref))
            near = q[a][:, :128]
            far = pltpu.roll(near, 64, 1)
            back[:GRID, 128 * a : 128 * (a + 1)] = near
            back[GRID:, 128 * a : 128 * (a + 1)] = jnp.where(lower, far, -far)
        way = lane % 8 // 2
        chosen = jnp.where(way == 0, q[0][:, 128:], jnp.where(way == 1, q[1][:, 128:], q[2][:, 128:]))
        back64[:GRID] = jnp.where(lane // 8 == x, chosen, back64[:GRID])
        wide = table_by_data(eyt_ref, back[...], ((1,), (0,)))
        for a in range(3):
            closed[a, x] = wide[:, 128 * a : 128 * (a + 1)].reshape(len(LIVE), 8, 128)
        for j, offset in others:
            device = peer(offset)

            @pl.when(is_live(flat(device)))
            def _():
                remote(
                    closed.at[:, x, place(flat(device)), pl.ds(0, BAND), :],
                    out_hbm.at[:, x, me, pl.ds(0, BAND), :],
                    back_send.at[flat(device)],
                    back_recv.at[me],
                    device,
                ).start()

        return carry

    lax.fori_loop(0, BAND, plane, 0)

    q = back64[:GRID]
    back64[GRID:] = jnp.where(lane % 2 == 0, pltpu.roll(q, 127, 1), -pltpu.roll(q, 1, 1))
    wide = table_by_data(eyt_ref, back64[...], ((1,), (0,)))
    closed64[...] = wide.reshape(len(LIVE), 8, 128)
    stat[...] = jnp.where(lane8 == 0, jnp.max(top[...]), jnp.sum(total[...]))

    def stat_copy(device):
        return remote(stat, stats_hbm.at[me], stat_send.at[flat(device)], stat_recv.at[me], device)

    for j, offset in others:
        device = peer(offset)
        stat_copy(device).start()

        @pl.when(is_live(flat(device)))
        def _():
            remote(
                closed64.at[place(flat(device))],
                last_hbm.at[me],
                last_send.at[flat(device)],
                last_recv.at[me],
                device,
            ).start()

    own = (
        pltpu.make_async_copy(
            closed.at[:, :, place(me), pl.ds(0, BAND), :],
            out_hbm.at[:, :, me, pl.ds(0, BAND), :],
            own_sems.at[0],
        ),
        pltpu.make_async_copy(closed64.at[place(me)], last_hbm.at[me], own_sems.at[1]),
    )
    stat_own = pltpu.make_async_copy(stat, stats_hbm.at[me], own_sems.at[2])
    stat_own.start()

    @pl.when(live)
    def _():
        own[0].start()
        own[1].start()
        own[0].wait()
        own[1].wait()

    stat_own.wait()

    def whole_back(source, send):
        return remote(
            closed.at[:, :, 0, pl.ds(0, BAND), :],
            out_hbm.at[:, :, source, pl.ds(0, BAND), :],
            back_send.at[send],
            back_recv.at[source],
            (px, pz),
        )

    def whole_last(source, send):
        return remote(
            closed64.at[0], last_hbm.at[source], last_send.at[send], last_recv.at[source], (px, pz)
        )

    for j, offset in others:
        device = peer(offset)
        d = flat(device)
        stat_copy(device).wait_send()

        @pl.when(live)
        def _():
            remote(
                ready.at[0, :, pl.ds(0, BAND), :],
                arrived.at[:, 0, pl.ds(0, BAND), :],
                send_sems.at[d],
                recv_sems.at[0, 0],
                (px, pz),
            ).wait_send()

        @pl.when(is_live(d))
        def _():
            whole_back(0, d).wait_send()
            whole_last(0, d).wait_send()

    for s in range(PARTS):

        @pl.when(s != me)
        def _():
            remote(stat, stats_hbm.at[s], stat_send.at[0], stat_recv.at[s], (px, pz)).wait_recv()

        @pl.when((s != me) & live)
        def _():
            whole_back(s, 0).wait_recv()
            whole_last(s, 0).wait_recv()


def close_kernel(
    cut_ref, dt_ref, power_ref, old_ref, in_ref, last_ref, stats_ref, cs_ref,
    out_ref, cfl_ref, energy_ref, terms, spectra,
):
    fastest = stats_ref[0]
    summed = stats_ref[0]
    for s in range(1, PARTS):
        fastest = jnp.maximum(fastest, stats_ref[s])
        summed = summed + stats_ref[s]
    fastest, summed = jnp.max(fastest[:, :1]), jnp.max(summed[:, 1:2])
    energy = 0.5 * summed * (1.0 / float(GRID**3))
    dt = dt_ref[0]
    cfl_ref[0] = dt * fastest * GRID * (1.0 / (2.0 * math.pi))
    energy_ref[0] = energy
    twice = jnp.maximum(jnp.full((DEPTH, 384), 2.0 * energy, f32), 0.5)
    forcing = power_ref[0] / twice
    eighth = lax.broadcasted_iota(jnp.int32, (PARTS, 128), 1) // 8

    out_ref[:, :, DEPTH:, :] = jnp.zeros((2, 3, 96 - DEPTH, 1152), f32)

    def step(pair, carry):
        window = pl.ds(pl.multiple_of(pair * 384, 128), 384)
        for odd in range(2):
            ky = 2 * pair + odd
            for a in range(3):
                terms[128 * a : 128 * (a + 1), :] = in_ref[a, pl.ds(ky, GRID, stride=8), :].T
            last = last_ref[pl.ds(ky, PARTS, stride=8), :]
            apart = jnp.concatenate(
                [jnp.where(eighth == x, last, 0.0) for x in range(BAND)], axis=0
            )
            terms[384:432, :] = apart.T[:48]
            spectra[odd] = data_by_table(terms[...], cs_ref)
        waves, square, inverse, keep = pair_waves(pair, cut_ref)

        def of_pair(a, c):
            halves = []
            for odd in range(2):
                re, im = (
                    spectra[odd, 128 * a + 64 * k : 128 * a + 64 * (k + 1), :] for k in range(2)
                )
                last = spectra[odd, 384:392, :]
                for x in range(1, BAND):
                    last = last + spectra[odd, 384 + 8 * x : 392 + 8 * x, :]
                re64, im64 = last[2 * a : 2 * a + 1], last[2 * a + 1 : 2 * a + 2]
                if c == 0:
                    value, value64 = (r[:, :256] + i[:, 256:] for r, i in ((re, im), (re64, im64)))
                else:
                    value, value64 = (i[:, :256] - r[:, 256:] for r, i in ((re, im), (re64, im64)))
                value = jnp.concatenate([value, value64, jnp.zeros((7, 256), f32)], axis=0)
                halves.append(pltpu.roll(value, 64, 1) if odd else value)
            even, odd = halves
            return jnp.concatenate([even[:, :128], even[:, 128:] + odd[:, :128], odd[:, 128:]], axis=1)

        for c in range(2):
            old = project([old_ref[c, a, :, window] for a in range(3)], waves, inverse, keep)
            forced = project([of_pair(a, c) for a in range(3)], waves, inverse, keep)
            for a in range(3):
                out_ref[c, a, :DEPTH, window] = old[a] + dt * (
                    forced[a] + forcing * old[a] - viscosity * square * old[a]
                )
        return carry

    live = is_live(lax.axis_index("py") * lax.axis_size("pz") + lax.axis_index("pz"))

    @pl.when(live)
    def _():
        lax.fori_loop(0, 3, step, 0)

    @pl.when(jnp.logical_not(live))
    def _():
        out_ref[:, :, :DEPTH, :] = jnp.zeros((2, 3, DEPTH, 1152), f32)


SM = pl.BlockSpec(memory_space=pltpu.SMEM)
ANY = pl.BlockSpec(memory_space=pl.ANY)
VMEM_BYTES = 60 * 1024 * 1024


def on_device(velocity_hat, time_step, power, cutoffs):
    tx, cs, ey, zt, zb, eyt = (jnp.asarray(t) for t in tables())
    shape = jax.ShapeDtypeStruct
    block = pl.BlockSpec((2, 3, DEPTH, 1152), lambda i: (0, 0, 0, 0))
    whole = lambda a: pl.BlockSpec(a.shape, lambda i: (0,) * a.ndim)
    dma = pltpu.SemaphoreType.DMA
    chunks, last, stats = pl.pallas_call(
        exchange_kernel,
        out_shape=(
            shape((3, BAND, PARTS, 8, 128), f32),
            shape((PARTS, 8, 128), f32),
            shape((PARTS, 8, 128), f32),
        ),
        in_specs=[SM] + [ANY] * 6,
        out_specs=(ANY, ANY, ANY),
        scratch_shapes=[
            pltpu.VMEM((3, 2, 3, DEPTH, 384), f32),
            pltpu.VMEM((2, 512, 512), bf16),
            *(pltpu.VMEM(t.shape, bf16) for t in (ey, zt, zb, eyt)),
            pltpu.VMEM((2304, 512), f32),
            pltpu.VMEM((40, 512), f32),
            pltpu.VMEM((4, 40, 128), f32),
            pltpu.VMEM((BAND * STRIDE, 128), f32),
            pltpu.VMEM((PARTS, SLOTS, 8, 128), f32),
            pltpu.VMEM((SLOTS, PARTS, 8, 128), f32),
            pltpu.VMEM((256, 256), f32),
            pltpu.VMEM((GRID, 128), f32),
            pltpu.VMEM((6, BAND, GRID, GRID), f32),
            pltpu.VMEM((2 * GRID, 384), f32),
            pltpu.VMEM((2 * GRID, 128), f32),
            pltpu.VMEM((3, BAND, len(LIVE), 8, 128), f32),
            pltpu.VMEM((len(LIVE), 8, 128), f32),
            pltpu.VMEM((8, GRID), f32),
            pltpu.VMEM((8, GRID), f32),
            pltpu.VMEM((8, 128), f32),
            dma((11,)),
            dma((PARTS,)),
            dma((3, PARTS)),
            *[dma((PARTS,))] * 6,
            dma((3,)),
        ],
        compiler_params=pltpu.CompilerParams(
            collective_id=0, has_side_effects=True, vmem_limit_bytes=VMEM_BYTES
        ),
    )(cutoffs, velocity_hat, tx, ey, zt, zb, eyt)
    chunks = chunks.reshape(3, BAND * PARTS * 8, 128)
    last = last.reshape(PARTS * 8, 128)
    return pl.pallas_call(
        close_kernel,
        grid=(1,),
        out_shape=(shape((2, 3, 96, 1152), f32), shape((1,), f32), shape((1,), f32)),
        in_specs=[SM, SM, SM, block, whole(chunks), whole(last), whole(stats), whole(cs)],
        out_specs=(pl.BlockSpec((2, 3, 96, 1152), lambda i: (0, 0, 0, 0)), SM, SM),
        scratch_shapes=[pltpu.VMEM((432, GRID), f32), pltpu.VMEM((2, 432, 512), f32)],
        compiler_params=pltpu.CompilerParams(vmem_limit_bytes=VMEM_BYTES),
    )(cutoffs, time_step, power, velocity_hat, chunks, last, stats, cs)


def solution(mesh):
    return jax.shard_map(
        on_device,
        mesh=mesh,
        in_specs=(P("member", None, None, ("py", "pz")), P("member"), P("member"), P("member")),
        out_specs=(P("member", None, None, ("py", "pz")), P("member"), P("member")),
        check_vma=False,
    )
```

```python
import functools
import math

import jax
import jax.numpy as jnp
import ml_dtypes
import numpy as np
from jax import lax
from jax.experimental import pallas as pl
from jax.experimental.pallas import tpu as pltpu
from jax.sharding import PartitionSpec as P

GRID = 192
PARTS = 32
BAND = 6
DEPTH = 72
LIVE = tuple(range(11)) + tuple(range(21, 32))
viscosity = 0.004
f32 = jnp.float32
bf16 = jnp.bfloat16


def halves(table):
    high = table.astype(ml_dtypes.bfloat16)
    low = (table - high.astype(np.float64)).astype(ml_dtypes.bfloat16)
    return np.stack([high, low])


def angle(rows, cols):
    turns = np.outer(rows, cols) % GRID
    return turns * (2.0 * math.pi / GRID)


@functools.lru_cache
def tables():
    n = GRID
    every = np.arange(n)
    phase = angle(every, every)
    tx = np.zeros((PARTS, 8, 768))
    cosine, sine = (f(phase).reshape(PARTS, BAND, n) for f in (np.cos, np.sin))
    for at, part in ((0, cosine), (256, sine), (512, -sine)):
        tx[:, :BAND, at : at + n] = part
    tx = tx.reshape(256, 768)
    cs = np.zeros((n, 512))
    cs[:, :n] = cosine.transpose(1, 0, 2).reshape(n, n)
    cs[:, 256 : 256 + n] = sine.transpose(1, 0, 2).reshape(n, n)
    ey = np.zeros((2 * n, 256))
    eyt = np.zeros((8 * len(LIVE), 2 * n))
    for at, band in enumerate(LIVE):
        phase = angle(every, band * BAND + np.arange(BAND))
        cols = slice(8 * band, 8 * band + BAND)
        ey[:n, cols], ey[n:, cols] = np.cos(phase), np.sin(phase)
        rows = slice(8 * at, 8 * at + BAND)
        eyt[rows, :n], eyt[rows, n:] = np.cos(phase).T, np.sin(phase).T
    factor = float(n) ** -1.5
    phase = angle(np.arange(65), every)
    cosine, sine = factor * np.cos(phase), factor * np.sin(phase)
    zt = np.zeros((256, n))
    weight = np.where(np.arange(64) == 0, 1.0, 2.0)[:, None]
    zt[:64], zt[64:128] = weight * cosine[:64], -weight * sine[:64]
    for f in range(6):
        zt[128 + 16 * f : 136 + 16 * f] = 2.0 * cosine[64]
        zt[136 + 16 * f : 144 + 16 * f] = -2.0 * sine[64]
    zb = np.zeros((n, 256))
    zb[:, :64], zb[:, 64:128] = cosine[:64].T, -sine[:64].T
    for x in range(BAND):
        for a in range(3):
            zb[:, 128 + 8 * x + 2 * a] = cosine[64]
            zb[:, 128 + 8 * x + 2 * a + 1] = -sine[64]
    return tuple(halves(t) for t in (tx, cs, ey, zt, zb, eyt))


def split(value):
    high = value.astype(bf16)
    return high, (value - high.astype(f32)).astype(bf16)


def table_by_data(table, data, dims):
    high, low = split(data)
    dot = functools.partial(
        lax.dot_general, dimension_numbers=(dims, ((), ())), preferred_element_type=f32
    )
    return dot(table[0], high) + dot(table[0], low) + dot(table[1], high)


def data_by_table(data, table):
    high, low = split(data)
    dot = functools.partial(jnp.dot, preferred_element_type=f32)
    return dot(high, table[0]) + dot(low, table[0]) + dot(high, table[1])


def signed(index):
    return jnp.where(index < GRID // 2, index, index - GRID)


def pair_waves(pair, cut_ref):
    band = lax.axis_index("py") * lax.axis_size("pz") + lax.axis_index("pz")
    lane = lax.broadcasted_iota(jnp.int32, (DEPTH, 384), 1)
    upper = lane >= GRID
    kx = signed(jnp.where(upper, lane - GRID, lane))
    ky = signed(band * BAND + 2 * pair + upper.astype(jnp.int32))
    kz = lax.broadcasted_iota(jnp.int32, (DEPTH, 384), 0)
    keep = (
        (jnp.abs(kx) <= cut_ref[0]) & (jnp.abs(ky) <= cut_ref[1]) & (kz <= cut_ref[2])
    )
    waves = tuple(k.astype(f32) for k in (kx, ky, kz))
    square = waves[0] * waves[0] + waves[1] * waves[1] + waves[2] * waves[2]
    return waves, square, 1.0 / jnp.maximum(square, 1.0), keep


def project(field, waves, inverse, keep):
    normal = (waves[0] * field[0] + waves[1] * field[1] + waves[2] * field[2]) * inverse
    return [jnp.where(keep, field[a] - waves[a] * normal, 0.0) for a in range(3)]


MESH = pl.DeviceIdType.MESH
TURNS = ((1, 1), (3, 0), (2, 1), (0, 0), (1, 0), (3, 1), (2, 0), (0, 1))
OFFSETS = tuple(
    (dx, *TURNS[(k + 2 * j) % 8]) for k in range(8) for j, dx in enumerate((2, 1, 3, 0))
)


SLOTS = 31
STRIDE = 520


def slot_of(f, x):
    return 1 + 5 * x + f


def is_live(band):
    return (band < 11) | (band >= 21)


def exchange_kernel(
    cut_ref, in_hbm, tx_hbm, ey_hbm, zt_hbm, zb_hbm, eyt_hbm, out_hbm, last_hbm, stats_hbm,
    held, tx_ref, ey_ref, zt_ref, zb_ref, eyt_ref, data, data64, wide64, made, ready, arrived,
    turns, strips64, physical, back, back64, closed, closed64, top, total, stat,
    load_sems, send_sems, recv_sems, send64, recv64, back_send, back_recv, last_send, last_recv,
    stat_send, stat_recv, own_sems,
):
    px, pz = lax.axis_index("py"), lax.axis_index("pz")
    me = px * 8 + pz
    live = is_live(me)

    def peer(offset):
        x = lax.rem(px + offset[0], 4)
        y = lax.rem(pz // 2 + offset[1], 4)
        z = lax.rem(pz % 2 + offset[2], 2)
        return x, y * 2 + z

    def flat(device):
        return device[0] * 8 + device[1]

    def place(band):
        return jnp.where(band < 11, band, band - 10)

    def remote(source, target, send, recv, device):
        return pltpu.make_async_remote_copy(
            src_ref=source,
            dst_ref=target,
            send_sem=send,
            recv_sem=recv,
            device_id={"py": device[0], "pz": device[1]},
            device_id_type=MESH,
        )

    others = [(j, offset) for j, offset in enumerate(OFFSETS) if offset != (0, 0, 0)]

    loads = [
        pltpu.make_async_copy(
            in_hbm.at[:, :, pl.ds(0, DEPTH), pl.ds(384 * p, 384)], held.at[p], load_sems.at[p]
        )
        for p in range(3)
    ]
    tabled = [
        pltpu.make_async_copy(source, target, load_sems.at[3 + k])
        for k, (source, target) in enumerate(
            ((ey_hbm, ey_ref), (zt_hbm, zt_ref), (zb_hbm, zb_ref), (eyt_hbm, eyt_ref))
        )
    ]
    quarters = [
        pltpu.make_async_copy(
            tx_hbm.at[:, :, pl.ds(low, 256)],
            tx_ref.at[:, pl.ds(256 * (k // 2), 256), pl.ds(256 * (k % 2), 256)],
            load_sems.at[7 + k],
        )
        for k, low in enumerate((0, 512, 256, 0))
    ]
    for copy in (*loads, *quarters, *tabled):
        copy.start()

    def clear(slot, carry):
        arrived[slot] = jnp.zeros((PARTS, 8, 128), f32)
        return carry

    lax.fori_loop(0, SLOTS, clear, 0)
    barrier = pltpu.get_barrier_semaphore()
    for _, offset in others:
        device = peer(offset)
        pl.semaphore_signal(
            barrier, inc=1, device_id={"py": device[0], "pz": device[1]}, device_id_type=MESH
        )

    def first_copy(x, device):
        slots = pl.ds(1 + 5 * x, 5)
        return remote(
            ready.at[flat(device), slots, pl.ds(0, BAND), :],
            arrived.at[slots, me, pl.ds(0, BAND), :],
            send_sems.at[flat(device)],
            recv_sems.at[x, me],
            device,
        )

    lane8 = lax.broadcasted_iota(jnp.int32, (8, 128), 1)
    low6 = lax.broadcasted_iota(jnp.int32, (BAND, 128), 1) < 64

    data64[...] = jnp.zeros_like(data64)
    for pair in range(3):
        loads[pair].wait()

        @pl.when(live)
        def _():
            waves, _, inverse, keep = pair_waves(pair, cut_ref)
            parts = []
            for c in range(2):
                sol = project([held[pair, c, a] for a in range(3)], waves, inverse, keep)
                curl_y = waves[2] * sol[0] - waves[0] * sol[2]
                curl_z = waves[0] * sol[1] - waves[1] * sol[0]
                parts.append((sol, (curl_y, curl_z)))
            fields = []
            for c in range(2):
                turn = parts[1 - c][1]
                if c == 0:
                    turn = (-turn[0], -turn[1])
                sol = parts[c][0]
                fields.append((sol[1], sol[2], sol[0], turn[0], turn[1]))
            for odd in range(2):
                ky = 2 * pair + odd
                for c in range(2):
                    cols = slice(c * 256, (c + 1) * 256)
                    for f in range(5):
                        value = fields[c][f]
                        if odd:
                            value = pltpu.roll(value[:, 128:], 192, 1)
                        else:
                            value = value[:, :256]
                        low = 768 * (f // 2) + 128 * ky + 64 * (f % 2)
                        data[low : low + 64, cols] = value[:64]
                        if f == 4:
                            data[low + 64 : low + 128, cols] = value[:64]
                        data64[8 * f + ky : 8 * f + ky + 1, cols] = value[64:65]

    for copy in quarters:
        copy.wait()

    @pl.when(live)
    def _():
        high, low = split(data64[...])
        dot = functools.partial(
            lax.dot_general,
            dimension_numbers=(((1,), (1,)), ((), ())),
            preferred_element_type=f32,
        )
        wide = dot(high, tx_ref[0]) + dot(low, tx_ref[0]) + dot(high, tx_ref[1])
        for k in range(4):
            wide64[k] = wide[:, 128 * k : 128 * (k + 1)]
        for d in range(PARTS):
            tile = jnp.zeros((8, 128), f32)
            for f in range(5):
                for c in range(2):
                    spot = 16 * f + 8 * c
                    part = wide64[2 * c + d // 16, 8 * f : 8 * f + 8, :]
                    shift = (spot - 8 * (d % 16)) % 128
                    if shift:
                        part = pltpu.roll(part, shift, 1)
                    tile = jnp.where((lane8 >= spot) & (lane8 < spot + 8), part, tile)
            ready[d, 0] = tile

        for group in range(3):
            for pair in range(3):
                low = 768 * group + 256 * pair
                wide = table_by_data(tx_ref, data[low : low + 256, :], ((1,), (1,)))
                for odd in range(2):
                    at = (2 * pair + odd) * STRIDE
                    made[group, at : at + 512, :] = wide[:, 128 * odd : 128 * (odd + 1)]

    pl.semaphore_wait(barrier, PARTS - 1)

    @pl.when(live)
    def _():
        for j, offset in others:
            device = peer(offset)
            remote(
                ready.at[flat(device), 0],
                arrived.at[0, me],
                send64.at[flat(device)],
                recv64.at[me],
                device,
            ).start()
        arrived[0, me] = ready[me, 0]

        def spread(x, carry):
            def fill(d, write):
                for group in range(3):
                    re, im = (
                        made[group, pl.ds(256 * c + 8 * d + x, BAND, stride=STRIDE), :]
                        for c in range(2)
                    )
                    if group == 2:
                        write(4, jnp.where(low6, re, im))
                    else:
                        write(2 * group, jnp.where(low6, re, pltpu.roll(im, 64, 1)))
                        write(2 * group + 1, jnp.where(low6, pltpu.roll(re, 64, 1), im))

            for j, offset in others:
                device = peer(offset)
                d = flat(device)

                def write(f, value):
                    ready[d, slot_of(f, x), :BAND, :] = value

                fill(d, write)
                first_copy(x, device).start()

            def keep_own(f, value):
                arrived[slot_of(f, x), me, :BAND, :] = value

            fill(me, keep_own)
            return carry

        lax.fori_loop(0, BAND, spread, 0)

    top[...] = jnp.zeros_like(top)
    total[...] = jnp.zeros_like(total)
    for copy in tabled:
        copy.wait()

    row = lax.broadcasted_iota(jnp.int32, (256, 128), 0)
    col = lax.broadcasted_iota(jnp.int32, (256, 128), 1)
    ky = signed(row // 8 * BAND + row % 8).astype(f32)
    kz = (col % 64).astype(f32)
    sign = jnp.where(col < 64, -1.0, 1.0)
    lane = lax.broadcasted_iota(jnp.int32, (GRID, 128), 1)
    lower = lane < 64

    def to_grid(x, pair, tiles):
        for odd in range(2):
            turns[:, 128 * odd : 128 * (odd + 1)] = tiles[odd]
        wide = table_by_data(ey_ref, turns[...], ((1,), (0,)))
        for odd in range(2):
            f = 2 * pair + odd
            cosine = wide[:GRID, 128 * odd : 128 * (odd + 1)]
            sine = pltpu.roll(wide[GRID:, 128 * odd : 128 * (odd + 1)], 64, 1)
            near = cosine + jnp.where(lower, -sine, sine)
            mine = (lane == 16 * f + x) | (lane == 16 * f + 8 + x)
            far = jnp.where(mine, strips64[...], 0.0)
            physical[f] = data_by_table(jnp.concatenate([near, far], axis=1), zt_ref)

    for s in LIVE:

        @pl.when(s != me)
        def _():
            remote(
                ready.at[0, 0], arrived.at[0, s], send64.at[0], recv64.at[s], (px, pz)
            ).wait_recv()

    tile = arrived[0].reshape(256, 128)
    d = ky * pltpu.roll(tile, 64, 1) - 64.0 * pltpu.roll(tile, 80, 1)
    d = jnp.where(col < 88, -pltpu.roll(d, 120, 1), pltpu.roll(d, 8, 1))
    tile = jnp.where((col >= 80) & (col < 96), d, tile)
    wide = table_by_data(ey_ref, tile, ((1,), (0,)))
    strips64[...] = wide[:GRID] + jnp.where(
        lane // 8 % 2 == 0, -pltpu.roll(wide[GRID:], 120, 1), pltpu.roll(wide[GRID:], 8, 1)
    )
    back64[...] = jnp.zeros_like(back64)

    def plane(x, carry):
        for s in LIVE:

            @pl.when(s != me)
            def _():
                slots = pl.ds(1 + 5 * x, 5)
                remote(
                    ready.at[0, slots, pl.ds(0, BAND), :],
                    arrived.at[slots, s, pl.ds(0, BAND), :],
                    send_sems.at[0],
                    recv_sems.at[x, s],
                    (px, pz),
                ).wait_recv()

        tiles = [arrived[slot_of(f, x)].reshape(256, 128) for f in range(2)]
        to_grid(x, 0, tiles)
        turned = sign * pltpu.roll(ky * tiles[1] - kz * tiles[0], 64, 1)
        to_grid(x, 1, [arrived[slot_of(f, x)].reshape(256, 128) for f in (2, 3)])
        to_grid(x, 2, [arrived[slot_of(4, x)].reshape(256, 128), turned])
        u = [physical[f] for f in (2, 0, 1)]
        w = [physical[f] for f in (5, 3, 4)]
        speed = jnp.abs(u[0]) + jnp.abs(u[1]) + jnp.abs(u[2])
        squares = u[0] * u[0] + u[1] * u[1] + u[2] * u[2]
        top[...] = jnp.maximum(top[...], jnp.max(speed.reshape(24, 8, GRID), axis=0))
        total[...] += jnp.sum(squares.reshape(24, 8, GRID), axis=0)
        q = []
        for a in range(3):
            b, c = (a + 1) % 3, (a + 2) % 3
            q.append(data_by_table(u[b] * w[c] - u[c] * w[b], zb_ref))
            near = q[a][:, :128]
            far = pltpu.roll(near, 64, 1)
            back[:GRID, 128 * a : 128 * (a + 1)] = near
            back[GRID:, 128 * a : 128 * (a + 1)] = jnp.where(lower, far, -far)
        way = lane % 8 // 2
        chosen = jnp.where(way == 0, q[0][:, 128:], jnp.where(way == 1, q[1][:, 128:], q[2][:, 128:]))
        back64[:GRID] = jnp.where(lane // 8 == x, chosen, back64[:GRID])
        wide = table_by_data(eyt_ref, back[...], ((1,), (0,)))
        for a in range(3):
            closed[a, x] = wide[:, 128 * a : 128 * (a + 1)].reshape(len(LIVE), 8, 128)
        for j, offset in others:
            device = peer(offset)

            @pl.when(is_live(flat(device)))
            def _():
                remote(
                    closed.at[:, x, place(flat(device)), pl.ds(0, BAND), :],
                    out_hbm.at[:, x, me, pl.ds(0, BAND), :],
                    back_send.at[flat(device)],
                    back_recv.at[me],
                    device,
                ).start()

        return carry

    lax.fori_loop(0, BAND, plane, 0)

    q = back64[:GRID]
    back64[GRID:] = jnp.where(lane % 2 == 0, pltpu.roll(q, 127, 1), -pltpu.roll(q, 1, 1))
    wide = table_by_data(eyt_ref, back64[...], ((1,), (0,)))
    closed64[...] = wide.reshape(len(LIVE), 8, 128)
    stat[...] = jnp.where(lane8 == 0, jnp.max(top[...]), jnp.sum(total[...]))

    def stat_copy(device):
        return remote(stat, stats_hbm.at[me], stat_send.at[flat(device)], stat_recv.at[me], device)

    for j, offset in others:
        device = peer(offset)
        stat_copy(device).start()

        @pl.when(is_live(flat(device)))
        def _():
            remote(
                closed64.at[place(flat(device))],
                last_hbm.at[me],
                last_send.at[flat(device)],
                last_recv.at[me],
                device,
            ).start()

    own = (
        pltpu.make_async_copy(
            closed.at[:, :, place(me), pl.ds(0, BAND), :],
            out_hbm.at[:, :, me, pl.ds(0, BAND), :],
            own_sems.at[0],
        ),
        pltpu.make_async_copy(closed64.at[place(me)], last_hbm.at[me], own_sems.at[1]),
    )
    stat_own = pltpu.make_async_copy(stat, stats_hbm.at[me], own_sems.at[2])
    stat_own.start()

    @pl.when(live)
    def _():
        own[0].start()
        own[1].start()
        own[0].wait()
        own[1].wait()

    stat_own.wait()

    def whole_back(source, send):
        return remote(
            closed.at[:, :, 0, pl.ds(0, BAND), :],
            out_hbm.at[:, :, source, pl.ds(0, BAND), :],
            back_send.at[send],
            back_recv.at[source],
            (px, pz),
        )

    def whole_last(source, send):
        return remote(
            closed64.at[0], last_hbm.at[source], last_send.at[send], last_recv.at[source], (px, pz)
        )

    for j, offset in others:
        device = peer(offset)
        d = flat(device)
        stat_copy(device).wait_send()

        @pl.when(live)
        def _():
            remote(
                ready.at[0, pl.ds(1, SLOTS - 1), pl.ds(0, BAND), :],
                arrived.at[pl.ds(1, SLOTS - 1), 0, pl.ds(0, BAND), :],
                send_sems.at[d],
                recv_sems.at[0, 0],
                (px, pz),
            ).wait_send()
            remote(
                ready.at[0, 0], arrived.at[0, 0], send64.at[d], recv64.at[0], (px, pz)
            ).wait_send()

        @pl.when(is_live(d))
        def _():
            whole_back(0, d).wait_send()
            whole_last(0, d).wait_send()

    for s in range(PARTS):

        @pl.when(s != me)
        def _():
            remote(stat, stats_hbm.at[s], stat_send.at[0], stat_recv.at[s], (px, pz)).wait_recv()

        @pl.when((s != me) & live)
        def _():
            whole_back(s, 0).wait_recv()
            whole_last(s, 0).wait_recv()


def close_kernel(
    cut_ref, dt_ref, power_ref, old_ref, in_ref, last_ref, stats_ref, cs_ref,
    out_ref, cfl_ref, energy_ref, terms, spectra,
):
    fastest = stats_ref[0]
    summed = stats_ref[0]
    for s in range(1, PARTS):
        fastest = jnp.maximum(fastest, stats_ref[s])
        summed = summed + stats_ref[s]
    fastest, summed = jnp.max(fastest[:, :1]), jnp.max(summed[:, 1:2])
    energy = 0.5 * summed * (1.0 / float(GRID**3))
    dt = dt_ref[0]
    cfl_ref[0] = dt * fastest * GRID * (1.0 / (2.0 * math.pi))
    energy_ref[0] = energy
    twice = jnp.maximum(jnp.full((DEPTH, 384), 2.0 * energy, f32), 0.5)
    forcing = power_ref[0] / twice
    eighth = lax.broadcasted_iota(jnp.int32, (PARTS, 128), 1) // 8

    out_ref[:, :, DEPTH:, :] = jnp.zeros((2, 3, 96 - DEPTH, 384), f32)

    pair = pl.program_id(0)
    live = is_live(lax.axis_index("py") * lax.axis_size("pz") + lax.axis_index("pz"))

    @pl.when(live)
    def _():
        for odd in range(2):
            ky = 2 * pair + odd
            for a in range(3):
                terms[128 * a : 128 * (a + 1), :] = in_ref[a, pl.ds(ky, GRID, stride=8), :].T
            last = last_ref[pl.ds(ky, PARTS, stride=8), :]
            apart = jnp.concatenate(
                [jnp.where(eighth == x, last, 0.0) for x in range(BAND)], axis=0
            )
            terms[384:432, :] = apart.T[:48]
            spectra[odd] = data_by_table(terms[...], cs_ref)
        waves, square, inverse, keep = pair_waves(pair, cut_ref)

        def of_pair(a, c):
            halves = []
            for odd in range(2):
                re, im = (
                    spectra[odd, 128 * a + 64 * k : 128 * a + 64 * (k + 1), :] for k in range(2)
                )
                last = spectra[odd, 384:392, :]
                for x in range(1, BAND):
                    last = last + spectra[odd, 384 + 8 * x : 392 + 8 * x, :]
                re64, im64 = last[2 * a : 2 * a + 1], last[2 * a + 1 : 2 * a + 2]
                if c == 0:
                    value, value64 = (r[:, :256] + i[:, 256:] for r, i in ((re, im), (re64, im64)))
                else:
                    value, value64 = (i[:, :256] - r[:, 256:] for r, i in ((re, im), (re64, im64)))
                value = jnp.concatenate([value, value64, jnp.zeros((7, 256), f32)], axis=0)
                halves.append(pltpu.roll(value, 64, 1) if odd else value)
            even, odd = halves
            return jnp.concatenate([even[:, :128], even[:, 128:] + odd[:, :128], odd[:, 128:]], axis=1)

        for c in range(2):
            old = project([old_ref[c, a, :, :] for a in range(3)], waves, inverse, keep)
            forced = project([of_pair(a, c) for a in range(3)], waves, inverse, keep)
            for a in range(3):
                out_ref[c, a, :DEPTH, :] = old[a] + dt * (
                    forced[a] + forcing * old[a] - viscosity * square * old[a]
                )

    @pl.when(jnp.logical_not(live))
    def _():
        out_ref[:, :, :DEPTH, :] = jnp.zeros((2, 3, DEPTH, 384), f32)


SM = pl.BlockSpec(memory_space=pltpu.SMEM)
ANY = pl.BlockSpec(memory_space=pl.ANY)
VMEM_BYTES = 60 * 1024 * 1024


def on_device(velocity_hat, time_step, power, cutoffs):
    tx, cs, ey, zt, zb, eyt = (jnp.asarray(t) for t in tables())
    shape = jax.ShapeDtypeStruct
    block = pl.BlockSpec((2, 3, DEPTH, 384), lambda i: (0, 0, 0, i))
    whole = lambda a: pl.BlockSpec(a.shape, lambda i: (0,) * a.ndim)
    dma = pltpu.SemaphoreType.DMA
    chunks, last, stats = pl.pallas_call(
        exchange_kernel,
        out_shape=(
            shape((3, BAND, PARTS, 8, 128), f32),
            shape((PARTS, 8, 128), f32),
            shape((PARTS, 8, 128), f32),
        ),
        in_specs=[SM] + [ANY] * 6,
        out_specs=(ANY, ANY, ANY),
        scratch_shapes=[
            pltpu.VMEM((3, 2, 3, DEPTH, 384), f32),
            pltpu.VMEM((2, 512, 512), bf16),
            *(pltpu.VMEM(t.shape, bf16) for t in (ey, zt, zb, eyt)),
            pltpu.VMEM((2304, 512), f32),
            pltpu.VMEM((40, 512), f32),
            pltpu.VMEM((4, 40, 128), f32),
            pltpu.VMEM((3, BAND * STRIDE, 128), f32),
            pltpu.VMEM((PARTS, SLOTS, 8, 128), f32),
            pltpu.VMEM((SLOTS, PARTS, 8, 128), f32),
            pltpu.VMEM((256, 256), f32),
            pltpu.VMEM((GRID, 128), f32),
            pltpu.VMEM((6, GRID, GRID), f32),
            pltpu.VMEM((2 * GRID, 384), f32),
            pltpu.VMEM((2 * GRID, 128), f32),
            pltpu.VMEM((3, BAND, len(LIVE), 8, 128), f32),
            pltpu.VMEM((len(LIVE), 8, 128), f32),
            pltpu.VMEM((8, GRID), f32),
            pltpu.VMEM((8, GRID), f32),
            pltpu.VMEM((8, 128), f32),
            dma((11,)),
            dma((PARTS,)),
            dma((BAND, PARTS)),
            *[dma((PARTS,))] * 8,
            dma((3,)),
        ],
        compiler_params=pltpu.CompilerParams(
            collective_id=0, has_side_effects=True, vmem_limit_bytes=VMEM_BYTES
        ),
    )(cutoffs, velocity_hat, tx, ey, zt, zb, eyt)
    chunks = chunks.reshape(3, BAND * PARTS * 8, 128)
    last = last.reshape(PARTS * 8, 128)
    return pl.pallas_call(
        close_kernel,
        grid=(3,),
        out_shape=(shape((2, 3, 96, 1152), f32), shape((1,), f32), shape((1,), f32)),
        in_specs=[SM, SM, SM, block, whole(chunks), whole(last), whole(stats), whole(cs)],
        out_specs=(pl.BlockSpec((2, 3, 96, 384), lambda i: (0, 0, 0, i)), SM, SM),
        scratch_shapes=[pltpu.VMEM((432, GRID), f32), pltpu.VMEM((2, 432, 512), f32)],
        compiler_params=pltpu.CompilerParams(vmem_limit_bytes=VMEM_BYTES),
    )(cutoffs, time_step, power, velocity_hat, chunks, last, stats, cs)


def solution(mesh):
    return jax.shard_map(
        on_device,
        mesh=mesh,
        in_specs=(P("member", None, None, ("py", "pz")), P("member"), P("member"), P("member")),
        out_specs=(P("member", None, None, ("py", "pz")), P("member"), P("member")),
        check_vma=False,
    )
```

```python
import functools
import math

import jax
import jax.numpy as jnp
import ml_dtypes
import numpy as np
from jax import lax
from jax.experimental import pallas as pl
from jax.experimental.pallas import tpu as pltpu
from jax.sharding import PartitionSpec as P

GRID = 192
PARTS = 32
BAND = 6
DEPTH = 72
LIVE = tuple(range(11)) + tuple(range(21, 32))
viscosity = 0.004
f32 = jnp.float32
bf16 = jnp.bfloat16


def halves(table):
    high = table.astype(ml_dtypes.bfloat16)
    low = (table - high.astype(np.float64)).astype(ml_dtypes.bfloat16)
    return np.stack([high, low])


def angle(rows, cols):
    turns = np.outer(rows, cols) % GRID
    return turns * (2.0 * math.pi / GRID)


@functools.lru_cache
def tables():
    n = GRID
    every = np.arange(n)
    phase = angle(every, every)
    tx = np.zeros((PARTS, 8, 768))
    cosine, sine = (f(phase).reshape(PARTS, BAND, n) for f in (np.cos, np.sin))
    for at, part in ((0, cosine), (256, sine), (512, -sine)):
        tx[:, :BAND, at : at + n] = part
    tx = tx.reshape(256, 768)
    cs = np.zeros((n, 512))
    cs[:, :n] = cosine.transpose(1, 0, 2).reshape(n, n)
    cs[:, 256 : 256 + n] = sine.transpose(1, 0, 2).reshape(n, n)
    ey = np.zeros((2 * n, 256))
    eyt = np.zeros((8 * len(LIVE), 2 * n))
    for at, band in enumerate(LIVE):
        phase = angle(every, band * BAND + np.arange(BAND))
        cols = slice(8 * band, 8 * band + BAND)
        ey[:n, cols], ey[n:, cols] = np.cos(phase), np.sin(phase)
        rows = slice(8 * at, 8 * at + BAND)
        eyt[rows, :n], eyt[rows, n:] = np.cos(phase).T, np.sin(phase).T
    factor = float(n) ** -1.5
    phase = angle(np.arange(65), every)
    cosine, sine = factor * np.cos(phase), factor * np.sin(phase)
    zt = np.zeros((256, n))
    weight = np.where(np.arange(64) == 0, 1.0, 2.0)[:, None]
    zt[:64], zt[64:128] = weight * cosine[:64], -weight * sine[:64]
    for f in range(6):
        zt[128 + 16 * f : 136 + 16 * f] = 2.0 * cosine[64]
        zt[136 + 16 * f : 144 + 16 * f] = -2.0 * sine[64]
    zb = np.zeros((n, 256))
    zb[:, :64], zb[:, 64:128] = cosine[:64].T, -sine[:64].T
    for x in range(BAND):
        for a in range(3):
            zb[:, 128 + 8 * x + 2 * a] = cosine[64]
            zb[:, 128 + 8 * x + 2 * a + 1] = -sine[64]
    return tuple(halves(t) for t in (tx, cs, ey, zt, zb, eyt))


def split(value):
    high = value.astype(bf16)
    return high, (value - high.astype(f32)).astype(bf16)


def table_by_data(table, data, dims):
    high, low = split(data)
    dot = functools.partial(
        lax.dot_general, dimension_numbers=(dims, ((), ())), preferred_element_type=f32
    )
    return dot(table[0], high) + dot(table[0], low) + dot(table[1], high)


def data_by_table(data, table):
    high, low = split(data)
    dot = functools.partial(jnp.dot, preferred_element_type=f32)
    return dot(high, table[0]) + dot(low, table[0]) + dot(high, table[1])


def signed(index):
    return jnp.where(index < GRID // 2, index, index - GRID)


def pair_waves(pair, cut_ref):
    band = lax.axis_index("py") * lax.axis_size("pz") + lax.axis_index("pz")
    lane = lax.broadcasted_iota(jnp.int32, (DEPTH, 384), 1)
    upper = lane >= GRID
    kx = signed(jnp.where(upper, lane - GRID, lane))
    ky = signed(band * BAND + 2 * pair + upper.astype(jnp.int32))
    kz = lax.broadcasted_iota(jnp.int32, (DEPTH, 384), 0)
    keep = (
        (jnp.abs(kx) <= cut_ref[0]) & (jnp.abs(ky) <= cut_ref[1]) & (kz <= cut_ref[2])
    )
    waves = tuple(k.astype(f32) for k in (kx, ky, kz))
    square = waves[0] * waves[0] + waves[1] * waves[1] + waves[2] * waves[2]
    return waves, square, 1.0 / jnp.maximum(square, 1.0), keep


def project(field, waves, inverse, keep):
    normal = (waves[0] * field[0] + waves[1] * field[1] + waves[2] * field[2]) * inverse
    return [jnp.where(keep, field[a] - waves[a] * normal, 0.0) for a in range(3)]


MESH = pl.DeviceIdType.MESH
TURNS = ((1, 1), (3, 0), (2, 1), (0, 0), (1, 0), (3, 1), (2, 0), (0, 1))
OFFSETS = tuple(
    (dx, *TURNS[(k + 2 * j) % 8]) for k in range(8) for j, dx in enumerate((2, 1, 3, 0))
)


SLOTS = 31
STRIDE = 520


def slot_of(f, x):
    return 1 + 5 * x + f


def is_live(band):
    return (band < 11) | (band >= 21)


def exchange_kernel(
    cut_ref, in_hbm, tx_hbm, ey_hbm, zt_hbm, zb_hbm, eyt_hbm, out_hbm, last_hbm, stats_hbm,
    held, tx_ref, ey_ref, zt_ref, zb_ref, eyt_ref, data, data64, wide64, made, ready, arrived,
    turns, strips64, physical, back, back64, closed, closed64, top, total, stat,
    load_sems, send_sems, recv_sems, back_sems, own_sems,
):
    px, pz = lax.axis_index("py"), lax.axis_index("pz")
    me = px * 8 + pz
    live = is_live(me)

    def peer(offset):
        x = lax.rem(px + offset[0], 4)
        y = lax.rem(pz // 2 + offset[1], 4)
        z = lax.rem(pz % 2 + offset[2], 2)
        return x, y * 2 + z

    def flat(device):
        return device[0] * 8 + device[1]

    def place(band):
        return jnp.where(band < 11, band, band - 10)

    def remote(source, target, send, recv, device):
        return pltpu.make_async_remote_copy(
            src_ref=source,
            dst_ref=target,
            send_sem=send,
            recv_sem=recv,
            device_id={"py": device[0], "pz": device[1]},
            device_id_type=MESH,
        )

    others = [(j, offset) for j, offset in enumerate(OFFSETS) if offset != (0, 0, 0)]

    loads = [
        pltpu.make_async_copy(
            in_hbm.at[:, :, pl.ds(0, DEPTH), pl.ds(384 * p, 384)], held.at[p], load_sems.at[p]
        )
        for p in range(3)
    ]
    tabled = [
        pltpu.make_async_copy(source, target, load_sems.at[3 + k])
        for k, (source, target) in enumerate(
            ((ey_hbm, ey_ref), (zt_hbm, zt_ref), (zb_hbm, zb_ref), (eyt_hbm, eyt_ref))
        )
    ]
    quarters = [
        pltpu.make_async_copy(
            tx_hbm.at[:, :, pl.ds(low, 256)],
            tx_ref.at[:, pl.ds(256 * (k // 2), 256), pl.ds(256 * (k % 2), 256)],
            load_sems.at[7 + k],
        )
        for k, low in enumerate((0, 512, 256, 0))
    ]
    for copy in (*loads, *quarters, *tabled):
        copy.start()

    def clear(slot, carry):
        arrived[slot] = jnp.zeros((PARTS, 8, 128), f32)
        return carry

    lax.fori_loop(0, SLOTS, clear, 0)
    barrier = pltpu.get_barrier_semaphore()
    for _, offset in others:
        device = peer(offset)
        pl.semaphore_signal(
            barrier, inc=1, device_id={"py": device[0], "pz": device[1]}, device_id_type=MESH
        )

    def first_copy(x, device):
        slots = pl.ds(1 + 5 * x, 5)
        return remote(
            ready.at[flat(device), slots, pl.ds(0, BAND), :],
            arrived.at[slots, me, pl.ds(0, BAND), :],
            send_sems.at[0],
            recv_sems.at[x],
            device,
        )

    lane8 = lax.broadcasted_iota(jnp.int32, (8, 128), 1)
    low6 = lax.broadcasted_iota(jnp.int32, (BAND, 128), 1) < 64

    data64[...] = jnp.zeros_like(data64)
    for pair in range(3):
        loads[pair].wait()

        @pl.when(live)
        def _():
            waves, _, inverse, keep = pair_waves(pair, cut_ref)
            parts = []
            for c in range(2):
                sol = project([held[pair, c, a] for a in range(3)], waves, inverse, keep)
                curl_y = waves[2] * sol[0] - waves[0] * sol[2]
                curl_z = waves[0] * sol[1] - waves[1] * sol[0]
                parts.append((sol, (curl_y, curl_z)))
            fields = []
            for c in range(2):
                turn = parts[1 - c][1]
                if c == 0:
                    turn = (-turn[0], -turn[1])
                sol = parts[c][0]
                fields.append((sol[1], sol[2], sol[0], turn[0], turn[1]))
            for odd in range(2):
                ky = 2 * pair + odd
                for c in range(2):
                    cols = slice(c * 256, (c + 1) * 256)
                    for f in range(5):
                        value = fields[c][f]
                        if odd:
                            value = pltpu.roll(value[:, 128:], 192, 1)
                        else:
                            value = value[:, :256]
                        low = 768 * (f // 2) + 128 * ky + 64 * (f % 2)
                        data[low : low + 64, cols] = value[:64]
                        if f == 4:
                            data[low + 64 : low + 128, cols] = value[:64]
                        data64[8 * f + ky : 8 * f + ky + 1, cols] = value[64:65]

    for copy in quarters:
        copy.wait()

    @pl.when(live)
    def _():
        high, low = split(data64[...])
        dot = functools.partial(
            lax.dot_general,
            dimension_numbers=(((1,), (1,)), ((), ())),
            preferred_element_type=f32,
        )
        wide = dot(high, tx_ref[0]) + dot(low, tx_ref[0]) + dot(high, tx_ref[1])
        for k in range(4):
            wide64[k] = wide[:, 128 * k : 128 * (k + 1)]
        for d in range(PARTS):
            tile = jnp.zeros((8, 128), f32)
            for f in range(5):
                for c in range(2):
                    spot = 16 * f + 8 * c
                    part = wide64[2 * c + d // 16, 8 * f : 8 * f + 8, :]
                    shift = (spot - 8 * (d % 16)) % 128
                    if shift:
                        part = pltpu.roll(part, shift, 1)
                    tile = jnp.where((lane8 >= spot) & (lane8 < spot + 8), part, tile)
            ready[d, 0] = tile

        for group in range(3):
            for pair in range(3):
                low = 768 * group + 256 * pair
                wide = table_by_data(tx_ref, data[low : low + 256, :], ((1,), (1,)))
                for odd in range(2):
                    at = (2 * pair + odd) * STRIDE
                    made[group, at : at + 512, :] = wide[:, 128 * odd : 128 * (odd + 1)]

    pl.semaphore_wait(barrier, PARTS - 1)

    @pl.when(live)
    def _():
        for j, offset in others:
            device = peer(offset)
            remote(
                ready.at[flat(device), 0],
                arrived.at[0, me],
                send_sems.at[1],
                recv_sems.at[BAND],
                device,
            ).start()
        arrived[0, me] = ready[me, 0]

        def spread(x, carry):
            def fill(d, write):
                for group in range(3):
                    re, im = (
                        made[group, pl.ds(256 * c + 8 * d + x, BAND, stride=STRIDE), :]
                        for c in range(2)
                    )
                    if group == 2:
                        write(4, jnp.where(low6, re, im))
                    else:
                        write(2 * group, jnp.where(low6, re, pltpu.roll(im, 64, 1)))
                        write(2 * group + 1, jnp.where(low6, pltpu.roll(re, 64, 1), im))

            for j, offset in others:
                device = peer(offset)
                d = flat(device)

                def write(f, value):
                    ready[d, slot_of(f, x), :BAND, :] = value

                fill(d, write)
                first_copy(x, device).start()

            def keep_own(f, value):
                arrived[slot_of(f, x), me, :BAND, :] = value

            fill(me, keep_own)
            return carry

        lax.fori_loop(0, BAND, spread, 0)

    top[...] = jnp.zeros_like(top)
    total[...] = jnp.zeros_like(total)
    for copy in tabled:
        copy.wait()

    row = lax.broadcasted_iota(jnp.int32, (256, 128), 0)
    col = lax.broadcasted_iota(jnp.int32, (256, 128), 1)
    ky = signed(row // 8 * BAND + row % 8).astype(f32)
    kz = (col % 64).astype(f32)
    sign = jnp.where(col < 64, -1.0, 1.0)
    lane = lax.broadcasted_iota(jnp.int32, (GRID, 128), 1)
    lower = lane < 64

    def to_grid(x, pair, tiles):
        for odd in range(2):
            turns[:, 128 * odd : 128 * (odd + 1)] = tiles[odd]
        wide = table_by_data(ey_ref, turns[...], ((1,), (0,)))
        for odd in range(2):
            f = 2 * pair + odd
            cosine = wide[:GRID, 128 * odd : 128 * (odd + 1)]
            sine = pltpu.roll(wide[GRID:, 128 * odd : 128 * (odd + 1)], 64, 1)
            near = cosine + jnp.where(lower, -sine, sine)
            mine = (lane == 16 * f + x) | (lane == 16 * f + 8 + x)
            far = jnp.where(mine, strips64[...], 0.0)
            physical[f] = data_by_table(jnp.concatenate([near, far], axis=1), zt_ref)

    def from_live(await_count):
        pl.when(live)(lambda: await_count(len(LIVE) - 1))
        pl.when(jnp.logical_not(live))(lambda: await_count(len(LIVE)))

    def await_last(count):
        part = arrived.at[0, pl.ds(0, count)]
        remote(part, part, send_sems.at[1], recv_sems.at[BAND], (px, pz)).wait_recv()

    from_live(await_last)
    tile = arrived[0].reshape(256, 128)
    d = ky * pltpu.roll(tile, 64, 1) - 64.0 * pltpu.roll(tile, 80, 1)
    d = jnp.where(col < 88, -pltpu.roll(d, 120, 1), pltpu.roll(d, 8, 1))
    tile = jnp.where((col >= 80) & (col < 96), d, tile)
    wide = table_by_data(ey_ref, tile, ((1,), (0,)))
    strips64[...] = wide[:GRID] + jnp.where(
        lane // 8 % 2 == 0, -pltpu.roll(wide[GRID:], 120, 1), pltpu.roll(wide[GRID:], 8, 1)
    )
    back64[...] = jnp.zeros_like(back64)

    def plane(x, carry):
        def await_plane(count):
            part = arrived.at[pl.ds(1 + 5 * x, 5), pl.ds(0, count), pl.ds(0, BAND), :]
            remote(part, part, send_sems.at[0], recv_sems.at[x], (px, pz)).wait_recv()

        from_live(await_plane)
        tiles = [arrived[slot_of(f, x)].reshape(256, 128) for f in range(2)]
        to_grid(x, 0, tiles)
        turned = sign * pltpu.roll(ky * tiles[1] - kz * tiles[0], 64, 1)
        to_grid(x, 1, [arrived[slot_of(f, x)].reshape(256, 128) for f in (2, 3)])
        to_grid(x, 2, [arrived[slot_of(4, x)].reshape(256, 128), turned])
        u = [physical[f] for f in (2, 0, 1)]
        w = [physical[f] for f in (5, 3, 4)]
        speed = jnp.abs(u[0]) + jnp.abs(u[1]) + jnp.abs(u[2])
        squares = u[0] * u[0] + u[1] * u[1] + u[2] * u[2]
        top[...] = jnp.maximum(top[...], jnp.max(speed.reshape(24, 8, GRID), axis=0))
        total[...] += jnp.sum(squares.reshape(24, 8, GRID), axis=0)
        q = []
        for a in range(3):
            b, c = (a + 1) % 3, (a + 2) % 3
            q.append(data_by_table(u[b] * w[c] - u[c] * w[b], zb_ref))
            near = q[a][:, :128]
            far = pltpu.roll(near, 64, 1)
            back[:GRID, 128 * a : 128 * (a + 1)] = near
            back[GRID:, 128 * a : 128 * (a + 1)] = jnp.where(lower, far, -far)
        way = lane % 8 // 2
        chosen = jnp.where(way == 0, q[0][:, 128:], jnp.where(way == 1, q[1][:, 128:], q[2][:, 128:]))
        back64[:GRID] = jnp.where(lane // 8 == x, chosen, back64[:GRID])
        wide = table_by_data(eyt_ref, back[...], ((1,), (0,)))
        for a in range(3):
            closed[a, x] = wide[:, 128 * a : 128 * (a + 1)].reshape(len(LIVE), 8, 128)
        for j, offset in others:
            device = peer(offset)

            @pl.when(is_live(flat(device)))
            def _():
                remote(
                    closed.at[:, x, place(flat(device)), pl.ds(0, BAND), :],
                    out_hbm.at[:, x, me, pl.ds(0, BAND), :],
                    back_sems.at[0],
                    back_sems.at[1],
                    device,
                ).start()

        return carry

    lax.fori_loop(0, BAND, plane, 0)

    q = back64[:GRID]
    back64[GRID:] = jnp.where(lane % 2 == 0, pltpu.roll(q, 127, 1), -pltpu.roll(q, 1, 1))
    wide = table_by_data(eyt_ref, back64[...], ((1,), (0,)))
    closed64[...] = wide.reshape(len(LIVE), 8, 128)
    stat[...] = jnp.where(lane8 == 0, jnp.max(top[...]), jnp.sum(total[...]))

    def stat_copy(device):
        return remote(stat, stats_hbm.at[me], back_sems.at[2], back_sems.at[3], device)

    for j, offset in others:
        device = peer(offset)
        stat_copy(device).start()

        @pl.when(is_live(flat(device)))
        def _():
            remote(
                closed64.at[place(flat(device))],
                last_hbm.at[me],
                back_sems.at[4],
                back_sems.at[5],
                device,
            ).start()

    own = (
        pltpu.make_async_copy(
            closed.at[:, :, place(me), pl.ds(0, BAND), :],
            out_hbm.at[:, :, me, pl.ds(0, BAND), :],
            own_sems.at[0],
        ),
        pltpu.make_async_copy(closed64.at[place(me)], last_hbm.at[me], own_sems.at[1]),
    )
    stat_own = pltpu.make_async_copy(stat, stats_hbm.at[me], own_sems.at[2])
    stat_own.start()

    @pl.when(live)
    def _():
        own[0].start()
        own[1].start()
        own[0].wait()
        own[1].wait()

    stat_own.wait()

    def sent(part, sem):
        remote(part, part, sem, recv_sems.at[0], (px, pz)).wait_send()

    def came(part, sem):
        remote(part, part, send_sems.at[0], sem, (px, pz)).wait_recv()

    rest = pl.ds(0, PARTS - 1)

    def await_sent(count):
        sent(closed.at[:, :, pl.ds(0, count), pl.ds(0, BAND), :], back_sems.at[0])
        sent(closed64.at[pl.ds(0, count)], back_sems.at[4])

    from_live(await_sent)
    sent(arrived.at[0, rest], back_sems.at[2])
    came(stats_hbm.at[rest], back_sems.at[3])

    @pl.when(live)
    def _():
        sent(ready.at[rest, pl.ds(1, SLOTS - 1), pl.ds(0, BAND), :], send_sems.at[0])
        sent(ready.at[rest, 0], send_sems.at[1])
        came(out_hbm.at[:, :, rest, pl.ds(0, BAND), :], back_sems.at[1])
        came(last_hbm.at[rest], back_sems.at[5])


def close_kernel(
    cut_ref, dt_ref, power_ref, old_ref, in_ref, last_ref, stats_ref, cs_ref,
    out_ref, cfl_ref, energy_ref, terms, spectra,
):
    fastest = stats_ref[0]
    summed = stats_ref[0]
    for s in range(1, PARTS):
        fastest = jnp.maximum(fastest, stats_ref[s])
        summed = summed + stats_ref[s]
    fastest, summed = jnp.max(fastest[:, :1]), jnp.max(summed[:, 1:2])
    energy = 0.5 * summed * (1.0 / float(GRID**3))
    dt = dt_ref[0]
    cfl_ref[0] = dt * fastest * GRID * (1.0 / (2.0 * math.pi))
    energy_ref[0] = energy
    twice = jnp.maximum(jnp.full((DEPTH, 384), 2.0 * energy, f32), 0.5)
    forcing = power_ref[0] / twice
    eighth = lax.broadcasted_iota(jnp.int32, (PARTS, 128), 1) // 8

    out_ref[:, :, DEPTH:, :] = jnp.zeros((2, 3, 96 - DEPTH, 384), f32)

    pair = pl.program_id(0)
    live = is_live(lax.axis_index("py") * lax.axis_size("pz") + lax.axis_index("pz"))

    @pl.when(live)
    def _():
        for odd in range(2):
            ky = 2 * pair + odd
            for a in range(3):
                terms[128 * a : 128 * (a + 1), :] = in_ref[a, pl.ds(ky, GRID, stride=8), :].T
            last = last_ref[pl.ds(ky, PARTS, stride=8), :]
            apart = jnp.concatenate(
                [jnp.where(eighth == x, last, 0.0) for x in range(BAND)], axis=0
            )
            terms[384:432, :] = apart.T[:48]
            spectra[odd] = data_by_table(terms[...], cs_ref)
        waves, square, inverse, keep = pair_waves(pair, cut_ref)

        def of_pair(a, c):
            halves = []
            for odd in range(2):
                re, im = (
                    spectra[odd, 128 * a + 64 * k : 128 * a + 64 * (k + 1), :] for k in range(2)
                )
                last = spectra[odd, 384:392, :]
                for x in range(1, BAND):
                    last = last + spectra[odd, 384 + 8 * x : 392 + 8 * x, :]
                re64, im64 = last[2 * a : 2 * a + 1], last[2 * a + 1 : 2 * a + 2]
                if c == 0:
                    value, value64 = (r[:, :256] + i[:, 256:] for r, i in ((re, im), (re64, im64)))
                else:
                    value, value64 = (i[:, :256] - r[:, 256:] for r, i in ((re, im), (re64, im64)))
                value = jnp.concatenate([value, value64, jnp.zeros((7, 256), f32)], axis=0)
                halves.append(pltpu.roll(value, 64, 1) if odd else value)
            even, odd = halves
            return jnp.concatenate([even[:, :128], even[:, 128:] + odd[:, :128], odd[:, 128:]], axis=1)

        for c in range(2):
            old = project([old_ref[c, a, :, :] for a in range(3)], waves, inverse, keep)
            forced = project([of_pair(a, c) for a in range(3)], waves, inverse, keep)
            for a in range(3):
                out_ref[c, a, :DEPTH, :] = old[a] + dt * (
                    forced[a] + forcing * old[a] - viscosity * square * old[a]
                )

    @pl.when(jnp.logical_not(live))
    def _():
        out_ref[:, :, :DEPTH, :] = jnp.zeros((2, 3, DEPTH, 384), f32)


SM = pl.BlockSpec(memory_space=pltpu.SMEM)
ANY = pl.BlockSpec(memory_space=pl.ANY)
VMEM_BYTES = 60 * 1024 * 1024


def on_device(velocity_hat, time_step, power, cutoffs):
    tx, cs, ey, zt, zb, eyt = (jnp.asarray(t) for t in tables())
    shape = jax.ShapeDtypeStruct
    block = pl.BlockSpec((2, 3, DEPTH, 384), lambda i: (0, 0, 0, i))
    whole = lambda a: pl.BlockSpec(a.shape, lambda i: (0,) * a.ndim)
    dma = pltpu.SemaphoreType.DMA
    chunks, last, stats = pl.pallas_call(
        exchange_kernel,
        out_shape=(
            shape((3, BAND, PARTS, 8, 128), f32),
            shape((PARTS, 8, 128), f32),
            shape((PARTS, 8, 128), f32),
        ),
        in_specs=[SM] + [ANY] * 6,
        out_specs=(ANY, ANY, ANY),
        scratch_shapes=[
            pltpu.VMEM((3, 2, 3, DEPTH, 384), f32),
            pltpu.VMEM((2, 512, 512), bf16),
            *(pltpu.VMEM(t.shape, bf16) for t in (ey, zt, zb, eyt)),
            pltpu.VMEM((2304, 512), f32),
            pltpu.VMEM((40, 512), f32),
            pltpu.VMEM((4, 40, 128), f32),
            pltpu.VMEM((3, BAND * STRIDE, 128), f32),
            pltpu.VMEM((PARTS, SLOTS, 8, 128), f32),
            pltpu.VMEM((SLOTS, PARTS, 8, 128), f32),
            pltpu.VMEM((256, 256), f32),
            pltpu.VMEM((GRID, 128), f32),
            pltpu.VMEM((6, GRID, GRID), f32),
            pltpu.VMEM((2 * GRID, 384), f32),
            pltpu.VMEM((2 * GRID, 128), f32),
            pltpu.VMEM((3, BAND, len(LIVE), 8, 128), f32),
            pltpu.VMEM((len(LIVE), 8, 128), f32),
            pltpu.VMEM((8, GRID), f32),
            pltpu.VMEM((8, GRID), f32),
            pltpu.VMEM((8, 128), f32),
            dma((11,)),
            dma((2,)),
            dma((BAND + 1,)),
            dma((6,)),
            dma((3,)),
        ],
        compiler_params=pltpu.CompilerParams(
            collective_id=0, has_side_effects=True, vmem_limit_bytes=VMEM_BYTES
        ),
    )(cutoffs, velocity_hat, tx, ey, zt, zb, eyt)
    chunks = chunks.reshape(3, BAND * PARTS * 8, 128)
    last = last.reshape(PARTS * 8, 128)
    return pl.pallas_call(
        close_kernel,
        grid=(3,),
        out_shape=(shape((2, 3, 96, 1152), f32), shape((1,), f32), shape((1,), f32)),
        in_specs=[SM, SM, SM, block, whole(chunks), whole(last), whole(stats), whole(cs)],
        out_specs=(pl.BlockSpec((2, 3, 96, 384), lambda i: (0, 0, 0, i)), SM, SM),
        scratch_shapes=[pltpu.VMEM((432, GRID), f32), pltpu.VMEM((2, 432, 512), f32)],
        compiler_params=pltpu.CompilerParams(vmem_limit_bytes=VMEM_BYTES),
    )(cutoffs, time_step, power, velocity_hat, chunks, last, stats, cs)


def solution(mesh):
    return jax.shard_map(
        on_device,
        mesh=mesh,
        in_specs=(P("member", None, None, ("py", "pz")), P("member"), P("member"), P("member")),
        out_specs=(P("member", None, None, ("py", "pz")), P("member"), P("member")),
        check_vma=False,
    )
```

```python
import functools
import math

import jax
import jax.numpy as jnp
import ml_dtypes
import numpy as np
from jax import lax
from jax.experimental import pallas as pl
from jax.experimental.pallas import tpu as pltpu
from jax.sharding import PartitionSpec as P

GRID = 192
PARTS = 32
BAND = 6
DEPTH = 72
LIVE = tuple(range(11)) + tuple(range(21, 32))
viscosity = 0.004
f32 = jnp.float32
bf16 = jnp.bfloat16


def halves(table):
    high = table.astype(ml_dtypes.bfloat16)
    low = (table - high.astype(np.float64)).astype(ml_dtypes.bfloat16)
    return np.stack([high, low])


def angle(rows, cols):
    turns = np.outer(rows, cols) % GRID
    return turns * (2.0 * math.pi / GRID)


@functools.lru_cache
def tables():
    n = GRID
    every = np.arange(n)
    phase = angle(every, every)
    near = np.where(np.arange(128) <= 64, np.arange(128), np.arange(128) + 64)
    phase = angle(every, near)
    tx = np.zeros((PARTS, 8, 384))
    cosine, sine = (f(phase).reshape(PARTS, BAND, 128) for f in (np.cos, np.sin))
    for at, part in ((0, cosine), (128, sine), (256, -sine)):
        tx[:, :BAND, at : at + 128] = part
    tx = tx.reshape(256, 384)
    cs = np.zeros((n, 256))
    cs[:, :128] = cosine.transpose(1, 0, 2).reshape(n, 128)
    cs[:, 128:] = sine.transpose(1, 0, 2).reshape(n, 128)
    ey = np.zeros((2 * n, 256))
    eyt = np.zeros((8 * len(LIVE), 2 * n))
    for at, band in enumerate(LIVE):
        phase = angle(every, band * BAND + np.arange(BAND))
        cols = slice(8 * band, 8 * band + BAND)
        ey[:n, cols], ey[n:, cols] = np.cos(phase), np.sin(phase)
        rows = slice(8 * at, 8 * at + BAND)
        eyt[rows, :n], eyt[rows, n:] = np.cos(phase).T, np.sin(phase).T
    factor = float(n) ** -1.5
    phase = angle(np.arange(65), every)
    cosine, sine = factor * np.cos(phase), factor * np.sin(phase)
    zt = np.zeros((256, n))
    weight = np.where(np.arange(64) == 0, 1.0, 2.0)[:, None]
    zt[:64], zt[64:128] = weight * cosine[:64], -weight * sine[:64]
    for f in range(6):
        zt[128 + 16 * f : 136 + 16 * f] = 2.0 * cosine[64]
        zt[136 + 16 * f : 144 + 16 * f] = -2.0 * sine[64]
    zb = np.zeros((n, 256))
    zb[:, :64], zb[:, 64:128] = cosine[:64].T, -sine[:64].T
    for x in range(BAND):
        for a in range(3):
            zb[:, 128 + 8 * x + 2 * a] = cosine[64]
            zb[:, 128 + 8 * x + 2 * a + 1] = -sine[64]
    return tuple(halves(t) for t in (tx, cs, ey, zt, zb, eyt))


def split(value):
    high = value.astype(bf16)
    return high, (value - high.astype(f32)).astype(bf16)


def table_by_data(table, data, dims):
    high, low = split(data)
    dot = functools.partial(
        lax.dot_general, dimension_numbers=(dims, ((), ())), preferred_element_type=f32
    )
    return dot(table[0], high) + dot(table[0], low) + dot(table[1], high)


def data_by_table(data, table):
    high, low = split(data)
    dot = functools.partial(jnp.dot, preferred_element_type=f32)
    return dot(high, table[0]) + dot(low, table[0]) + dot(high, table[1])


def signed(index):
    return jnp.where(index < GRID // 2, index, index - GRID)


def pair_waves(pair, cut_ref):
    band = lax.axis_index("py") * lax.axis_size("pz") + lax.axis_index("pz")
    lane = lax.broadcasted_iota(jnp.int32, (DEPTH, 384), 1)
    upper = lane >= GRID
    kx = signed(jnp.where(upper, lane - GRID, lane))
    ky = signed(band * BAND + 2 * pair + upper.astype(jnp.int32))
    kz = lax.broadcasted_iota(jnp.int32, (DEPTH, 384), 0)
    keep = (
        (jnp.abs(kx) <= cut_ref[0]) & (jnp.abs(ky) <= cut_ref[1]) & (kz <= cut_ref[2])
    )
    waves = tuple(k.astype(f32) for k in (kx, ky, kz))
    square = waves[0] * waves[0] + waves[1] * waves[1] + waves[2] * waves[2]
    return waves, square, 1.0 / jnp.maximum(square, 1.0), keep


def project(field, waves, inverse, keep):
    normal = (waves[0] * field[0] + waves[1] * field[1] + waves[2] * field[2]) * inverse
    return [jnp.where(keep, field[a] - waves[a] * normal, 0.0) for a in range(3)]


MESH = pl.DeviceIdType.MESH
TURNS = ((1, 1), (3, 0), (2, 1), (0, 0), (1, 0), (3, 1), (2, 0), (0, 1))
OFFSETS = tuple(
    (dx, *TURNS[(k + 2 * j) % 8]) for k in range(8) for j, dx in enumerate((2, 1, 3, 0))
)


SLOTS = 31
STRIDE = 520


def slot_of(f, x):
    return 1 + 5 * x + f


def is_live(band):
    return (band < 11) | (band >= 21)


def exchange_kernel(
    cut_ref, in_hbm, tx_hbm, ey_hbm, zt_hbm, zb_hbm, eyt_hbm, out_hbm, last_hbm, stats_hbm,
    held, tx_ref, ey_ref, zt_ref, zb_ref, eyt_ref, data, data64, wide64, made, ready, arrived,
    turns, strips64, physical, back, back64, closed, closed64, top, total, stat,
    load_sems, send_sems, recv_sems, back_sems, own_sems,
):
    px, pz = lax.axis_index("py"), lax.axis_index("pz")
    me = px * 8 + pz
    live = is_live(me)

    def peer(offset):
        x = lax.rem(px + offset[0], 4)
        y = lax.rem(pz // 2 + offset[1], 4)
        z = lax.rem(pz % 2 + offset[2], 2)
        return x, y * 2 + z

    def flat(device):
        return device[0] * 8 + device[1]

    def place(band):
        return jnp.where(band < 11, band, band - 10)

    def remote(source, target, send, recv, device):
        return pltpu.make_async_remote_copy(
            src_ref=source,
            dst_ref=target,
            send_sem=send,
            recv_sem=recv,
            device_id={"py": device[0], "pz": device[1]},
            device_id_type=MESH,
        )

    others = [(j, offset) for j, offset in enumerate(OFFSETS) if offset != (0, 0, 0)]

    loads = [
        pltpu.make_async_copy(
            in_hbm.at[:, :, pl.ds(0, DEPTH), pl.ds(384 * p, 384)], held.at[p], load_sems.at[p]
        )
        for p in range(3)
    ]
    tabled = [
        pltpu.make_async_copy(source, target, load_sems.at[3 + k])
        for k, (source, target) in enumerate(
            ((ey_hbm, ey_ref), (zt_hbm, zt_ref), (zb_hbm, zb_ref), (eyt_hbm, eyt_ref))
        )
    ]
    quarters = [
        pltpu.make_async_copy(
            tx_hbm.at[:, :, pl.ds(low, 128)],
            tx_ref.at[:, pl.ds(256 * (k // 2), 256), pl.ds(128 * (k % 2), 128)],
            load_sems.at[7 + k],
        )
        for k, low in enumerate((0, 256, 128, 0))
    ]
    for copy in (*loads, *quarters, *tabled):
        copy.start()

    def clear(slot, carry):
        arrived[slot] = jnp.zeros((PARTS, 8, 128), f32)
        return carry

    lax.fori_loop(0, SLOTS, clear, 0)
    barrier = pltpu.get_barrier_semaphore()
    for _, offset in others:
        device = peer(offset)
        pl.semaphore_signal(
            barrier, inc=1, device_id={"py": device[0], "pz": device[1]}, device_id_type=MESH
        )

    def first_copy(x, device):
        slots = pl.ds(1 + 5 * x, 5)
        return remote(
            ready.at[flat(device), slots, pl.ds(0, BAND), :],
            arrived.at[slots, me, pl.ds(0, BAND), :],
            send_sems.at[0],
            recv_sems.at[x],
            device,
        )

    lane8 = lax.broadcasted_iota(jnp.int32, (8, 128), 1)
    low6 = lax.broadcasted_iota(jnp.int32, (BAND, 128), 1) < 64

    data64[...] = jnp.zeros_like(data64)
    for pair in range(3):
        loads[pair].wait()

        @pl.when(live)
        def _():
            waves, _, inverse, keep = pair_waves(pair, cut_ref)
            parts = []
            for c in range(2):
                sol = project([held[pair, c, a] for a in range(3)], waves, inverse, keep)
                curl_y = waves[2] * sol[0] - waves[0] * sol[2]
                curl_z = waves[0] * sol[1] - waves[1] * sol[0]
                parts.append((sol, (curl_y, curl_z)))
            fields = []
            for c in range(2):
                turn = parts[1 - c][1]
                if c == 0:
                    turn = (-turn[0], -turn[1])
                sol = parts[c][0]
                fields.append((sol[1], sol[2], sol[0], turn[0], turn[1]))
            spot = lax.broadcasted_iota(jnp.int32, (DEPTH, 128), 1)
            for odd in range(2):
                ky = 2 * pair + odd
                for c in range(2):
                    for f in range(5):
                        value = fields[c][f]
                        if odd:
                            first = pltpu.roll(value[:, 128:256], 64, 1)
                            last = value[:, 256:]
                            edge = pltpu.roll(last, 64, 1)
                        else:
                            first = edge = value[:, :128]
                            last = pltpu.roll(value[:, 128:256], 64, 1)
                        base = jnp.where(spot < 64, first, last)
                        both = (
                            jnp.where(spot == 64, edge + last, base),
                            jnp.where(spot == 64, edge - last, base),
                        )
                        low = 768 * (f // 2) + 128 * ky + 64 * (f % 2)
                        cols = slice(128 * c, 128 * (c + 1))
                        for k in range(2):
                            part = both[(k + c) % 2]
                            data[k, low : low + 64, cols] = part[:64]
                            if f == 4:
                                data[k, low + 64 : low + 128, cols] = part[:64]
                            data64[k, 8 * f + ky : 8 * f + ky + 1, cols] = part[64:65]

    for copy in quarters:
        copy.wait()

    @pl.when(live)
    def _():
        dot = functools.partial(
            lax.dot_general,
            dimension_numbers=(((1,), (1,)), ((), ())),
            preferred_element_type=f32,
        )
        for c in range(2):
            high, low = split(data64[c])
            fine, rest = (tx_ref[k, 256 * c : 256 * (c + 1), :] for k in range(2))
            wide = dot(high, fine) + dot(low, fine) + dot(high, rest)
            for k in range(2):
                wide64[2 * c + k] = wide[:, 128 * k : 128 * (k + 1)]
        for d in range(PARTS):
            tile = jnp.zeros((8, 128), f32)
            for f in range(5):
                for c in range(2):
                    spot = 16 * f + 8 * c
                    part = wide64[2 * c + d // 16, 8 * f : 8 * f + 8, :]
                    shift = (spot - 8 * (d % 16)) % 128
                    if shift:
                        part = pltpu.roll(part, shift, 1)
                    tile = jnp.where((lane8 >= spot) & (lane8 < spot + 8), part, tile)
            ready[d, 0] = tile

        for group in range(3):
            for pair in range(3):
                low = 768 * group + 256 * pair
                for c in range(2):
                    wide = table_by_data(
                        tx_ref[:, 256 * c : 256 * (c + 1), :],
                        data[c, low : low + 256, :],
                        ((1,), (1,)),
                    )
                    for odd in range(2):
                        at = (2 * pair + odd) * STRIDE + 256 * c
                        made[group, at : at + 256, :] = wide[:, 128 * odd : 128 * (odd + 1)]

    pl.semaphore_wait(barrier, PARTS - 1)

    @pl.when(live)
    def _():
        for j, offset in others:
            device = peer(offset)
            remote(
                ready.at[flat(device), 0],
                arrived.at[0, me],
                send_sems.at[1],
                recv_sems.at[BAND],
                device,
            ).start()
        arrived[0, me] = ready[me, 0]

        def spread(x, carry):
            def fill(d, write):
                for group in range(3):
                    re, im = (
                        made[group, pl.ds(256 * c + 8 * d + x, BAND, stride=STRIDE), :]
                        for c in range(2)
                    )
                    if group == 2:
                        write(4, jnp.where(low6, re, im))
                    else:
                        write(2 * group, jnp.where(low6, re, pltpu.roll(im, 64, 1)))
                        write(2 * group + 1, jnp.where(low6, pltpu.roll(re, 64, 1), im))

            for j, offset in others:
                device = peer(offset)
                d = flat(device)

                def write(f, value):
                    ready[d, slot_of(f, x), :BAND, :] = value

                fill(d, write)
                first_copy(x, device).start()

            def keep_own(f, value):
                arrived[slot_of(f, x), me, :BAND, :] = value

            fill(me, keep_own)
            return carry

        lax.fori_loop(0, BAND, spread, 0)

    top[...] = jnp.zeros_like(top)
    total[...] = jnp.zeros_like(total)
    for copy in tabled:
        copy.wait()

    row = lax.broadcasted_iota(jnp.int32, (256, 128), 0)
    col = lax.broadcasted_iota(jnp.int32, (256, 128), 1)
    ky = signed(row // 8 * BAND + row % 8).astype(f32)
    kz = (col % 64).astype(f32)
    sign = jnp.where(col < 64, -1.0, 1.0)
    lane = lax.broadcasted_iota(jnp.int32, (GRID, 128), 1)
    lower = lane < 64

    def to_grid(x, pair, tiles):
        for odd in range(2):
            turns[:, 128 * odd : 128 * (odd + 1)] = tiles[odd]
        wide = table_by_data(ey_ref, turns[...], ((1,), (0,)))
        for odd in range(2):
            f = 2 * pair + odd
            cosine = wide[:GRID, 128 * odd : 128 * (odd + 1)]
            sine = pltpu.roll(wide[GRID:, 128 * odd : 128 * (odd + 1)], 64, 1)
            near = cosine + jnp.where(lower, -sine, sine)
            mine = (lane == 16 * f + x) | (lane == 16 * f + 8 + x)
            far = jnp.where(mine, strips64[...], 0.0)
            physical[f] = data_by_table(jnp.concatenate([near, far], axis=1), zt_ref)

    def from_live(await_count):
        pl.when(live)(lambda: await_count(len(LIVE) - 1))
        pl.when(jnp.logical_not(live))(lambda: await_count(len(LIVE)))

    def await_last(count):
        part = arrived.at[0, pl.ds(0, count)]
        remote(part, part, send_sems.at[1], recv_sems.at[BAND], (px, pz)).wait_recv()

    from_live(await_last)
    tile = arrived[0].reshape(256, 128)
    d = ky * pltpu.roll(tile, 64, 1) - 64.0 * pltpu.roll(tile, 80, 1)
    d = jnp.where(col < 88, -pltpu.roll(d, 120, 1), pltpu.roll(d, 8, 1))
    tile = jnp.where((col >= 80) & (col < 96), d, tile)
    wide = table_by_data(ey_ref, tile, ((1,), (0,)))
    strips64[...] = wide[:GRID] + jnp.where(
        lane // 8 % 2 == 0, -pltpu.roll(wide[GRID:], 120, 1), pltpu.roll(wide[GRID:], 8, 1)
    )
    back64[...] = jnp.zeros_like(back64)

    def plane(x, carry):
        def await_plane(count):
            part = arrived.at[pl.ds(1 + 5 * x, 5), pl.ds(0, count), pl.ds(0, BAND), :]
            remote(part, part, send_sems.at[0], recv_sems.at[x], (px, pz)).wait_recv()

        from_live(await_plane)
        tiles = [arrived[slot_of(f, x)].reshape(256, 128) for f in range(2)]
        to_grid(x, 0, tiles)
        turned = sign * pltpu.roll(ky * tiles[1] - kz * tiles[0], 64, 1)
        to_grid(x, 1, [arrived[slot_of(f, x)].reshape(256, 128) for f in (2, 3)])
        to_grid(x, 2, [arrived[slot_of(4, x)].reshape(256, 128), turned])
        u = [physical[f] for f in (2, 0, 1)]
        w = [physical[f] for f in (5, 3, 4)]
        speed = jnp.abs(u[0]) + jnp.abs(u[1]) + jnp.abs(u[2])
        squares = u[0] * u[0] + u[1] * u[1] + u[2] * u[2]
        top[...] = jnp.maximum(top[...], jnp.max(speed.reshape(24, 8, GRID), axis=0))
        total[...] += jnp.sum(squares.reshape(24, 8, GRID), axis=0)
        q = []
        for a in range(3):
            b, c = (a + 1) % 3, (a + 2) % 3
            q.append(data_by_table(u[b] * w[c] - u[c] * w[b], zb_ref))
            near = q[a][:, :128]
            far = pltpu.roll(near, 64, 1)
            back[:GRID, 128 * a : 128 * (a + 1)] = near
            back[GRID:, 128 * a : 128 * (a + 1)] = jnp.where(lower, far, -far)
        way = lane % 8 // 2
        chosen = jnp.where(way == 0, q[0][:, 128:], jnp.where(way == 1, q[1][:, 128:], q[2][:, 128:]))
        back64[:GRID] = jnp.where(lane // 8 == x, chosen, back64[:GRID])
        wide = table_by_data(eyt_ref, back[...], ((1,), (0,)))
        for a in range(3):
            closed[a, x] = wide[:, 128 * a : 128 * (a + 1)].reshape(len(LIVE), 8, 128)
        for j, offset in others:
            device = peer(offset)

            @pl.when(is_live(flat(device)))
            def _():
                remote(
                    closed.at[:, x, place(flat(device)), pl.ds(0, BAND), :],
                    out_hbm.at[:, x, me, pl.ds(0, BAND), :],
                    back_sems.at[0],
                    back_sems.at[1],
                    device,
                ).start()

        return carry

    lax.fori_loop(0, BAND, plane, 0)

    q = back64[:GRID]
    back64[GRID:] = jnp.where(lane % 2 == 0, pltpu.roll(q, 127, 1), -pltpu.roll(q, 1, 1))
    wide = table_by_data(eyt_ref, back64[...], ((1,), (0,)))
    closed64[...] = wide.reshape(len(LIVE), 8, 128)
    stat[...] = jnp.where(lane8 == 0, jnp.max(top[...]), jnp.sum(total[...]))

    def stat_copy(device):
        return remote(stat, stats_hbm.at[me], back_sems.at[2], back_sems.at[3], device)

    for j, offset in others:
        device = peer(offset)
        stat_copy(device).start()

        @pl.when(is_live(flat(device)))
        def _():
            remote(
                closed64.at[place(flat(device))],
                last_hbm.at[me],
                back_sems.at[4],
                back_sems.at[5],
                device,
            ).start()

    own = (
        pltpu.make_async_copy(
            closed.at[:, :, place(me), pl.ds(0, BAND), :],
            out_hbm.at[:, :, me, pl.ds(0, BAND), :],
            own_sems.at[0],
        ),
        pltpu.make_async_copy(closed64.at[place(me)], last_hbm.at[me], own_sems.at[1]),
    )
    stat_own = pltpu.make_async_copy(stat, stats_hbm.at[me], own_sems.at[2])
    stat_own.start()

    @pl.when(live)
    def _():
        own[0].start()
        own[1].start()
        own[0].wait()
        own[1].wait()

    stat_own.wait()

    def sent(part, sem):
        remote(part, part, sem, recv_sems.at[0], (px, pz)).wait_send()

    def came(part, sem):
        remote(part, part, send_sems.at[0], sem, (px, pz)).wait_recv()

    rest = pl.ds(0, PARTS - 1)

    def await_sent(count):
        sent(closed.at[:, :, pl.ds(0, count), pl.ds(0, BAND), :], back_sems.at[0])
        sent(closed64.at[pl.ds(0, count)], back_sems.at[4])

    from_live(await_sent)
    sent(arrived.at[0, rest], back_sems.at[2])
    came(stats_hbm.at[rest], back_sems.at[3])

    @pl.when(live)
    def _():
        sent(ready.at[rest, pl.ds(1, SLOTS - 1), pl.ds(0, BAND), :], send_sems.at[0])
        sent(ready.at[rest, 0], send_sems.at[1])
        came(out_hbm.at[:, :, rest, pl.ds(0, BAND), :], back_sems.at[1])
        came(last_hbm.at[rest], back_sems.at[5])


def close_kernel(
    cut_ref, dt_ref, power_ref, old_ref, in_ref, last_ref, stats_ref, cs_ref,
    out_ref, cfl_ref, energy_ref, terms, spectra,
):
    fastest = stats_ref[0]
    summed = stats_ref[0]
    for s in range(1, PARTS):
        fastest = jnp.maximum(fastest, stats_ref[s])
        summed = summed + stats_ref[s]
    fastest, summed = jnp.max(fastest[:, :1]), jnp.max(summed[:, 1:2])
    energy = 0.5 * summed * (1.0 / float(GRID**3))
    dt = dt_ref[0]
    cfl_ref[0] = dt * fastest * GRID * (1.0 / (2.0 * math.pi))
    energy_ref[0] = energy
    twice = jnp.maximum(jnp.full((DEPTH, 384), 2.0 * energy, f32), 0.5)
    forcing = power_ref[0] / twice
    eighth = lax.broadcasted_iota(jnp.int32, (PARTS, 128), 1) // 8

    out_ref[:, :, DEPTH:, :] = jnp.zeros((2, 3, 96 - DEPTH, 384), f32)

    pair = pl.program_id(0)
    live = is_live(lax.axis_index("py") * lax.axis_size("pz") + lax.axis_index("pz"))

    @pl.when(live)
    def _():
        for odd in range(2):
            ky = 2 * pair + odd
            for a in range(3):
                terms[128 * a : 128 * (a + 1), :] = in_ref[a, pl.ds(ky, GRID, stride=8), :].T
            last = last_ref[pl.ds(ky, PARTS, stride=8), :]
            apart = jnp.concatenate(
                [jnp.where(eighth == x, last, 0.0) for x in range(BAND)], axis=0
            )
            terms[384:432, :] = apart.T[:48]
            spectra[odd] = data_by_table(terms[...], cs_ref)
        waves, square, inverse, keep = pair_waves(pair, cut_ref)

        spot = lax.broadcasted_iota(jnp.int32, (DEPTH, 128), 1)

        def of_pair(a, c):
            found = []
            for odd in range(2):
                re, im = (
                    spectra[odd, 128 * a + 64 * k : 128 * a + 64 * (k + 1), :] for k in range(2)
                )
                last = spectra[odd, 384:392, :]
                for x in range(1, BAND):
                    last = last + spectra[odd, 384 + 8 * x : 392 + 8 * x, :]
                zeros = jnp.zeros((7, 256), f32)
                re = jnp.concatenate([re, last[2 * a : 2 * a + 1], zeros], axis=0)
                im = jnp.concatenate([im, last[2 * a + 1 : 2 * a + 2], zeros], axis=0)
                if c == 0:
                    one, other = re[:, :128], im[:, 128:]
                else:
                    one, other = im[:, :128], -re[:, 128:]
                found.append((one + other, jnp.where(spot == 64, one - other, one + other)))
            (even, even_low), (odd, odd_low) = found
            even_low, odd = pltpu.roll(even_low, 64, 1), pltpu.roll(odd, 64, 1)
            return jnp.concatenate(
                [even, jnp.where(spot < 64, even_low, odd), jnp.where(spot < 64, odd, odd_low)], axis=1
            )

        for c in range(2):
            old = project([old_ref[c, a, :, :] for a in range(3)], waves, inverse, keep)
            forced = project([of_pair(a, c) for a in range(3)], waves, inverse, keep)
            for a in range(3):
                out_ref[c, a, :DEPTH, :] = old[a] + dt * (
                    forced[a] + forcing * old[a] - viscosity * square * old[a]
                )

    @pl.when(jnp.logical_not(live))
    def _():
        out_ref[:, :, :DEPTH, :] = jnp.zeros((2, 3, DEPTH, 384), f32)


SM = pl.BlockSpec(memory_space=pltpu.SMEM)
ANY = pl.BlockSpec(memory_space=pl.ANY)
VMEM_BYTES = 60 * 1024 * 1024


def on_device(velocity_hat, time_step, power, cutoffs):
    tx, cs, ey, zt, zb, eyt = (jnp.asarray(t) for t in tables())
    shape = jax.ShapeDtypeStruct
    block = pl.BlockSpec((2, 3, DEPTH, 384), lambda i: (0, 0, 0, i))
    whole = lambda a: pl.BlockSpec(a.shape, lambda i: (0,) * a.ndim)
    dma = pltpu.SemaphoreType.DMA
    chunks, last, stats = pl.pallas_call(
        exchange_kernel,
        out_shape=(
            shape((3, BAND, PARTS, 8, 128), f32),
            shape((PARTS, 8, 128), f32),
            shape((PARTS, 8, 128), f32),
        ),
        in_specs=[SM] + [ANY] * 6,
        out_specs=(ANY, ANY, ANY),
        scratch_shapes=[
            pltpu.VMEM((3, 2, 3, DEPTH, 384), f32),
            pltpu.VMEM((2, 512, 256), bf16),
            *(pltpu.VMEM(t.shape, bf16) for t in (ey, zt, zb, eyt)),
            pltpu.VMEM((2, 2304, 256), f32),
            pltpu.VMEM((2, 40, 256), f32),
            pltpu.VMEM((4, 40, 128), f32),
            pltpu.VMEM((3, BAND * STRIDE, 128), f32),
            pltpu.VMEM((PARTS, SLOTS, 8, 128), f32),
            pltpu.VMEM((SLOTS, PARTS, 8, 128), f32),
            pltpu.VMEM((256, 256), f32),
            pltpu.VMEM((GRID, 128), f32),
            pltpu.VMEM((6, GRID, GRID), f32),
            pltpu.VMEM((2 * GRID, 384), f32),
            pltpu.VMEM((2 * GRID, 128), f32),
            pltpu.VMEM((3, BAND, len(LIVE), 8, 128), f32),
            pltpu.VMEM((len(LIVE), 8, 128), f32),
            pltpu.VMEM((8, GRID), f32),
            pltpu.VMEM((8, GRID), f32),
            pltpu.VMEM((8, 128), f32),
            dma((11,)),
            dma((2,)),
            dma((BAND + 1,)),
            dma((6,)),
            dma((3,)),
        ],
        compiler_params=pltpu.CompilerParams(
            collective_id=0, has_side_effects=True, vmem_limit_bytes=VMEM_BYTES
        ),
    )(cutoffs, velocity_hat, tx, ey, zt, zb, eyt)
    chunks = chunks.reshape(3, BAND * PARTS * 8, 128)
    last = last.reshape(PARTS * 8, 128)
    return pl.pallas_call(
        close_kernel,
        grid=(3,),
        out_shape=(shape((2, 3, 96, 1152), f32), shape((1,), f32), shape((1,), f32)),
        in_specs=[SM, SM, SM, block, whole(chunks), whole(last), whole(stats), whole(cs)],
        out_specs=(pl.BlockSpec((2, 3, 96, 384), lambda i: (0, 0, 0, i)), SM, SM),
        scratch_shapes=[pltpu.VMEM((432, GRID), f32), pltpu.VMEM((2, 432, 256), f32)],
        compiler_params=pltpu.CompilerParams(vmem_limit_bytes=VMEM_BYTES),
    )(cutoffs, time_step, power, velocity_hat, chunks, last, stats, cs)


def solution(mesh):
    return jax.shard_map(
        on_device,
        mesh=mesh,
        in_specs=(P("member", None, None, ("py", "pz")), P("member"), P("member"), P("member")),
        out_specs=(P("member", None, None, ("py", "pz")), P("member"), P("member")),
        check_vma=False,
    )
```

```python
import functools
import math

import jax
import jax.numpy as jnp
import ml_dtypes
import numpy as np
from jax import lax
from jax.experimental import pallas as pl
from jax.experimental.pallas import tpu as pltpu
from jax.sharding import PartitionSpec as P

GRID = 192
PARTS = 32
BAND = 6
DEPTH = 72
LIVE = tuple(range(11)) + tuple(range(21, 32))
viscosity = 0.004
f32 = jnp.float32
bf16 = jnp.bfloat16


def halves(table):
    high = table.astype(ml_dtypes.bfloat16)
    low = (table - high.astype(np.float64)).astype(ml_dtypes.bfloat16)
    return np.stack([high, low])


def angle(rows, cols):
    turns = np.outer(rows, cols) % GRID
    return turns * (2.0 * math.pi / GRID)


@functools.lru_cache
def tables():
    n = GRID
    every = np.arange(n)
    phase = angle(every, every)
    near = np.where(np.arange(128) <= 64, np.arange(128), np.arange(128) + 64)
    phase = angle(every, near)
    tx = np.zeros((PARTS, 8, 384))
    cosine, sine = (f(phase).reshape(PARTS, BAND, 128) for f in (np.cos, np.sin))
    for at, part in ((0, cosine), (128, sine), (256, -sine)):
        tx[:, :BAND, at : at + 128] = part
    tx = tx.reshape(256, 384)
    cs = np.zeros((n, 256))
    cs[:, :128] = cosine.transpose(1, 0, 2).reshape(n, 128)
    cs[:, 128:] = sine.transpose(1, 0, 2).reshape(n, 128)
    ey = np.zeros((2 * n, 256))
    eyt = np.zeros((8 * len(LIVE), 2 * n))
    for at, band in enumerate(LIVE):
        phase = angle(every, band * BAND + np.arange(BAND))
        cols = slice(8 * band, 8 * band + BAND)
        ey[:n, cols], ey[n:, cols] = np.cos(phase), np.sin(phase)
        rows = slice(8 * at, 8 * at + BAND)
        eyt[rows, :n], eyt[rows, n:] = np.cos(phase).T, np.sin(phase).T
    factor = float(n) ** -1.5
    phase = angle(np.arange(65), every)
    cosine, sine = factor * np.cos(phase), factor * np.sin(phase)
    zt = np.zeros((256, n))
    weight = np.where(np.arange(64) == 0, 1.0, 2.0)[:, None]
    zt[:64], zt[64:128] = weight * cosine[:64], -weight * sine[:64]
    for f in range(6):
        zt[128 + 16 * f : 136 + 16 * f] = 2.0 * cosine[64]
        zt[136 + 16 * f : 144 + 16 * f] = -2.0 * sine[64]
    zb = np.zeros((n, 256))
    zb[:, :64], zb[:, 64:128] = cosine[:64].T, -sine[:64].T
    for x in range(BAND):
        for a in range(3):
            zb[:, 128 + 8 * x + 2 * a] = cosine[64]
            zb[:, 128 + 8 * x + 2 * a + 1] = -sine[64]
    return tuple(halves(t) for t in (tx, cs, ey, zt, zb, eyt))


def split(value):
    high = value.astype(bf16)
    return high, (value - high.astype(f32)).astype(bf16)


def table_by_data(table, data, dims):
    high, low = split(data)
    dot = functools.partial(
        lax.dot_general, dimension_numbers=(dims, ((), ())), preferred_element_type=f32
    )
    return dot(table[0], high) + dot(table[0], low) + dot(table[1], high)


def data_by_table(data, table):
    high, low = split(data)
    dot = functools.partial(jnp.dot, preferred_element_type=f32)
    return dot(high, table[0]) + dot(low, table[0]) + dot(high, table[1])


def signed(index):
    return jnp.where(index < GRID // 2, index, index - GRID)


def pair_waves(pair, cut_ref):
    band = lax.axis_index("py") * lax.axis_size("pz") + lax.axis_index("pz")
    lane = lax.broadcasted_iota(jnp.int32, (DEPTH, 384), 1)
    upper = lane >= GRID
    kx = signed(jnp.where(upper, lane - GRID, lane))
    ky = signed(band * BAND + 2 * pair + upper.astype(jnp.int32))
    kz = lax.broadcasted_iota(jnp.int32, (DEPTH, 384), 0)
    keep = (
        (jnp.abs(kx) <= cut_ref[0]) & (jnp.abs(ky) <= cut_ref[1]) & (kz <= cut_ref[2])
    )
    waves = tuple(k.astype(f32) for k in (kx, ky, kz))
    square = waves[0] * waves[0] + waves[1] * waves[1] + waves[2] * waves[2]
    return waves, square, 1.0 / jnp.maximum(square, 1.0), keep


def project(field, waves, inverse, keep):
    normal = (waves[0] * field[0] + waves[1] * field[1] + waves[2] * field[2]) * inverse
    return [jnp.where(keep, field[a] - waves[a] * normal, 0.0) for a in range(3)]


MESH = pl.DeviceIdType.MESH
TURNS = ((1, 1), (3, 0), (2, 1), (0, 0), (1, 0), (3, 1), (2, 0), (0, 1))
OFFSETS = tuple(
    (dx, *TURNS[(k + 2 * j) % 8]) for k in range(8) for j, dx in enumerate((2, 1, 3, 0))
)


SLOTS = 31
STRIDE = 520


def slot_of(f, x):
    return 1 + 5 * x + f


def is_live(band):
    return (band < 11) | (band >= 21)


def exchange_kernel(
    cut_ref, in_hbm, tx_hbm, ey_hbm, zt_hbm, zb_hbm, eyt_hbm, out_hbm, last_hbm, stats_hbm,
    held, tx_ref, ey_ref, zt_ref, zb_ref, eyt_ref, data, data64, wide64, made, ready, arrived,
    turns, strips64, physical, back, back64, closed, closed64, top, total, stat,
    load_sems, send_sems, recv_sems, back_sems, own_sems,
):
    px, pz = lax.axis_index("py"), lax.axis_index("pz")
    me = px * 8 + pz
    live = is_live(me)

    def peer(offset):
        x = lax.rem(px + offset[0], 4)
        y = lax.rem(pz // 2 + offset[1], 4)
        z = lax.rem(pz % 2 + offset[2], 2)
        return x, y * 2 + z

    def flat(device):
        return device[0] * 8 + device[1]

    def place(band):
        return jnp.where(band < 11, band, band - 10)

    def remote(source, target, send, recv, device):
        return pltpu.make_async_remote_copy(
            src_ref=source,
            dst_ref=target,
            send_sem=send,
            recv_sem=recv,
            device_id={"py": device[0], "pz": device[1]},
            device_id_type=MESH,
        )

    others = [(j, offset) for j, offset in enumerate(OFFSETS) if offset != (0, 0, 0)]

    loads = [
        pltpu.make_async_copy(
            in_hbm.at[:, :, pl.ds(0, DEPTH), pl.ds(384 * p, 384)], held.at[p], load_sems.at[p]
        )
        for p in range(3)
    ]
    tabled = [
        pltpu.make_async_copy(source, target, load_sems.at[3 + k])
        for k, (source, target) in enumerate(
            ((ey_hbm, ey_ref), (zt_hbm, zt_ref), (zb_hbm, zb_ref), (eyt_hbm, eyt_ref))
        )
    ]
    quarters = [
        pltpu.make_async_copy(
            tx_hbm.at[:, :, pl.ds(low, 128)],
            tx_ref.at[:, pl.ds(256 * (k // 2), 256), pl.ds(128 * (k % 2), 128)],
            load_sems.at[7 + k],
        )
        for k, low in enumerate((0, 256, 128, 0))
    ]
    for copy in (*loads, *quarters, *tabled):
        copy.start()

    def clear(slot, carry):
        arrived[slot] = jnp.zeros((PARTS, 8, 128), f32)
        return carry

    lax.fori_loop(0, SLOTS, clear, 0)
    barrier = pltpu.get_barrier_semaphore()
    for _, offset in others:
        device = peer(offset)
        pl.semaphore_signal(
            barrier, inc=1, device_id={"py": device[0], "pz": device[1]}, device_id_type=MESH
        )

    def first_copy(x, device):
        slots = pl.ds(1 + 5 * x, 5)
        return remote(
            ready.at[flat(device), slots, pl.ds(0, BAND), :],
            arrived.at[slots, me, pl.ds(0, BAND), :],
            send_sems.at[0],
            recv_sems.at[x],
            device,
        )

    lane8 = lax.broadcasted_iota(jnp.int32, (8, 128), 1)
    low6 = lax.broadcasted_iota(jnp.int32, (BAND, 128), 1) < 64

    data64[...] = jnp.zeros_like(data64)
    for pair in range(3):
        loads[pair].wait()

        @pl.when(live)
        def _():
            waves, _, inverse, keep = pair_waves(pair, cut_ref)
            parts = []
            for c in range(2):
                sol = project([held[pair, c, a] for a in range(3)], waves, inverse, keep)
                curl_y = waves[2] * sol[0] - waves[0] * sol[2]
                curl_z = waves[0] * sol[1] - waves[1] * sol[0]
                parts.append((sol, (curl_y, curl_z)))
            fields = []
            for c in range(2):
                turn = parts[1 - c][1]
                if c == 0:
                    turn = (-turn[0], -turn[1])
                sol = parts[c][0]
                fields.append((sol[1], sol[2], sol[0], turn[0], turn[1]))
            spot = lax.broadcasted_iota(jnp.int32, (DEPTH, 128), 1)
            for odd in range(2):
                ky = 2 * pair + odd
                for c in range(2):
                    for f in range(5):
                        value = fields[c][f]
                        if odd:
                            first = pltpu.roll(value[:, 128:256], 64, 1)
                            last = value[:, 256:]
                            edge = pltpu.roll(last, 64, 1)
                        else:
                            first = edge = value[:, :128]
                            last = pltpu.roll(value[:, 128:256], 64, 1)
                        base = jnp.where(spot < 64, first, last)
                        both = (
                            jnp.where(spot == 64, edge + last, base),
                            jnp.where(spot == 64, edge - last, base),
                        )
                        low = 768 * (f // 2) + 128 * ky + 64 * (f % 2)
                        cols = slice(128 * c, 128 * (c + 1))
                        for k in range(2):
                            part = both[(k + c) % 2]
                            data[k, low : low + 64, cols] = part[:64]
                            if f == 4:
                                data[k, low + 64 : low + 128, cols] = part[:64]
                            data64[k, 8 * f + ky : 8 * f + ky + 1, cols] = part[64:65]

    for copy in quarters:
        copy.wait()

    @pl.when(live)
    def _():
        dot = functools.partial(
            lax.dot_general,
            dimension_numbers=(((1,), (1,)), ((), ())),
            preferred_element_type=f32,
        )
        for c in range(2):
            high, low = split(data64[c])
            fine, rest = (tx_ref[k, 256 * c : 256 * (c + 1), :] for k in range(2))
            wide = dot(high, fine) + dot(low, fine) + dot(high, rest)
            for k in range(2):
                wide64[2 * c + k] = wide[:, 128 * k : 128 * (k + 1)]
        for d in range(PARTS):
            tile = jnp.zeros((8, 128), f32)
            for f in range(5):
                for c in range(2):
                    spot = 16 * f + 8 * c
                    part = wide64[2 * c + d // 16, 8 * f : 8 * f + 8, :]
                    shift = (spot - 8 * (d % 16)) % 128
                    if shift:
                        part = pltpu.roll(part, shift, 1)
                    tile = jnp.where((lane8 >= spot) & (lane8 < spot + 8), part, tile)
            ready[d, 0] = tile

        for group in range(3):
            for pair in range(3):
                low = 768 * group + 256 * pair
                for c in range(2):
                    wide = table_by_data(
                        tx_ref[:, 256 * c : 256 * (c + 1), :],
                        data[c, low : low + 256, :],
                        ((1,), (1,)),
                    )
                    for odd in range(2):
                        at = (2 * pair + odd) * STRIDE + 256 * c
                        made[group, at : at + 256, :] = wide[:, 128 * odd : 128 * (odd + 1)]

    pl.semaphore_wait(barrier, PARTS - 1)

    @pl.when(live)
    def _():
        for j, offset in others:
            device = peer(offset)
            remote(
                ready.at[flat(device), 0, pl.ds(0, BAND), :],
                arrived.at[0, me, pl.ds(0, BAND), :],
                send_sems.at[1],
                recv_sems.at[BAND],
                device,
            ).start()
        arrived[0, me] = ready[me, 0]

        def spread(x, carry):
            def fill(d, write):
                for group in range(3):
                    re, im = (
                        made[group, pl.ds(256 * c + 8 * d + x, BAND, stride=STRIDE), :]
                        for c in range(2)
                    )
                    if group == 2:
                        write(4, jnp.where(low6, re, im))
                    else:
                        write(2 * group, jnp.where(low6, re, pltpu.roll(im, 64, 1)))
                        write(2 * group + 1, jnp.where(low6, pltpu.roll(re, 64, 1), im))

            for j, offset in others:
                device = peer(offset)
                d = flat(device)

                def write(f, value):
                    ready[d, slot_of(f, x), :BAND, :] = value

                fill(d, write)
                first_copy(x, device).start()

            def keep_own(f, value):
                arrived[slot_of(f, x), me, :BAND, :] = value

            fill(me, keep_own)
            return carry

        lax.fori_loop(0, BAND, spread, 0)

    top[...] = jnp.zeros_like(top)
    total[...] = jnp.zeros_like(total)
    for copy in tabled:
        copy.wait()

    row = lax.broadcasted_iota(jnp.int32, (256, 128), 0)
    col = lax.broadcasted_iota(jnp.int32, (256, 128), 1)
    ky = signed(row // 8 * BAND + row % 8).astype(f32)
    kz = (col % 64).astype(f32)
    sign = jnp.where(col < 64, -1.0, 1.0)
    lane = lax.broadcasted_iota(jnp.int32, (GRID, 128), 1)
    lower = lane < 64

    def to_grid(x, pair, tiles):
        for odd in range(2):
            turns[:, 128 * odd : 128 * (odd + 1)] = tiles[odd]
        wide = table_by_data(ey_ref, turns[...], ((1,), (0,)))
        for odd in range(2):
            f = 2 * pair + odd
            cosine = wide[:GRID, 128 * odd : 128 * (odd + 1)]
            sine = pltpu.roll(wide[GRID:, 128 * odd : 128 * (odd + 1)], 64, 1)
            near = cosine + jnp.where(lower, -sine, sine)
            mine = (lane == 16 * f + x) | (lane == 16 * f + 8 + x)
            far = jnp.where(mine, strips64[...], 0.0)
            physical[f] = data_by_table(jnp.concatenate([near, far], axis=1), zt_ref)

    def from_live(await_count):
        pl.when(live)(lambda: await_count(len(LIVE) - 1))
        pl.when(jnp.logical_not(live))(lambda: await_count(len(LIVE)))

    def await_last(count):
        part = arrived.at[0, pl.ds(0, count), pl.ds(0, BAND), :]
        remote(part, part, send_sems.at[1], recv_sems.at[BAND], (px, pz)).wait_recv()

    from_live(await_last)
    tile = arrived[0].reshape(256, 128)
    d = ky * pltpu.roll(tile, 64, 1) - 64.0 * pltpu.roll(tile, 80, 1)
    d = jnp.where(col < 88, -pltpu.roll(d, 120, 1), pltpu.roll(d, 8, 1))
    tile = jnp.where((col >= 80) & (col < 96), d, tile)
    wide = table_by_data(ey_ref, tile, ((1,), (0,)))
    strips64[...] = wide[:GRID] + jnp.where(
        lane // 8 % 2 == 0, -pltpu.roll(wide[GRID:], 120, 1), pltpu.roll(wide[GRID:], 8, 1)
    )
    back64[...] = jnp.zeros_like(back64)

    def plane(x, carry):
        def await_plane(count):
            part = arrived.at[pl.ds(1 + 5 * x, 5), pl.ds(0, count), pl.ds(0, BAND), :]
            remote(part, part, send_sems.at[0], recv_sems.at[x], (px, pz)).wait_recv()

        from_live(await_plane)
        tiles = [arrived[slot_of(f, x)].reshape(256, 128) for f in range(2)]
        to_grid(x, 0, tiles)
        turned = sign * pltpu.roll(ky * tiles[1] - kz * tiles[0], 64, 1)
        to_grid(x, 1, [arrived[slot_of(f, x)].reshape(256, 128) for f in (2, 3)])
        to_grid(x, 2, [arrived[slot_of(4, x)].reshape(256, 128), turned])
        u = [physical[f] for f in (2, 0, 1)]
        w = [physical[f] for f in (5, 3, 4)]
        speed = jnp.abs(u[0]) + jnp.abs(u[1]) + jnp.abs(u[2])
        squares = u[0] * u[0] + u[1] * u[1] + u[2] * u[2]
        top[...] = jnp.maximum(top[...], jnp.max(speed.reshape(24, 8, GRID), axis=0))
        total[...] += jnp.sum(squares.reshape(24, 8, GRID), axis=0)
        q = []
        for a in range(3):
            b, c = (a + 1) % 3, (a + 2) % 3
            q.append(data_by_table(u[b] * w[c] - u[c] * w[b], zb_ref))
            near = q[a][:, :128]
            far = pltpu.roll(near, 64, 1)
            back[:GRID, 128 * a : 128 * (a + 1)] = near
            back[GRID:, 128 * a : 128 * (a + 1)] = jnp.where(lower, far, -far)
        way = lane % 8 // 2
        chosen = jnp.where(way == 0, q[0][:, 128:], jnp.where(way == 1, q[1][:, 128:], q[2][:, 128:]))
        back64[:GRID] = jnp.where(lane // 8 == x, chosen, back64[:GRID])
        wide = table_by_data(eyt_ref, back[...], ((1,), (0,)))
        for a in range(3):
            closed[a, x] = wide[:, 128 * a : 128 * (a + 1)].reshape(len(LIVE), 8, 128)
        for j, offset in others:
            device = peer(offset)

            @pl.when(is_live(flat(device)))
            def _():
                remote(
                    closed.at[:, x, place(flat(device)), pl.ds(0, BAND), :],
                    out_hbm.at[:, x, me, pl.ds(0, BAND), :],
                    back_sems.at[0],
                    back_sems.at[1],
                    device,
                ).start()

        return carry

    lax.fori_loop(0, BAND, plane, 0)

    q = back64[:GRID]
    back64[GRID:] = jnp.where(lane % 2 == 0, pltpu.roll(q, 127, 1), -pltpu.roll(q, 1, 1))
    wide = table_by_data(eyt_ref, back64[...], ((1,), (0,)))
    closed64[...] = wide.reshape(len(LIVE), 8, 128)
    stat[...] = jnp.where(lane8[:1] == 0, jnp.max(top[...]), jnp.sum(total[...]))

    def stat_copy(device):
        return remote(stat, stats_hbm.at[me], back_sems.at[2], back_sems.at[3], device)

    for j, offset in others:
        device = peer(offset)
        stat_copy(device).start()

        @pl.when(is_live(flat(device)))
        def _():
            remote(
                closed64.at[place(flat(device)), pl.ds(0, BAND), :],
                last_hbm.at[me, pl.ds(0, BAND), :],
                back_sems.at[4],
                back_sems.at[5],
                device,
            ).start()

    own = (
        pltpu.make_async_copy(
            closed.at[:, :, place(me), pl.ds(0, BAND), :],
            out_hbm.at[:, :, me, pl.ds(0, BAND), :],
            own_sems.at[0],
        ),
        pltpu.make_async_copy(closed64.at[place(me)], last_hbm.at[me], own_sems.at[1]),
    )
    stat_own = pltpu.make_async_copy(stat, stats_hbm.at[me], own_sems.at[2])
    stat_own.start()

    @pl.when(live)
    def _():
        own[0].start()
        own[1].start()
        own[0].wait()
        own[1].wait()

    stat_own.wait()

    def sent(part, sem):
        remote(part, part, sem, recv_sems.at[0], (px, pz)).wait_send()

    def came(part, sem):
        remote(part, part, send_sems.at[0], sem, (px, pz)).wait_recv()

    rest = pl.ds(0, PARTS - 1)

    def await_sent(count):
        sent(closed.at[:, :, pl.ds(0, count), pl.ds(0, BAND), :], back_sems.at[0])
        sent(closed64.at[pl.ds(0, count), pl.ds(0, BAND), :], back_sems.at[4])

    from_live(await_sent)
    sent(arrived.at[0, rest, pl.ds(0, 1), :], back_sems.at[2])
    came(stats_hbm.at[rest], back_sems.at[3])

    @pl.when(live)
    def _():
        sent(ready.at[rest, pl.ds(1, SLOTS - 1), pl.ds(0, BAND), :], send_sems.at[0])
        sent(ready.at[rest, 0, pl.ds(0, BAND), :], send_sems.at[1])
        came(out_hbm.at[:, :, rest, pl.ds(0, BAND), :], back_sems.at[1])
        came(last_hbm.at[rest, pl.ds(0, BAND), :], back_sems.at[5])


def close_kernel(
    cut_ref, dt_ref, power_ref, old_ref, in_ref, last_ref, stats_ref, cs_ref,
    out_ref, cfl_ref, energy_ref, terms, spectra,
):
    fastest = stats_ref[0]
    summed = stats_ref[0]
    for s in range(1, PARTS):
        fastest = jnp.maximum(fastest, stats_ref[s])
        summed = summed + stats_ref[s]
    fastest, summed = jnp.max(fastest[:, :1]), jnp.max(summed[:, 1:2])
    energy = 0.5 * summed * (1.0 / float(GRID**3))
    dt = dt_ref[0]
    cfl_ref[0] = dt * fastest * GRID * (1.0 / (2.0 * math.pi))
    energy_ref[0] = energy
    twice = jnp.maximum(jnp.full((DEPTH, 384), 2.0 * energy, f32), 0.5)
    forcing = power_ref[0] / twice
    eighth = lax.broadcasted_iota(jnp.int32, (PARTS, 128), 1) // 8

    out_ref[:, :, DEPTH:, :] = jnp.zeros((2, 3, 96 - DEPTH, 384), f32)

    pair = pl.program_id(0)
    live = is_live(lax.axis_index("py") * lax.axis_size("pz") + lax.axis_index("pz"))

    @pl.when(live)
    def _():
        for odd in range(2):
            ky = 2 * pair + odd
            for a in range(3):
                terms[128 * a : 128 * (a + 1), :] = in_ref[a, pl.ds(ky, GRID, stride=8), :].T
            last = last_ref[pl.ds(ky, PARTS, stride=8), :]
            apart = jnp.concatenate(
                [jnp.where(eighth == x, last, 0.0) for x in range(BAND)], axis=0
            )
            terms[384:432, :] = apart.T[:48]
            spectra[odd] = data_by_table(terms[...], cs_ref)
        waves, square, inverse, keep = pair_waves(pair, cut_ref)

        spot = lax.broadcasted_iota(jnp.int32, (DEPTH, 128), 1)

        def of_pair(a, c):
            found = []
            for odd in range(2):
                re, im = (
                    spectra[odd, 128 * a + 64 * k : 128 * a + 64 * (k + 1), :] for k in range(2)
                )
                last = spectra[odd, 384:392, :]
                for x in range(1, BAND):
                    last = last + spectra[odd, 384 + 8 * x : 392 + 8 * x, :]
                zeros = jnp.zeros((7, 256), f32)
                re = jnp.concatenate([re, last[2 * a : 2 * a + 1], zeros], axis=0)
                im = jnp.concatenate([im, last[2 * a + 1 : 2 * a + 2], zeros], axis=0)
                if c == 0:
                    one, other = re[:, :128], im[:, 128:]
                else:
                    one, other = im[:, :128], -re[:, 128:]
                found.append((one + other, jnp.where(spot == 64, one - other, one + other)))
            (even, even_low), (odd, odd_low) = found
            even_low, odd = pltpu.roll(even_low, 64, 1), pltpu.roll(odd, 64, 1)
            return jnp.concatenate(
                [even, jnp.where(spot < 64, even_low, odd), jnp.where(spot < 64, odd, odd_low)], axis=1
            )

        for c in range(2):
            old = project([old_ref[c, a, :, :] for a in range(3)], waves, inverse, keep)
            forced = project([of_pair(a, c) for a in range(3)], waves, inverse, keep)
            for a in range(3):
                out_ref[c, a, :DEPTH, :] = old[a] + dt * (
                    forced[a] + forcing * old[a] - viscosity * square * old[a]
                )

    @pl.when(jnp.logical_not(live))
    def _():
        out_ref[:, :, :DEPTH, :] = jnp.zeros((2, 3, DEPTH, 384), f32)


SM = pl.BlockSpec(memory_space=pltpu.SMEM)
ANY = pl.BlockSpec(memory_space=pl.ANY)
VMEM_BYTES = 60 * 1024 * 1024


def on_device(velocity_hat, time_step, power, cutoffs):
    tx, cs, ey, zt, zb, eyt = (jnp.asarray(t) for t in tables())
    shape = jax.ShapeDtypeStruct
    block = pl.BlockSpec((2, 3, DEPTH, 384), lambda i: (0, 0, 0, i))
    whole = lambda a: pl.BlockSpec(a.shape, lambda i: (0,) * a.ndim)
    dma = pltpu.SemaphoreType.DMA
    chunks, last, stats = pl.pallas_call(
        exchange_kernel,
        out_shape=(
            shape((3, BAND, PARTS, 8, 128), f32),
            shape((PARTS, 8, 128), f32),
            shape((PARTS, 1, 128), f32),
        ),
        in_specs=[SM] + [ANY] * 6,
        out_specs=(ANY, ANY, ANY),
        scratch_shapes=[
            pltpu.VMEM((3, 2, 3, DEPTH, 384), f32),
            pltpu.VMEM((2, 512, 256), bf16),
            *(pltpu.VMEM(t.shape, bf16) for t in (ey, zt, zb, eyt)),
            pltpu.VMEM((2, 2304, 256), f32),
            pltpu.VMEM((2, 40, 256), f32),
            pltpu.VMEM((4, 40, 128), f32),
            pltpu.VMEM((3, BAND * STRIDE, 128), f32),
            pltpu.VMEM((PARTS, SLOTS, 8, 128), f32),
            pltpu.VMEM((SLOTS, PARTS, 8, 128), f32),
            pltpu.VMEM((256, 256), f32),
            pltpu.VMEM((GRID, 128), f32),
            pltpu.VMEM((6, GRID, GRID), f32),
            pltpu.VMEM((2 * GRID, 384), f32),
            pltpu.VMEM((2 * GRID, 128), f32),
            pltpu.VMEM((3, BAND, len(LIVE), 8, 128), f32),
            pltpu.VMEM((len(LIVE), 8, 128), f32),
            pltpu.VMEM((8, GRID), f32),
            pltpu.VMEM((8, GRID), f32),
            pltpu.VMEM((1, 128), f32),
            dma((11,)),
            dma((2,)),
            dma((BAND + 1,)),
            dma((6,)),
            dma((3,)),
        ],
        compiler_params=pltpu.CompilerParams(
            collective_id=0, has_side_effects=True, vmem_limit_bytes=VMEM_BYTES
        ),
    )(cutoffs, velocity_hat, tx, ey, zt, zb, eyt)
    chunks = chunks.reshape(3, BAND * PARTS * 8, 128)
    last = last.reshape(PARTS * 8, 128)
    return pl.pallas_call(
        close_kernel,
        grid=(3,),
        out_shape=(shape((2, 3, 96, 1152), f32), shape((1,), f32), shape((1,), f32)),
        in_specs=[SM, SM, SM, block, whole(chunks), whole(last), whole(stats), whole(cs)],
        out_specs=(pl.BlockSpec((2, 3, 96, 384), lambda i: (0, 0, 0, i)), SM, SM),
        scratch_shapes=[pltpu.VMEM((432, GRID), f32), pltpu.VMEM((2, 432, 256), f32)],
        compiler_params=pltpu.CompilerParams(vmem_limit_bytes=VMEM_BYTES),
    )(cutoffs, time_step, power, velocity_hat, chunks, last, stats, cs)


def solution(mesh):
    return jax.shard_map(
        on_device,
        mesh=mesh,
        in_specs=(P("member", None, None, ("py", "pz")), P("member"), P("member"), P("member")),
        out_specs=(P("member", None, None, ("py", "pz")), P("member"), P("member")),
        check_vma=False,
    )
```

```python
import functools
import math

import jax
import jax.numpy as jnp
import ml_dtypes
import numpy as np
from jax import lax
from jax.experimental import pallas as pl
from jax.experimental.pallas import tpu as pltpu
from jax.sharding import PartitionSpec as P

GRID = 192
PARTS = 32
BAND = 6
DEPTH = 72
LIVE = tuple(range(11)) + tuple(range(21, 32))
viscosity = 0.004
f32 = jnp.float32
bf16 = jnp.bfloat16


def halves(table):
    high = table.astype(ml_dtypes.bfloat16)
    low = (table - high.astype(np.float64)).astype(ml_dtypes.bfloat16)
    return np.stack([high, low])


def angle(rows, cols):
    turns = np.outer(rows, cols) % GRID
    return turns * (2.0 * math.pi / GRID)


@functools.lru_cache
def tables():
    n = GRID
    every = np.arange(n)
    phase = angle(every, every)
    near = np.where(np.arange(128) <= 64, np.arange(128), np.arange(128) + 64)
    phase = angle(every, near)
    tx = np.zeros((PARTS, 8, 384))
    cosine, sine = (f(phase).reshape(PARTS, BAND, 128) for f in (np.cos, np.sin))
    for at, part in ((0, cosine), (128, sine), (256, -sine)):
        tx[:, :BAND, at : at + 128] = part
    tx = tx.reshape(256, 384)
    cs = np.zeros((n, 256))
    cs[:, :128] = cosine.transpose(1, 0, 2).reshape(n, 128)
    cs[:, 128:] = sine.transpose(1, 0, 2).reshape(n, 128)
    ey = np.zeros((2 * n, 256))
    eyt = np.zeros((8 * len(LIVE), 2 * n))
    for at, band in enumerate(LIVE):
        phase = angle(every, band * BAND + np.arange(BAND))
        cols = slice(8 * band, 8 * band + BAND)
        ey[:n, cols], ey[n:, cols] = np.cos(phase), np.sin(phase)
        rows = slice(8 * at, 8 * at + BAND)
        eyt[rows, :n], eyt[rows, n:] = np.cos(phase).T, np.sin(phase).T
    factor = float(n) ** -1.5
    phase = angle(np.arange(65), every)
    cosine, sine = factor * np.cos(phase), factor * np.sin(phase)
    zt = np.zeros((256, n))
    weight = np.where(np.arange(64) == 0, 1.0, 2.0)[:, None]
    zt[:64], zt[64:128] = weight * cosine[:64], -weight * sine[:64]
    for f in range(6):
        zt[128 + 16 * f : 136 + 16 * f] = 2.0 * cosine[64]
        zt[136 + 16 * f : 144 + 16 * f] = -2.0 * sine[64]
    zb = np.zeros((n, 256))
    zb[:, :64], zb[:, 64:128] = cosine[:64].T, -sine[:64].T
    for x in range(BAND):
        for a in range(3):
            zb[:, 128 + 8 * x + 2 * a] = cosine[64]
            zb[:, 128 + 8 * x + 2 * a + 1] = -sine[64]
    return tuple(halves(t) for t in (tx, cs, ey, zt, zb, eyt))


def split(value):
    high = value.astype(bf16)
    return high, (value - high.astype(f32)).astype(bf16)


def table_by_data(table, data, dims):
    high, low = split(data)
    dot = functools.partial(
        lax.dot_general, dimension_numbers=(dims, ((), ())), preferred_element_type=f32
    )
    return dot(table[0], high) + dot(table[0], low) + dot(table[1], high)


def data_by_table(data, table):
    high, low = split(data)
    dot = functools.partial(jnp.dot, preferred_element_type=f32)
    return dot(high, table[0]) + dot(low, table[0]) + dot(high, table[1])


def signed(index):
    return jnp.where(index < GRID // 2, index, index - GRID)


def pair_waves(pair, cut_ref):
    band = lax.axis_index("py") * lax.axis_size("pz") + lax.axis_index("pz")
    lane = lax.broadcasted_iota(jnp.int32, (DEPTH, 384), 1)
    upper = lane >= GRID
    kx = signed(jnp.where(upper, lane - GRID, lane))
    ky = signed(band * BAND + 2 * pair + upper.astype(jnp.int32))
    kz = lax.broadcasted_iota(jnp.int32, (DEPTH, 384), 0)
    keep = (
        (jnp.abs(kx) <= cut_ref[0]) & (jnp.abs(ky) <= cut_ref[1]) & (kz <= cut_ref[2])
    )
    waves = tuple(k.astype(f32) for k in (kx, ky, kz))
    square = waves[0] * waves[0] + waves[1] * waves[1] + waves[2] * waves[2]
    return waves, square, 1.0 / jnp.maximum(square, 1.0), keep


def project(field, waves, inverse, keep):
    normal = (waves[0] * field[0] + waves[1] * field[1] + waves[2] * field[2]) * inverse
    return [jnp.where(keep, field[a] - waves[a] * normal, 0.0) for a in range(3)]


MESH = pl.DeviceIdType.MESH
TURNS = ((1, 1), (3, 0), (2, 1), (0, 0), (1, 0), (3, 1), (2, 0), (0, 1))
OFFSETS = tuple(
    (dx, *TURNS[(k + 2 * j) % 8]) for k in range(8) for j, dx in enumerate((2, 1, 3, 0))
)


SLOTS = 31
STRIDE = 520
AHEAD = 3


def slot_of(f, x):
    return 1 + 5 * x + f


def is_live(band):
    return (band < 11) | (band >= 21)


def exchange_kernel(
    cut_ref, in_hbm, tx_hbm, ey_hbm, zt_hbm, zb_hbm, eyt_hbm, out_hbm, last_hbm, stats_hbm,
    held, tx_ref, ey_ref, zt_ref, zb_ref, eyt_ref, data, data64, wide64, made, ready, arrived,
    turns, strips64, physical, back, back64, closed, closed64, top, total, stat,
    load_sems, send_sems, recv_sems, back_sems, own_sems,
):
    px, pz = lax.axis_index("py"), lax.axis_index("pz")
    me = px * 8 + pz
    live = is_live(me)

    def peer(offset):
        x = lax.rem(px + offset[0], 4)
        y = lax.rem(pz // 2 + offset[1], 4)
        z = lax.rem(pz % 2 + offset[2], 2)
        return x, y * 2 + z

    def flat(device):
        return device[0] * 8 + device[1]

    def place(band):
        return jnp.where(band < 11, band, band - 10)

    def remote(source, target, send, recv, device):
        return pltpu.make_async_remote_copy(
            src_ref=source,
            dst_ref=target,
            send_sem=send,
            recv_sem=recv,
            device_id={"py": device[0], "pz": device[1]},
            device_id_type=MESH,
        )

    others = [(j, offset) for j, offset in enumerate(OFFSETS) if offset != (0, 0, 0)]

    loads = [
        pltpu.make_async_copy(
            in_hbm.at[:, :, pl.ds(0, DEPTH), pl.ds(384 * p, 384)], held.at[p], load_sems.at[p]
        )
        for p in range(3)
    ]
    tabled = [
        pltpu.make_async_copy(source, target, load_sems.at[3 + k])
        for k, (source, target) in enumerate(
            ((ey_hbm, ey_ref), (zt_hbm, zt_ref), (zb_hbm, zb_ref), (eyt_hbm, eyt_ref))
        )
    ]
    quarters = [
        pltpu.make_async_copy(
            tx_hbm.at[:, :, pl.ds(low, 128)],
            tx_ref.at[:, pl.ds(256 * (k // 2), 256), pl.ds(128 * (k % 2), 128)],
            load_sems.at[7 + k],
        )
        for k, low in enumerate((0, 256, 128, 0))
    ]
    for copy in (*loads, *quarters, *tabled):
        copy.start()

    def clear(slot, carry):
        arrived[slot] = jnp.zeros((PARTS, 8, 128), f32)
        return carry

    lax.fori_loop(0, SLOTS, clear, 0)
    barrier = pltpu.get_barrier_semaphore()
    for _, offset in others:
        device = peer(offset)
        pl.semaphore_signal(
            barrier, inc=1, device_id={"py": device[0], "pz": device[1]}, device_id_type=MESH
        )

    def first_copy(x, device):
        slots = pl.ds(1 + 5 * x, 5)
        return remote(
            ready.at[flat(device), slots, pl.ds(0, BAND), :],
            arrived.at[slots, me, pl.ds(0, BAND), :],
            send_sems.at[0],
            recv_sems.at[x],
            device,
        )

    lane8 = lax.broadcasted_iota(jnp.int32, (8, 128), 1)
    low6 = lax.broadcasted_iota(jnp.int32, (BAND, 128), 1) < 64

    data64[...] = jnp.zeros_like(data64)
    for pair in range(3):
        loads[pair].wait()

        @pl.when(live)
        def _():
            waves, _, inverse, keep = pair_waves(pair, cut_ref)
            parts = []
            for c in range(2):
                sol = project([held[pair, c, a] for a in range(3)], waves, inverse, keep)
                curl_y = waves[2] * sol[0] - waves[0] * sol[2]
                curl_z = waves[0] * sol[1] - waves[1] * sol[0]
                parts.append((sol, (curl_y, curl_z)))
            fields = []
            for c in range(2):
                turn = parts[1 - c][1]
                if c == 0:
                    turn = (-turn[0], -turn[1])
                sol = parts[c][0]
                fields.append((sol[1], sol[2], sol[0], turn[0], turn[1]))
            spot = lax.broadcasted_iota(jnp.int32, (DEPTH, 128), 1)
            for odd in range(2):
                ky = 2 * pair + odd
                for c in range(2):
                    for f in range(5):
                        value = fields[c][f]
                        if odd:
                            first = pltpu.roll(value[:, 128:256], 64, 1)
                            last = value[:, 256:]
                            edge = pltpu.roll(last, 64, 1)
                        else:
                            first = edge = value[:, :128]
                            last = pltpu.roll(value[:, 128:256], 64, 1)
                        base = jnp.where(spot < 64, first, last)
                        both = (
                            jnp.where(spot == 64, edge + last, base),
                            jnp.where(spot == 64, edge - last, base),
                        )
                        low = 768 * (f // 2) + 128 * ky + 64 * (f % 2)
                        cols = slice(128 * c, 128 * (c + 1))
                        for k in range(2):
                            part = both[(k + c) % 2]
                            data[k, low : low + 64, cols] = part[:64]
                            if f == 4:
                                data[k, low + 64 : low + 128, cols] = part[:64]
                            data64[k, 8 * f + ky : 8 * f + ky + 1, cols] = part[64:65]

    for copy in quarters:
        copy.wait()

    @pl.when(live)
    def _():
        dot = functools.partial(
            lax.dot_general,
            dimension_numbers=(((1,), (1,)), ((), ())),
            preferred_element_type=f32,
        )
        for c in range(2):
            high, low = split(data64[c])
            fine, rest = (tx_ref[k, 256 * c : 256 * (c + 1), :] for k in range(2))
            wide = dot(high, fine) + dot(low, fine) + dot(high, rest)
            for k in range(2):
                wide64[2 * c + k] = wide[:, 128 * k : 128 * (k + 1)]
        for d in range(PARTS):
            tile = jnp.zeros((8, 128), f32)
            for f in range(5):
                for c in range(2):
                    spot = 16 * f + 8 * c
                    part = wide64[2 * c + d // 16, 8 * f : 8 * f + 8, :]
                    shift = (spot - 8 * (d % 16)) % 128
                    if shift:
                        part = pltpu.roll(part, shift, 1)
                    tile = jnp.where((lane8 >= spot) & (lane8 < spot + 8), part, tile)
            ready[d, 0] = tile

        for group in range(3):
            for pair in range(3):
                low = 768 * group + 256 * pair
                for c in range(2):
                    wide = table_by_data(
                        tx_ref[:, 256 * c : 256 * (c + 1), :],
                        data[c, low : low + 256, :],
                        ((1,), (1,)),
                    )
                    for odd in range(2):
                        at = (2 * pair + odd) * STRIDE + 256 * c
                        made[group, at : at + 256, :] = wide[:, 128 * odd : 128 * (odd + 1)]

    def spread(x, carry):
        def fill(d, write):
            for group in range(3):
                re, im = (
                    made[group, pl.ds(256 * c + 8 * d + x, BAND, stride=STRIDE), :]
                    for c in range(2)
                )
                if group == 2:
                    write(4, jnp.where(low6, re, im))
                else:
                    write(2 * group, jnp.where(low6, re, pltpu.roll(im, 64, 1)))
                    write(2 * group + 1, jnp.where(low6, pltpu.roll(re, 64, 1), im))

        for j, offset in others:
            device = peer(offset)
            d = flat(device)

            def write(f, value):
                ready[d, slot_of(f, x), :BAND, :] = value

            fill(d, write)
            first_copy(x, device).start()

        def keep_own(f, value):
            arrived[slot_of(f, x), me, :BAND, :] = value

        fill(me, keep_own)
        return carry

    pl.semaphore_wait(barrier, PARTS - 1)

    @pl.when(live)
    def _():
        for j, offset in others:
            device = peer(offset)
            remote(
                ready.at[flat(device), 0, pl.ds(0, BAND), :],
                arrived.at[0, me, pl.ds(0, BAND), :],
                send_sems.at[1],
                recv_sems.at[BAND],
                device,
            ).start()
        arrived[0, me] = ready[me, 0]

        lax.fori_loop(0, AHEAD, spread, 0)

    top[...] = jnp.zeros_like(top)
    total[...] = jnp.zeros_like(total)
    for copy in tabled:
        copy.wait()

    row = lax.broadcasted_iota(jnp.int32, (256, 128), 0)
    col = lax.broadcasted_iota(jnp.int32, (256, 128), 1)
    ky = signed(row // 8 * BAND + row % 8).astype(f32)
    kz = (col % 64).astype(f32)
    sign = jnp.where(col < 64, -1.0, 1.0)
    lane = lax.broadcasted_iota(jnp.int32, (GRID, 128), 1)
    lower = lane < 64

    def to_grid(x, pair, tiles):
        for odd in range(2):
            turns[:, 128 * odd : 128 * (odd + 1)] = tiles[odd]
        wide = table_by_data(ey_ref, turns[...], ((1,), (0,)))
        for odd in range(2):
            f = 2 * pair + odd
            cosine = wide[:GRID, 128 * odd : 128 * (odd + 1)]
            sine = pltpu.roll(wide[GRID:, 128 * odd : 128 * (odd + 1)], 64, 1)
            near = cosine + jnp.where(lower, -sine, sine)
            mine = (lane == 16 * f + x) | (lane == 16 * f + 8 + x)
            far = jnp.where(mine, strips64[...], 0.0)
            physical[f] = data_by_table(jnp.concatenate([near, far], axis=1), zt_ref)

    def from_live(await_count):
        pl.when(live)(lambda: await_count(len(LIVE) - 1))
        pl.when(jnp.logical_not(live))(lambda: await_count(len(LIVE)))

    def await_last(count):
        part = arrived.at[0, pl.ds(0, count), pl.ds(0, BAND), :]
        remote(part, part, send_sems.at[1], recv_sems.at[BAND], (px, pz)).wait_recv()

    from_live(await_last)
    tile = arrived[0].reshape(256, 128)
    d = ky * pltpu.roll(tile, 64, 1) - 64.0 * pltpu.roll(tile, 80, 1)
    d = jnp.where(col < 88, -pltpu.roll(d, 120, 1), pltpu.roll(d, 8, 1))
    tile = jnp.where((col >= 80) & (col < 96), d, tile)
    wide = table_by_data(ey_ref, tile, ((1,), (0,)))
    strips64[...] = wide[:GRID] + jnp.where(
        lane // 8 % 2 == 0, -pltpu.roll(wide[GRID:], 120, 1), pltpu.roll(wide[GRID:], 8, 1)
    )
    back64[...] = jnp.zeros_like(back64)

    def plane(x, carry):
        def await_plane(count):
            part = arrived.at[pl.ds(1 + 5 * x, 5), pl.ds(0, count), pl.ds(0, BAND), :]
            remote(part, part, send_sems.at[0], recv_sems.at[x], (px, pz)).wait_recv()

        from_live(await_plane)
        pl.when(live & (x + AHEAD < BAND))(lambda: spread(x + AHEAD, None))
        tiles = [arrived[slot_of(f, x)].reshape(256, 128) for f in range(2)]
        to_grid(x, 0, tiles)
        turned = sign * pltpu.roll(ky * tiles[1] - kz * tiles[0], 64, 1)
        to_grid(x, 1, [arrived[slot_of(f, x)].reshape(256, 128) for f in (2, 3)])
        to_grid(x, 2, [arrived[slot_of(4, x)].reshape(256, 128), turned])
        u = [physical[f] for f in (2, 0, 1)]
        w = [physical[f] for f in (5, 3, 4)]
        speed = jnp.abs(u[0]) + jnp.abs(u[1]) + jnp.abs(u[2])
        squares = u[0] * u[0] + u[1] * u[1] + u[2] * u[2]
        top[...] = jnp.maximum(top[...], jnp.max(speed.reshape(24, 8, GRID), axis=0))
        total[...] += jnp.sum(squares.reshape(24, 8, GRID), axis=0)
        q = []
        for a in range(3):
            b, c = (a + 1) % 3, (a + 2) % 3
            q.append(data_by_table(u[b] * w[c] - u[c] * w[b], zb_ref))
            near = q[a][:, :128]
            far = pltpu.roll(near, 64, 1)
            back[:GRID, 128 * a : 128 * (a + 1)] = near
            back[GRID:, 128 * a : 128 * (a + 1)] = jnp.where(lower, far, -far)
        way = lane % 8 // 2
        chosen = jnp.where(way == 0, q[0][:, 128:], jnp.where(way == 1, q[1][:, 128:], q[2][:, 128:]))
        back64[:GRID] = jnp.where(lane // 8 == x, chosen, back64[:GRID])
        wide = table_by_data(eyt_ref, back[...], ((1,), (0,)))
        for a in range(3):
            closed[a, x] = wide[:, 128 * a : 128 * (a + 1)].reshape(len(LIVE), 8, 128)
        for j, offset in others:
            device = peer(offset)

            @pl.when(is_live(flat(device)))
            def _():
                remote(
                    closed.at[:, x, place(flat(device)), pl.ds(0, BAND), :],
                    out_hbm.at[:, x, me, pl.ds(0, BAND), :],
                    back_sems.at[0],
                    back_sems.at[1],
                    device,
                ).start()

        return carry

    lax.fori_loop(0, BAND, plane, 0)

    stat[...] = jnp.where(lane8[:1] == 0, jnp.max(top[...]), jnp.sum(total[...]))

    def stat_copy(device):
        return remote(stat, stats_hbm.at[me], back_sems.at[2], back_sems.at[3], device)

    for _, offset in others:
        stat_copy(peer(offset)).start()

    q = back64[:GRID]
    back64[GRID:] = jnp.where(lane % 2 == 0, pltpu.roll(q, 127, 1), -pltpu.roll(q, 1, 1))
    wide = table_by_data(eyt_ref, back64[...], ((1,), (0,)))
    closed64[...] = wide.reshape(len(LIVE), 8, 128)

    for j, offset in others:
        device = peer(offset)

        @pl.when(is_live(flat(device)))
        def _():
            remote(
                closed64.at[place(flat(device)), pl.ds(0, BAND), :],
                last_hbm.at[me, pl.ds(0, BAND), :],
                back_sems.at[4],
                back_sems.at[5],
                device,
            ).start()

    own = (
        pltpu.make_async_copy(
            closed.at[:, :, place(me), pl.ds(0, BAND), :],
            out_hbm.at[:, :, me, pl.ds(0, BAND), :],
            own_sems.at[0],
        ),
        pltpu.make_async_copy(closed64.at[place(me)], last_hbm.at[me], own_sems.at[1]),
    )
    stat_own = pltpu.make_async_copy(stat, stats_hbm.at[me], own_sems.at[2])
    stat_own.start()

    @pl.when(live)
    def _():
        own[0].start()
        own[1].start()
        own[0].wait()
        own[1].wait()

    stat_own.wait()

    def sent(part, sem):
        remote(part, part, sem, recv_sems.at[0], (px, pz)).wait_send()

    def came(part, sem):
        remote(part, part, send_sems.at[0], sem, (px, pz)).wait_recv()

    rest = pl.ds(0, PARTS - 1)

    def await_sent(count):
        sent(closed.at[:, :, pl.ds(0, count), pl.ds(0, BAND), :], back_sems.at[0])
        sent(closed64.at[pl.ds(0, count), pl.ds(0, BAND), :], back_sems.at[4])

    from_live(await_sent)
    sent(arrived.at[0, rest, pl.ds(0, 1), :], back_sems.at[2])
    came(stats_hbm.at[rest], back_sems.at[3])

    @pl.when(live)
    def _():
        sent(ready.at[rest, pl.ds(1, SLOTS - 1), pl.ds(0, BAND), :], send_sems.at[0])
        sent(ready.at[rest, 0, pl.ds(0, BAND), :], send_sems.at[1])
        came(out_hbm.at[:, :, rest, pl.ds(0, BAND), :], back_sems.at[1])
        came(last_hbm.at[rest, pl.ds(0, BAND), :], back_sems.at[5])


def close_kernel(
    cut_ref, dt_ref, power_ref, old_ref, in_ref, last_ref, stats_ref, cs_ref,
    out_ref, cfl_ref, energy_ref, terms, spectra,
):
    fastest = stats_ref[0]
    summed = stats_ref[0]
    for s in range(1, PARTS):
        fastest = jnp.maximum(fastest, stats_ref[s])
        summed = summed + stats_ref[s]
    fastest, summed = jnp.max(fastest[:, :1]), jnp.max(summed[:, 1:2])
    energy = 0.5 * summed * (1.0 / float(GRID**3))
    dt = dt_ref[0]
    cfl_ref[0] = dt * fastest * GRID * (1.0 / (2.0 * math.pi))
    energy_ref[0] = energy
    twice = jnp.maximum(jnp.full((DEPTH, 384), 2.0 * energy, f32), 0.5)
    forcing = power_ref[0] / twice
    eighth = lax.broadcasted_iota(jnp.int32, (PARTS, 128), 1) // 8

    out_ref[:, :, DEPTH:, :] = jnp.zeros((2, 3, 96 - DEPTH, 384), f32)

    pair = pl.program_id(0)
    live = is_live(lax.axis_index("py") * lax.axis_size("pz") + lax.axis_index("pz"))

    @pl.when(live)
    def _():
        for odd in range(2):
            ky = 2 * pair + odd
            for a in range(3):
                terms[128 * a : 128 * (a + 1), :] = in_ref[a, pl.ds(ky, GRID, stride=8), :].T
            last = last_ref[pl.ds(ky, PARTS, stride=8), :]
            apart = jnp.concatenate(
                [jnp.where(eighth == x, last, 0.0) for x in range(BAND)], axis=0
            )
            terms[384:432, :] = apart.T[:48]
            spectra[odd] = data_by_table(terms[...], cs_ref)
        waves, square, inverse, keep = pair_waves(pair, cut_ref)

        spot = lax.broadcasted_iota(jnp.int32, (DEPTH, 128), 1)

        def of_pair(a, c):
            found = []
            for odd in range(2):
                re, im = (
                    spectra[odd, 128 * a + 64 * k : 128 * a + 64 * (k + 1), :] for k in range(2)
                )
                last = spectra[odd, 384:392, :]
                for x in range(1, BAND):
                    last = last + spectra[odd, 384 + 8 * x : 392 + 8 * x, :]
                zeros = jnp.zeros((7, 256), f32)
                re = jnp.concatenate([re, last[2 * a : 2 * a + 1], zeros], axis=0)
                im = jnp.concatenate([im, last[2 * a + 1 : 2 * a + 2], zeros], axis=0)
                if c == 0:
                    one, other = re[:, :128], im[:, 128:]
                else:
                    one, other = im[:, :128], -re[:, 128:]
                found.append((one + other, jnp.where(spot == 64, one - other, one + other)))
            (even, even_low), (odd, odd_low) = found
            even_low, odd = pltpu.roll(even_low, 64, 1), pltpu.roll(odd, 64, 1)
            return jnp.concatenate(
                [even, jnp.where(spot < 64, even_low, odd), jnp.where(spot < 64, odd, odd_low)], axis=1
            )

        for c in range(2):
            old = project([old_ref[c, a, :, :] for a in range(3)], waves, inverse, keep)
            forced = project([of_pair(a, c) for a in range(3)], waves, inverse, keep)
            for a in range(3):
                out_ref[c, a, :DEPTH, :] = old[a] + dt * (
                    forced[a] + forcing * old[a] - viscosity * square * old[a]
                )

    @pl.when(jnp.logical_not(live))
    def _():
        out_ref[:, :, :DEPTH, :] = jnp.zeros((2, 3, DEPTH, 384), f32)


SM = pl.BlockSpec(memory_space=pltpu.SMEM)
ANY = pl.BlockSpec(memory_space=pl.ANY)
VMEM_BYTES = 60 * 1024 * 1024


def on_device(velocity_hat, time_step, power, cutoffs):
    tx, cs, ey, zt, zb, eyt = (jnp.asarray(t) for t in tables())
    shape = jax.ShapeDtypeStruct
    block = pl.BlockSpec((2, 3, DEPTH, 384), lambda i: (0, 0, 0, i))
    whole = lambda a: pl.BlockSpec(a.shape, lambda i: (0,) * a.ndim)
    dma = pltpu.SemaphoreType.DMA
    chunks, last, stats = pl.pallas_call(
        exchange_kernel,
        out_shape=(
            shape((3, BAND, PARTS, 8, 128), f32),
            shape((PARTS, 8, 128), f32),
            shape((PARTS, 1, 128), f32),
        ),
        in_specs=[SM] + [ANY] * 6,
        out_specs=(ANY, ANY, ANY),
        scratch_shapes=[
            pltpu.VMEM((3, 2, 3, DEPTH, 384), f32),
            pltpu.VMEM((2, 512, 256), bf16),
            *(pltpu.VMEM(t.shape, bf16) for t in (ey, zt, zb, eyt)),
            pltpu.VMEM((2, 2304, 256), f32),
            pltpu.VMEM((2, 40, 256), f32),
            pltpu.VMEM((4, 40, 128), f32),
            pltpu.VMEM((3, BAND * STRIDE, 128), f32),
            pltpu.VMEM((PARTS, SLOTS, 8, 128), f32),
            pltpu.VMEM((SLOTS, PARTS, 8, 128), f32),
            pltpu.VMEM((256, 256), f32),
            pltpu.VMEM((GRID, 128), f32),
            pltpu.VMEM((6, GRID, GRID), f32),
            pltpu.VMEM((2 * GRID, 384), f32),
            pltpu.VMEM((2 * GRID, 128), f32),
            pltpu.VMEM((3, BAND, len(LIVE), 8, 128), f32),
            pltpu.VMEM((len(LIVE), 8, 128), f32),
            pltpu.VMEM((8, GRID), f32),
            pltpu.VMEM((8, GRID), f32),
            pltpu.VMEM((1, 128), f32),
            dma((11,)),
            dma((2,)),
            dma((BAND + 1,)),
            dma((6,)),
            dma((3,)),
        ],
        compiler_params=pltpu.CompilerParams(
            collective_id=0, has_side_effects=True, vmem_limit_bytes=VMEM_BYTES
        ),
    )(cutoffs, velocity_hat, tx, ey, zt, zb, eyt)
    chunks = chunks.reshape(3, BAND * PARTS * 8, 128)
    last = last.reshape(PARTS * 8, 128)
    return pl.pallas_call(
        close_kernel,
        grid=(3,),
        out_shape=(shape((2, 3, 96, 1152), f32), shape((1,), f32), shape((1,), f32)),
        in_specs=[SM, SM, SM, block, whole(chunks), whole(last), whole(stats), whole(cs)],
        out_specs=(pl.BlockSpec((2, 3, 96, 384), lambda i: (0, 0, 0, i)), SM, SM),
        scratch_shapes=[pltpu.VMEM((432, GRID), f32), pltpu.VMEM((2, 432, 256), f32)],
        compiler_params=pltpu.CompilerParams(vmem_limit_bytes=VMEM_BYTES),
    )(cutoffs, time_step, power, velocity_hat, chunks, last, stats, cs)


def solution(mesh):
    return jax.shard_map(
        on_device,
        mesh=mesh,
        in_specs=(P("member", None, None, ("py", "pz")), P("member"), P("member"), P("member")),
        out_specs=(P("member", None, None, ("py", "pz")), P("member"), P("member")),
        check_vma=False,
    )
```
